32 devices in a mesh: groups: 2 (over y), gx: 16 (over z, x, core).
Axes of the slice: x: 2, y: 2, z: 4, core: 2. Of those that a mesh axis runs over, the one named last changes fastest.
Arguments:
- stream_in: bfloat16 [32, 8192], P(('groups', 'gx')), parts along dimension 0, may hold values from -6 to 6
- query: bfloat16 [32, 8192], P(('groups', 'gx')), parts along dimension 0, may hold values from -4.5 to 4.5
- key_new: bfloat16 [32, 1024], P(('groups', 'gx')), parts along dimension 0, may hold values from -4.5 to 4.5
- value_new: bfloat16 [32, 1024], P(('groups', 'gx')), parts along dimension 0, may hold values from -6 to 6
- key_cache: bfloat16 [32, 128, 1024], P(('groups', 'gx')), parts along dimension 0, may hold values from -6 to 6
- value_cache: bfloat16 [32, 128, 1024], P(('groups', 'gx')), parts along dimension 0, may hold values from -6 to 6
- lengths: int32 [32], P(('groups', 'gx')), parts along dimension 0, may hold values from 1 to 128, as said below
- route_ids: int32 [32, 2], P(('groups', 'gx')), parts along dimension 0, may hold values from 0 to 3, as said below
- route_scores: float32 [32, 2], P(('groups', 'gx')), parts along dimension 0, may hold values from -6 to 6
- out_weight: bfloat16 [8192, 8192], P(None, 'gx'), may hold values from -0.0625 to 0.0625
- norm_gain: float32 [8192], replicated, may hold values from 0.1 to 1.9
- gate_weight: bfloat16 [2, 16384, 7168], P(None, 'gx'), may hold values from -0.0625 to 0.0625
- up_weight: bfloat16 [2, 16384, 7168], P(None, 'gx'), may hold values from -0.0625 to 0.0625
- down_weight: bfloat16 [2, 114688, 1024], P(None, 'gx'), may hold values from -0.046875 to 0.046875
Outputs:
- layer_out: bfloat16 [32, 8192], P(('groups', 'gx')), parts along dimension 0
The draws below stay inside these ranges and needn't reach their ends.
There are 2 independent parts, one for each index of `groups`. The reference program is written for one: setup_inputs(seed, part) draws one part's arguments, and reference() takes and returns one part's arrays. A program takes and returns all parts, laid end to end along the dimension named above; an argument that names none is the same for every part. Nothing has to cross between parts.
Inputs may be any that keep to these rules, and one draw needn't show every extreme that they name: `lengths`: 1 to 128; some sequence fills all 128 slots. `route_ids`: each row names two different experts of 0 to 3; in one replica's batch each of the experts 0 and 1 is named by at most 10 sequences, and one of them by exactly 10.
All inputs are finite; a program needn't handle non-finite values.
Results may differ from the reference program's by a relative error of at most 0.0095.
Values may be sent and summed in bfloat16 or wider, within the bound.
A program may use at most 192 MiB of HBM per device.

```python
import jax
import jax.numpy as jnp
from jax import lax

D = 8192
NH = 64
KVH = 8
HS = 128
H = 14336
RESIDENT = 2
MSPLIT = 8
CTX = 128
HSPLIT = 2
BATCH = 16


def shared_heads(key):
    base = jax.random.fold_in(key, 71)
    key_q, key_k = jax.random.split(base, 2)
    queries = jnp.clip(jax.random.normal(key_q, (BATCH, NH, HS), jnp.float32), -4.5, 4.5)
    keys = jnp.clip(jax.random.normal(key_k, (BATCH, KVH, HS), jnp.float32), -4.5, 4.5)
    return (queries.reshape(BATCH, NH * HS), keys.reshape(BATCH, KVH * HS))


def draw_query(key, part):
    return shared_heads(key)[0].astype(jnp.bfloat16)


def draw_key_new(key, part):
    return shared_heads(key)[1].astype(jnp.bfloat16)


def draw_lengths(key, part):
    key_len, key_full = jax.random.split(jax.random.fold_in(key, 5))
    filled = jax.random.randint(key_len, (BATCH,), 1, CTX + 1)
    chosen = jax.random.randint(key_full, (), 0, BATCH)
    return jnp.where(jnp.arange(BATCH) == chosen, CTX, filled).astype(jnp.int32)


def draw_route_ids(key, part):
    keys = jax.random.split(jax.random.fold_in(key, 9), 6)
    limit = 5 * BATCH // 8
    rank_a = jax.random.permutation(keys[0], BATCH)
    other_count = jax.random.randint(keys[1], (), BATCH // 4, limit + 1)
    rank_b = jax.random.permutation(keys[2], BATCH)
    in_a = rank_a < limit
    in_b = rank_b < other_count
    flip = jax.random.randint(keys[3], (), 0, 2)
    in_zero = jnp.where(flip == 0, in_a, in_b)
    in_one = jnp.where(flip == 0, in_b, in_a)
    spare = 2 + jax.random.randint(keys[4], (BATCH,), 0, 2)
    first = jnp.where(in_zero, 0, jnp.where(in_one, 1, 2))
    second = jnp.where(in_zero & in_one, 1, jnp.where(in_zero | in_one, spare, 3))
    order = jax.random.randint(keys[5], (BATCH,), 0, 2) == 1
    left = jnp.where(order, second, first)
    right = jnp.where(order, first, second)
    return jnp.stack([left, right], axis=-1).astype(jnp.int32)


def shard_levels(key, extent, pieces, smallest, largest):
    def one(dim, shards_of):
        steps = jax.random.uniform(jax.random.fold_in(jax.random.fold_in(key, 6), dim), (shards_of,), jnp.float32, smallest / len(pieces), largest / len(pieces))
        return jnp.repeat(jnp.exp(steps), extent[dim] // shards_of).reshape((-1,) + (1,) * (len(extent) - dim - 1))

    gain = one(*pieces[0])
    for cut in pieces[1:]:
        gain = gain * one(*cut)
    return gain


def noise(rng, dims, scale, reach, cuts=(), kind=jnp.bfloat16):
    array = scale * jax.random.normal(rng, dims, jnp.float32)
    if cuts:
        array = array * shard_levels(rng, dims, cuts, -0.22, 0.18)
    return jnp.clip(array, -reach, reach).astype(kind)


def setup_inputs(seed: int = 0, part: int = 0) -> dict:
    arg_keys = jax.random.split(jax.random.key(seed), 15)
    part_splits = jax.random.split(jax.random.fold_in(arg_keys[14], part), 15)
    return {
        "stream_in": noise(part_splits[0], (BATCH, D), 1.0, 6.0, ((0, 16),)),
        "query": draw_query(jax.random.fold_in(jax.random.fold_in(arg_keys[14], part), 71), part),
        "key_new": draw_key_new(jax.random.fold_in(jax.random.fold_in(arg_keys[14], part), 71), part),
        "value_new": noise(part_splits[3], (BATCH, KVH * HS), 1.0, 6.0, ((0, 16),)),
        "key_cache": noise(part_splits[4], (BATCH, CTX, KVH * HS), 1.0, 6.0, ((0, 16),)),
        "value_cache": noise(part_splits[5], (BATCH, CTX, KVH * HS), 1.0, 6.0, ((0, 16),)),
        "lengths": draw_lengths(jax.random.fold_in(jax.random.fold_in(arg_keys[14], part), 71), part),
        "route_ids": draw_route_ids(jax.random.fold_in(jax.random.fold_in(arg_keys[14], part), 71), part),
        "route_scores": noise(part_splits[8], (BATCH, 2), 1.0, 6.0, ((0, 16),), jnp.float32),
        "out_weight": noise(arg_keys[9], (NH * HS, D), (NH * HS) ** -0.5, 0.0625, ((1, 16),)),
        "norm_gain": jnp.clip(1.0 + 0.18 * jax.random.normal(arg_keys[10], (D,), jnp.float32), 0.1, 1.9),
        "gate_weight": noise(arg_keys[11], (RESIDENT, HSPLIT * D, H // HSPLIT), D ** -0.5, 0.0625, ((1, 16),)),
        "up_weight": noise(arg_keys[12], (RESIDENT, HSPLIT * D, H // HSPLIT), D ** -0.5, 0.0625, ((1, 16),)),
        "down_weight": noise(arg_keys[13], (RESIDENT, MSPLIT * H, D // MSPLIT), H ** -0.5, 0.046875, ((1, 16),)),
    }


def attend_one(items):
    query_row, key_row, value_row, key_slots, value_slots, length = items
    group = NH // KVH
    scale = HS ** (-0.5)
    q_four = query_row.astype(jnp.float32).reshape(KVH, group, HS)
    k_own = key_row.astype(jnp.float32).reshape(KVH, HS)
    v_own = value_row.astype(jnp.float32).reshape(KVH, HS)
    k_all = key_slots.astype(jnp.float32).reshape(CTX, KVH, HS)
    v_all = value_slots.astype(jnp.float32).reshape(CTX, KVH, HS)
    scores = jnp.einsum('kgd,ckd->kgc', q_four, k_all) * scale
    live = jnp.arange(CTX, dtype=jnp.int32) < length
    scores = jnp.where(live[None, None, :], scores, -1e+30)
    own = jnp.einsum('kgd,kd->kg', q_four, k_own) * scale
    top = jnp.maximum(lax.optimization_barrier(jnp.max(scores, axis=-1)), own)
    e_cache = jnp.exp(scores - top[:, :, None])
    e_own = jnp.exp(own - top)
    total = lax.optimization_barrier(jnp.sum(e_cache, axis=-1)) + e_own
    p_cache = (e_cache / total[:, :, None]).astype(jnp.bfloat16)
    p_own = (e_own / total).astype(jnp.bfloat16)
    mixed = jnp.einsum('kgc,ckd->kgd', p_cache.astype(jnp.float32), v_all)
    mixed = mixed + p_own.astype(jnp.float32)[:, :, None] * v_own[:, None, :]
    return mixed.reshape(NH * HS).astype(jnp.bfloat16)

def reference(stream_in, query, key_new, value_new, key_cache, value_cache, lengths, route_ids, route_scores, out_weight, norm_gain, gate_weight, up_weight, down_weight):
    gate_full = gate_weight.reshape(RESIDENT, MSPLIT, HSPLIT, D // MSPLIT, H // HSPLIT).transpose(0, 1, 3, 2, 4).reshape(RESIDENT, D, H)
    up_full = up_weight.reshape(RESIDENT, MSPLIT, HSPLIT, D // MSPLIT, H // HSPLIT).transpose(0, 1, 3, 2, 4).reshape(RESIDENT, D, H)
    down_full = down_weight.reshape(RESIDENT, MSPLIT, HSPLIT, H // HSPLIT, D // MSPLIT).transpose(0, 2, 3, 1, 4).reshape(RESIDENT, H, D)
    attn = lax.map(attend_one, (query, key_new, value_new, key_cache, value_cache, lengths))
    proj = jnp.dot(attn, out_weight, preferred_element_type=jnp.float32).astype(jnp.bfloat16)
    resid = stream_in.astype(jnp.float32) + proj.astype(jnp.float32)
    power = lax.optimization_barrier(jnp.mean(resid * resid, axis=-1, keepdims=True))
    normed = (resid * lax.rsqrt(power + 1e-05) * norm_gain).astype(jnp.bfloat16)
    probs = jax.nn.softmax(route_scores, axis=-1)
    columns = []
    for expert in range(RESIDENT):
        columns.append(lax.optimization_barrier(jnp.sum(jnp.where(route_ids == expert, probs, 0.0), axis=-1)))
    weight = jnp.stack(columns, axis=-1).astype(jnp.bfloat16)
    ffn = jnp.zeros(resid.shape, jnp.float32)
    for expert in range(RESIDENT):
        gate = jnp.dot(normed, gate_full[expert], preferred_element_type=jnp.float32)
        upper = jnp.dot(normed, up_full[expert], preferred_element_type=jnp.float32)
        hidden = (jax.nn.silu(gate) * upper).astype(jnp.bfloat16)
        result = jnp.dot(hidden, down_full[expert], preferred_element_type=jnp.float32)
        ffn = ffn + weight[:, expert].astype(jnp.float32)[:, None] * result
    return (resid + ffn).astype(jnp.bfloat16)
```

```python
import functools

import jax
import jax.numpy as jnp
from jax import lax
from jax.experimental import pallas as pl
from jax.experimental.pallas import tpu as pltpu
from jax.sharding import PartitionSpec as P

NH = 64
KVH = 8
HS = 128
RESIDENT = 2
MSPLIT = 8
PAD = 16
RING = 3
ORDER = (0, 2, 1, 3)
MESH = pl.DeviceIdType.MESH


QUADS = 7


def large_kernel(
    members,
    query_hbm,
    key_new_hbm,
    value_new_hbm,
    key_hbm,
    value_hbm,
    lengths,
    route_ids,
    route_scores,
    stream_hbm,
    gain_hbm,
    out_weight,
    gate_weight,
    up_weight,
    down_weight,
    out,
    query,
    key_new,
    value_new,
    stream,
    gain,
    key_cache,
    value_cache,
    in_sem,
    heads,
    own_rows,
    stream_rows,
    stream_recv,
    stream_flat,
    pool,
    attn_send,
    attn_recv,
    attn_wide,
    attn_rows,
    resid_keep,
    y_send,
    y_recv,
    sq_send,
    sq_recv,
    slots_in,
    acc,
    px_send,
    px_recv,
    pz_send,
    pz_recv,
    hid_send,
    hid_recv,
    total,
    final_flat,
    final_send,
    final_recv,
    wo_sem,
    gu_sem,
    down_sem,
    a_send,
    a_relay,
    a_recv,
    s_send,
    s_recv,
    q_send,
    q_recv,
    r_send,
    r_recv,
    x_send,
    x_recv,
    z_send,
    z_recv,
    h_send,
    h_relay,
    h_recv,
    f_send,
    f_recv,
):
    f32, bf16 = jnp.float32, jnp.bfloat16
    hsplit = members // MSPLIT
    me = lax.axis_index("gx")
    m = me // hsplit
    h = lax.rem(me, hsplit)
    batch = members
    cols = y_send.shape[1]
    width = cols * members
    block = width // MSPLIT
    group = NH // KVH
    chunk = acc.shape[1]
    cap = batch * 5 // 8
    packed = px_send.shape[1]
    hid_rows = hid_send.shape[0]
    lead = slots_in.shape[1]
    lanes = sq_send.shape[1]
    half = MSPLIT // 2
    side = block // cols
    pieces = NH * HS // block

    def peer(d):
        return lax.rem(me + d, members)

    def model(d):
        d = jnp.asarray(d, jnp.int32)
        to = 0
        for b in (1, 2, 4):
            to = to + lax.rem(lax.div(m, b) + lax.div(d, b), 2) * b
        return to

    def mate(d):
        return lax.rem(h + d, hsplit)

    def remote(src, dst, send, recv, device):
        return pltpu.make_async_remote_copy(
            src_ref=src,
            dst_ref=dst,
            send_sem=send,
            recv_sem=recv,
            device_id={"gx": device},
            device_id_type=MESH,
        )

    barrier = pltpu.get_barrier_semaphore()

    @pl.loop(1, members)
    def _(d):
        pl.semaphore_signal(barrier, inc=1, device_id={"gx": peer(d)}, device_id_type=MESH)

    inputs = [
        pltpu.make_async_copy(src, dst, in_sem.at[k])
        for k, (src, dst) in enumerate(
            (
                (stream_hbm, stream),
                (query_hbm, query),
                (key_new_hbm, key_new),
                (value_new_hbm, value_new),
                (key_hbm, key_cache),
                (value_hbm, value_cache),
                (gain_hbm.at[me], gain),
            )
        )
    ]
    for copy in inputs:
        copy.start()

    def wo_copy(k):
        return pltpu.make_async_copy(
            out_weight.at[pl.ds(k * block, block), :],
            pool.at[0, k // side, :, pl.ds(k % side * cols, cols)],
            wo_sem.at[k],
        )

    def order(i):
        return jnp.where(i < half, MSPLIT - 1 - 2 * i, 2 * (MSPLIT - 1 - i))

    def gu_copy(i, q):
        r, w = q // 2, (gate_weight, up_weight)[q % 2]
        at = pl.multiple_of(model(order(i)) * chunk, 128)
        return pltpu.make_async_copy(
            w.at[r, :, pl.ds(at, chunk)],
            pool.at[lax.rem(i + 1, QUADS), q, :, pl.ds(0, chunk)],
            gu_sem.at[i, q],
        )

    def down_order(k):
        return jnp.where(k < half, 2 * k, 2 * (k - half) + 1)

    def down_slot(k, r):
        return pool.at[2 + k // 2, k % 2 * 2 + r, pl.ds(0, chunk), :]

    def down_copy(k, r):
        at = pl.multiple_of(model(down_order(k)) * chunk, 16)
        return pltpu.make_async_copy(
            down_weight.at[r, pl.ds(at, chunk), :], down_slot(k, r), down_sem.at[k, r]
        )

    def down_pair(k):
        for j in range(2):
            for r in range(RESIDENT):
                down_copy(2 * k + j, r).start()

    for k in range(pieces):
        wo_copy(k).start()

    @pl.loop(0, QUADS - 1)
    def _(i):
        for q in range(4):
            gu_copy(i, q).start()

    scale = HS ** (-0.5)
    spot = lax.broadcasted_iota(jnp.int32, (1, HS), 1)
    full = lambda v: jnp.full((1, HS), v)
    s0, s1 = full(route_scores[0, 0]), full(route_scores[0, 1])
    i0, i1 = full(route_ids[0, 0]), full(route_ids[0, 1])
    peak = jnp.maximum(s0, s1)
    x0, x1 = jnp.exp(s0 - peak), jnp.exp(s1 - peak)
    pick = jnp.where(i0 == spot, x0 / (x0 + x1), 0.0) + jnp.where(i1 == spot, x1 / (x0 + x1), 0.0)
    pick = pick.astype(bf16).astype(f32)
    inputs[0].wait()
    for j in range(members):
        stream_rows[j, :, :cols] = stream[:, j * cols : (j + 1) * cols].astype(f32)
        stream_rows[j, :, cols:] = pick
    for copy in inputs[1:4]:
        copy.wait()
    for n in range(NH):
        heads[n : n + 1, :] = query[:, n * HS : (n + 1) * HS].astype(f32)
    for g in range(KVH):
        own_rows[0, g : g + 1, :] = key_new[:, g * HS : (g + 1) * HS].astype(f32)
        own_rows[1, g : g + 1, :] = value_new[:, g * HS : (g + 1) * HS].astype(f32)
    wide_q = heads[...]
    for copy in inputs[4:]:
        copy.wait()
    s = jnp.concatenate(
        [
            lax.dot_general(
                wide_q[g * group : (g + 1) * group].astype(bf16),
                key_cache[:, g * HS : (g + 1) * HS],
                (((1,), (1,)), ((), ())),
                preferred_element_type=f32,
            )
            for g in range(KVH)
        ],
        axis=0,
    )
    s = s * scale
    live = lax.broadcasted_iota(jnp.int32, s.shape, 1) < lengths[0]
    s = jnp.where(live, s, -1e30)
    k_own, v_own = own_rows[0], own_rows[1]
    spread = lambda v: jnp.concatenate(
        [jnp.broadcast_to(v[g : g + 1], (group, HS)) for g in range(KVH)], axis=0
    )
    own = jnp.sum(wide_q * spread(k_own), axis=-1, keepdims=True) * scale
    top = jnp.maximum(jnp.max(s, axis=-1, keepdims=True), own)
    e_cache = jnp.exp(s - top)
    e_own = jnp.exp(own - top)
    norm = jnp.sum(e_cache, axis=-1, keepdims=True) + e_own
    p = e_cache / norm
    p_own = (e_own / norm).astype(bf16).astype(f32)
    mixed = jnp.concatenate(
        [
            jnp.dot(
                p[g * group : (g + 1) * group].astype(bf16),
                value_cache[:, g * HS : (g + 1) * HS],
                preferred_element_type=f32,
            )
            for g in range(KVH)
        ],
        axis=0,
    )
    mixed = mixed + p_own * spread(v_own)
    attn_send[...] = mixed.astype(bf16)

    pl.semaphore_wait(barrier, members - 1)

    def attn_copy(d, slot):
        return remote(
            attn_send, attn_recv.at[slot], a_send.at[d], a_recv.at[slot], model(d) * hsplit + h
        )

    def attn_relay(d, t, slot):
        src = attn_send if isinstance(d, int) else attn_recv.at[slot]
        return remote(
            src, attn_recv.at[slot], a_relay.at[d, t], a_recv.at[slot], m * hsplit + t
        )

    def stream_copy(to, slot):
        return remote(
            stream_rows.at[to], stream_recv.at[slot], s_send.at[to], s_recv.at[slot], to
        )

    @pl.loop(0, MSPLIT - 1)
    def _(i):
        attn_copy(MSPLIT - 1 - i, me).start()

    @pl.loop(1, hsplit)
    def _(d):
        attn_relay(0, mate(d), me).start()

    @pl.loop(1, members)
    def _(d):
        stream_copy(peer(d), me).start()

    def widen(slot, rows):
        at = pl.multiple_of(slot * NH, NH)
        attn_wide[pl.ds(at, NH), :] = rows.astype(f32)

    widen(me, attn_send[...])
    stream_recv[me] = stream_rows[me]

    @pl.loop(1, MSPLIT)
    def _(i):
        slot = model(i) * hsplit + h
        attn_copy(i, slot).wait_recv()

        @pl.loop(1, hsplit)
        def _(d):
            attn_relay(i, mate(d), slot).start()

        widen(slot, attn_recv[slot])

    @pl.loop(1, members)
    def _(d):
        stream_copy(me, peer(d)).wait_recv()

    for j in range(members):
        stream_flat[j : j + 1, :] = stream_recv[j]

    scales = [stream_flat[:, cols + r : cols + r + 1] for r in range(RESIDENT)]
    sub = lax.broadcasted_iota(jnp.int32, (batch, batch), 0)
    lane = lax.broadcasted_iota(jnp.int32, (batch, batch), 1)
    named, rank, back = [], [], []
    for r in range(RESIDENT):
        col = jnp.where(scales[r] > 0.0, 1.0, 0.0)
        row = jnp.sum(jnp.where(sub == lane, col, 0.0), axis=0, keepdims=True)
        named.append(row)
        rank.append(jnp.sum(jnp.where(sub < lane, col, 0.0), axis=0, keepdims=True))
        place = jnp.sum(jnp.where(lane < sub, row, 0.0), axis=1, keepdims=True)
        at = lax.broadcasted_iota(jnp.int32, (batch, hid_rows), 1)
        hit = at == place.astype(jnp.int32) + r * cap
        back.append(jnp.where(hit, scales[r], 0.0))

    @pl.loop(0, MSPLIT)
    def _(i):
        @pl.loop(1, hsplit)
        def _(d):
            slot = model(i) * hsplit + mate(d)
            attn_copy(i, slot).wait_recv()
            widen(slot, attn_recv[slot])

    for n in range(NH):
        attn_rows[:, n * HS : (n + 1) * HS] = attn_wide[pl.ds(n, batch, stride=NH), :].astype(bf16)

    for k in range(pieces):
        wo_copy(k).wait()
    proj = jnp.zeros((batch, cols), f32)
    for k in range(pieces):
        proj = proj + jnp.dot(
            attn_rows[:, k * block : (k + 1) * block],
            pool[0, k // side, :, k % side * cols : (k % side + 1) * cols],
            preferred_element_type=f32,
        )
    for q in range(4):
        gu_copy(QUADS - 1, q).start()

    resid = stream_flat[:, :cols] + proj.astype(bf16).astype(f32)
    resid_keep[...] = resid
    y_send[...] = (resid * gain[...]).astype(bf16)

    def y_copy(to, slot):
        return remote(y_send, y_recv.at[slot], r_send.at[to], r_recv.at[slot], m * hsplit + to)

    @pl.loop(1, hsplit)
    def _(d):
        y_copy(mate(d), h).start()

    sub_w = lax.broadcasted_iota(jnp.int32, (batch, lanes), 0)
    lane_w = lax.broadcasted_iota(jnp.int32, (batch, lanes), 1)
    squares = jnp.sum(resid * resid, axis=-1, keepdims=True)
    sq_send[...] = jnp.sum(jnp.where(sub_w == lane_w, squares, 0.0), axis=0, keepdims=True)

    def sq_copy(to, slot):
        return remote(sq_send, sq_recv.at[slot], q_send.at[to], q_recv.at[slot], to)

    @pl.loop(1, members)
    def _(d):
        sq_copy(peer(d), me).start()

    sq_recv[me] = sq_send[...]
    y_recv[h] = y_send[...]

    @pl.loop(1, hsplit)
    def _(d):
        y_copy(h, mate(d)).wait_recv()

    y = jnp.concatenate([y_recv[j] for j in range(hsplit)], axis=1)
    bases = [q * cap // 8 * 8 for q in range(4)]
    for q in range(4):
        r = q % 2
        shift = q * cap - bases[q]
        at = lax.broadcasted_iota(jnp.int32, (lead, batch), 0)
        hit = (at == rank[r].astype(jnp.int32) + shift) & (named[r] > 0.0)
        slots_in[q] = jnp.dot(
            jnp.where(hit, 1.0, 0.0).astype(bf16), y, preferred_element_type=f32
        ).astype(bf16)

    def px_copy(i):
        return remote(
            px_send.at[i], px_recv.at[i], x_send.at[i], x_recv.at[i], model(1) * hsplit + h
        )

    def pz_copy(j):
        return remote(
            pz_send.at[j],
            pz_recv.at[j],
            z_send.at[j],
            z_recv.at[j],
            model(2 * (half - 1 - j)) * hsplit + h,
        )

    def sums(i):
        acc[...] = jnp.zeros_like(acc)
        for q in range(4):
            gu_copy(i, q).wait()
            acc[pl.ds(bases[ORDER[q]], lead), :] += jnp.dot(
                slots_in[ORDER[q]],
                pool[lax.rem(i + 1, QUADS), q, :, :chunk],
                preferred_element_type=f32,
            )

    @pl.loop(0, half)
    def _(i):
        sums(i)
        px_send[i] = acc[:packed, :].astype(bf16)
        px_copy(i).start()

        @pl.when(i == 0)
        def _():
            for q in range(4):
                gu_copy(MSPLIT - 1, q).start()

        @pl.when(i > 0)
        def _():
            down_pair(i - 1)

    @pl.loop(half, MSPLIT)
    def _(i):
        sums(i)

        @pl.when(i == half)
        def _():
            down_pair(half - 1)

        px_copy(i - half).wait_recv()
        acc[:packed, :] += px_recv[i - half].astype(f32)

        @pl.when(i < MSPLIT - 1)
        def _():
            pz_send[i - half] = acc[:packed, :].astype(bf16)
            pz_copy(i - half).start()

    @pl.loop(1, members)
    def _(d):
        sq_copy(me, peer(d)).wait_recv()

    power = jnp.sum(sq_recv[...], axis=0)[:, :batch] * (1.0 / width)
    inverse = lax.rsqrt(power + 1e-05)
    at = lax.broadcasted_iota(jnp.int32, (hid_rows, batch), 0)
    scaled = jnp.zeros((hid_rows, 1), f32)
    for r in range(RESIDENT):
        hit = (at == rank[r].astype(jnp.int32) + r * cap) & (named[r] > 0.0)
        scaled = scaled + jnp.sum(jnp.where(hit, inverse, 0.0), axis=1, keepdims=True)

    for j in range(half - 1):
        pz_copy(j).wait_recv()
        acc[:packed, :] += pz_recv[j].astype(f32)
    a = acc[:hid_rows, :] * scaled
    b = acc[2 * cap : 2 * cap + hid_rows, :] * scaled
    hid_send[...] = (a / (1.0 + jnp.exp(-a)) * b).astype(bf16)

    def hid_copy(d, slot):
        return remote(
            hid_send, hid_recv.at[slot], h_send.at[d], h_recv.at[slot], model(d) * hsplit + h
        )

    def hid_relay(j, slot):
        return remote(
            hid_recv.at[slot],
            hid_recv.at[slot],
            h_relay.at[j],
            h_recv.at[slot],
            model(1) * hsplit + h,
        )

    hid_copy(1, m).start()

    @pl.loop(1, half)
    def _(j):
        hid_copy(MSPLIT - 2 * j, m).start()

    hid_recv[m] = hid_send[...]
    total[...] = jnp.zeros_like(total)

    @pl.loop(0, MSPLIT)
    def _(k):
        d = down_order(k)
        slot = model(d)

        @pl.when(k > 0)
        def _():
            hid_copy(d, slot).wait_recv()

        @pl.when((k > 0) & (k < half))
        def _():
            hid_relay(k, slot).start()

        for r in range(RESIDENT):
            down_copy(k, r).wait()
            total[r] += jnp.dot(
                hid_recv[slot],
                pool[2 + k // 2, k % 2 * 2 + r, :chunk, :],
                preferred_element_type=f32,
            )

    resid = resid_keep[...]
    whole = jnp.concatenate([jnp.where(h == j, resid, 0.0) for j in range(hsplit)], axis=1)
    for r in range(RESIDENT):
        for n in range(r * cap, (r + 1) * cap):
            whole = whole + back[r][:, n : n + 1] * total[r, n : n + 1, :]
    tiles = block // HS
    for t in range(tiles):
        final_flat[t * batch : (t + 1) * batch, :] = whole[:, t * HS : (t + 1) * HS]
    for j in range(members):
        final_send[j] = final_flat[pl.ds(j, tiles, stride=batch), :].astype(bf16)

    def final_copy(to, slot):
        return remote(
            final_send.at[to], final_recv.at[slot], f_send.at[to], f_recv.at[slot], to
        )

    @pl.loop(1, members)
    def _(d):
        final_copy(peer(d), me).start()

    final_recv[me] = final_send[me]

    @pl.loop(1, members)
    def _(d):
        to = peer(d)
        stream_copy(to, me).wait_send()
        sq_copy(to, me).wait_send()

    @pl.loop(1, hsplit)
    def _(d):
        y_copy(mate(d), h).wait_send()

    @pl.loop(0, MSPLIT)
    def _(i):
        @pl.loop(1, hsplit)
        def _(d):
            attn_relay(i, mate(d), me).wait_send()

    @pl.loop(1, MSPLIT)
    def _(d):
        attn_copy(d, me).wait_send()

    for i in range(half):
        px_copy(i).wait_send()
    for j in range(half - 1):
        pz_copy(j).wait_send()
    hid_copy(1, m).wait_send()
    for j in range(1, half):
        hid_copy(2 * j, m).wait_send()
        hid_relay(j, m).wait_send()

    @pl.loop(1, members)
    def _(d):
        final_copy(me, peer(d)).wait_recv()

    for j in range(MSPLIT):
        line = final_recv[j * hsplit].astype(f32)
        for k in range(1, hsplit):
            line = line + final_recv[j * hsplit + k].astype(f32)
        out[j * tiles : (j + 1) * tiles, :] = line.astype(bf16)

    @pl.loop(1, members)
    def _(d):
        final_copy(peer(d), me).wait_send()


def large_call(
    stream_in,
    query,
    key_new,
    value_new,
    key_cache,
    value_cache,
    lengths,
    route_ids,
    route_scores,
    out_weight,
    norm_gain,
    gate_weight,
    up_weight,
    down_weight,
):
    f32, bf16 = jnp.float32, jnp.bfloat16
    members = lax.axis_size("gx")
    width = stream_in.shape[1]
    hsplit = members // MSPLIT
    cols = width // members
    block = width // MSPLIT
    batch = members
    narrow = gate_weight.shape[2] // MSPLIT
    vmem = pl.BlockSpec(memory_space=pltpu.VMEM)
    smem = pl.BlockSpec(memory_space=pltpu.SMEM)
    hbm = pl.BlockSpec(memory_space=pl.ANY)
    dma = pltpu.SemaphoreType.DMA
    rows = key_cache.shape[1]
    cap = batch * 5 // 8
    packed = 2 * RESIDENT * cap
    shifts = [q * cap % 8 for q in range(4)]
    lead = (cap + max(shifts) + 7) // 8 * 8
    hid_rows = (RESIDENT * cap + 7) // 8 * 8
    lanes = (batch + 127) // 128 * 128
    half = MSPLIT // 2
    tiles = block // HS
    result = pl.pallas_call(
        functools.partial(large_kernel, members),
        out_shape=jax.ShapeDtypeStruct((width // HS, HS), bf16),
        in_specs=[hbm] * 5 + [smem] * 3 + [hbm] * 6,
        out_specs=vmem,
        scratch_shapes=[
            pltpu.VMEM((1, NH * HS), bf16),
            pltpu.VMEM((1, KVH * HS), bf16),
            pltpu.VMEM((1, KVH * HS), bf16),
            pltpu.VMEM((1, width), bf16),
            pltpu.VMEM((1, cols), f32),
            pltpu.VMEM((rows, KVH * HS), bf16),
            pltpu.VMEM((rows, KVH * HS), bf16),
            dma((7,)),
            pltpu.VMEM((NH, HS), f32),
            pltpu.VMEM((2, KVH, HS), f32),
            pltpu.VMEM((members, 1, cols + HS), f32),
            pltpu.VMEM((members, 1, cols + HS), f32),
            pltpu.VMEM((batch, cols + HS), f32),
            pltpu.VMEM((QUADS, 4, block, block), bf16),
            pltpu.VMEM((NH, HS), bf16),
            pltpu.VMEM((members, NH, HS), bf16),
            pltpu.VMEM((members * NH, HS), f32),
            pltpu.VMEM((batch, NH * HS), bf16),
            pltpu.VMEM((batch, cols), f32),
            pltpu.VMEM((batch, cols), bf16),
            pltpu.VMEM((hsplit, batch, cols), bf16),
            pltpu.VMEM((1, lanes), f32),
            pltpu.VMEM((members, 1, lanes), f32),
            pltpu.VMEM((4, lead, block), bf16),
            pltpu.VMEM((packed + 8, narrow), f32),
            pltpu.VMEM((half, packed, narrow), bf16),
            pltpu.VMEM((half, packed, narrow), bf16),
            pltpu.VMEM((half - 1, packed, narrow), bf16),
            pltpu.VMEM((half - 1, packed, narrow), bf16),
            pltpu.VMEM((hid_rows, narrow), bf16),
            pltpu.VMEM((MSPLIT, hid_rows, narrow), bf16),
            pltpu.VMEM((RESIDENT, hid_rows, block), f32),
            pltpu.VMEM((tiles * batch, HS), f32),
            pltpu.VMEM((members, tiles, HS), bf16),
            pltpu.VMEM((members, tiles, HS), bf16),
            dma((NH * HS // block,)),
            dma((MSPLIT, 4)),
            dma((MSPLIT, RESIDENT)),
        ]
        + [dma((MSPLIT,)), dma((MSPLIT, hsplit))]
        + [dma((members,))] * 5
        + [dma((hsplit,))] * 2
        + [dma((half,))] * 4
        + [dma((MSPLIT,)), dma((half,)), dma((MSPLIT,))]
        + [dma((members,))] * 2,
        compiler_params=pltpu.CompilerParams(
            collective_id=0, has_side_effects=True, vmem_limit_bytes=67043328
        ),
    )(
        query,
        key_new,
        value_new,
        key_cache.reshape(rows, KVH * HS),
        value_cache.reshape(rows, KVH * HS),
        lengths,
        route_ids,
        route_scores,
        stream_in,
        norm_gain.reshape(members, 1, cols),
        out_weight,
        gate_weight,
        up_weight,
        down_weight,
    )
    return result.reshape(1, width)


def small_kernel(
    members,
    query,
    key_new,
    value_new,
    key_hbm,
    value_hbm,
    lengths,
    route_ids,
    route_scores,
    stream,
    gain,
    out_weight,
    gate_weight,
    up_weight,
    down_weight,
    out,
    key_cache,
    value_cache,
    cache_sem,
    heads,
    own_rows,
    stream_rows,
    wo,
    gu,
    down,
    attn_send,
    attn_recv,
    attn_wide,
    attn_rows,
    stream_recv,
    resid_recv,
    resid_send,
    sq_send,
    sq_recv,
    normed,
    slots_in,
    acc,
    part_send,
    part_recv,
    hid_send,
    hid_recv,
    total,
    resid_full,
    final_send,
    final_recv,
    wo_sem,
    gu_sem,
    down_sem,
    a_send,
    a_relay,
    a_recv,
    s_send,
    s_recv,
    q_send,
    q_recv,
    r_send,
    r_recv,
    p_send,
    p_recv,
    h_send,
    h_relay,
    h_recv,
    f_send,
    f_recv,
):
    f32, bf16 = jnp.float32, jnp.bfloat16
    hsplit = members // MSPLIT
    me = lax.axis_index("gx")
    m = me // hsplit
    h = lax.rem(me, hsplit)
    batch = members
    cols = wo.shape[1]
    width = cols * members
    block = width // MSPLIT
    group = NH // KVH
    chunk = gu.shape[3]
    chunks = gate_weight.shape[2] // chunk
    narrow = part_send.shape[2]
    cap = batch * 5 // 8
    packed = part_send.shape[1]
    hid_rows = hid_send.shape[0]
    lead = slots_in.shape[1]
    lanes = sq_send.shape[1]
    ring = gu.shape[0]

    def peer(d):
        return lax.rem(me + d, members)

    def model(d):
        d = jnp.asarray(d, jnp.int32)
        to = 0
        for b in (1, 2, 4):
            to = to + lax.rem(lax.div(m, b) + lax.div(d, b), 2) * b
        return to

    def mate(d):
        return lax.rem(h + d, hsplit)

    def remote(src, dst, send, recv, device):
        return pltpu.make_async_remote_copy(
            src_ref=src,
            dst_ref=dst,
            send_sem=send,
            recv_sem=recv,
            device_id={"gx": device},
            device_id_type=MESH,
        )

    barrier = pltpu.get_barrier_semaphore()

    @pl.loop(1, members)
    def _(d):
        pl.semaphore_signal(barrier, inc=1, device_id={"gx": peer(d)}, device_id_type=MESH)

    key_copy = pltpu.make_async_copy(key_hbm, key_cache, cache_sem.at[0])
    value_copy = pltpu.make_async_copy(value_hbm, value_cache, cache_sem.at[1])
    key_copy.start()
    value_copy.start()
    wo_copy = pltpu.make_async_copy(out_weight, wo, wo_sem)
    wo_copy.start()

    def gu_copy(i, q):
        r, w = q // 2, (gate_weight, up_weight)[q % 2]
        if chunks == 1:
            src = w.at[r]
        else:
            at = pl.multiple_of(model(MSPLIT - 1 - i) * chunk, 128)
            src = w.at[r, :, pl.ds(at, chunk)]
        slot = lax.rem(i, ring)
        return pltpu.make_async_copy(src, gu.at[slot, q], gu_sem.at[slot, q])

    def down_copy(i, r):
        at = pl.multiple_of(model(i) * narrow, 16)
        return pltpu.make_async_copy(
            down_weight.at[r, pl.ds(at, narrow), :], down.at[i, r], down_sem.at[i, r]
        )

    @pl.loop(0, ring)
    def _(i):
        for q in range(4):
            gu_copy(i, q).start()

    @pl.loop(0, MSPLIT)
    def _(i):
        for r in range(RESIDENT):
            down_copy(i, r).start()

    scale = HS ** (-0.5)
    for n in range(NH):
        heads[n : n + 1, :] = query[:, n * HS : (n + 1) * HS].astype(f32)
    for g in range(KVH):
        own_rows[0, g : g + 1, :] = key_new[:, g * HS : (g + 1) * HS].astype(f32)
        own_rows[1, g : g + 1, :] = value_new[:, g * HS : (g + 1) * HS].astype(f32)
    for j in range(members):
        stream_rows[j] = stream[:, j * cols : (j + 1) * cols].astype(f32)
    wide_q = heads[...]
    key_copy.wait()
    value_copy.wait()
    s = jnp.concatenate(
        [
            lax.dot_general(
                wide_q[g * group : (g + 1) * group].astype(bf16),
                key_cache[:, g * HS : (g + 1) * HS],
                (((1,), (1,)), ((), ())),
                preferred_element_type=f32,
            )
            for g in range(KVH)
        ],
        axis=0,
    )
    s = s * scale
    live = lax.broadcasted_iota(jnp.int32, s.shape, 1) < lengths[0]
    s = jnp.where(live, s, -1e30)
    k_own, v_own = own_rows[0], own_rows[1]
    spread = lambda v: jnp.concatenate(
        [jnp.broadcast_to(v[g : g + 1], (group, HS)) for g in range(KVH)], axis=0
    )
    own = jnp.sum(wide_q * spread(k_own), axis=-1, keepdims=True) * scale
    top = jnp.maximum(jnp.max(s, axis=-1, keepdims=True), own)
    e_cache = jnp.exp(s - top)
    e_own = jnp.exp(own - top)
    norm = jnp.sum(e_cache, axis=-1, keepdims=True) + e_own
    p = e_cache / norm
    p_own = (e_own / norm).astype(bf16).astype(f32)
    mixed = jnp.concatenate(
        [
            jnp.dot(
                p[g * group : (g + 1) * group].astype(bf16),
                value_cache[:, g * HS : (g + 1) * HS],
                preferred_element_type=f32,
            )
            for g in range(KVH)
        ],
        axis=0,
    )
    mixed = mixed + p_own * spread(v_own)
    attn_send[:NH, :] = mixed.astype(bf16)
    full = lambda v: jnp.full((PAD, HS), v)
    s0, s1 = full(route_scores[0, 0]), full(route_scores[0, 1])
    i0, i1 = full(route_ids[0, 0]), full(route_ids[0, 1])
    peak = jnp.maximum(s0, s1)
    x0, x1 = jnp.exp(s0 - peak), jnp.exp(s1 - peak)
    row = lax.broadcasted_iota(jnp.int32, (PAD, HS), 0)
    pick = jnp.where(i0 == row, x0 / (x0 + x1), 0.0) + jnp.where(i1 == row, x1 / (x0 + x1), 0.0)
    attn_send[NH:, :] = pick.astype(bf16)

    pl.semaphore_wait(barrier, members - 1)

    def attn_copy(d, slot):
        return remote(
            attn_send, attn_recv.at[slot], a_send.at[d], a_recv.at[slot], model(d) * hsplit + h
        )

    def attn_relay(d, t, slot):
        src = attn_send if isinstance(d, int) else attn_recv.at[slot]
        return remote(
            src, attn_recv.at[slot], a_relay.at[d, t], a_recv.at[slot], m * hsplit + t
        )

    def stream_copy(to, slot):
        return remote(
            stream_rows.at[to], stream_recv.at[slot], s_send.at[to], s_recv.at[slot], to
        )

    @pl.loop(0, MSPLIT - 1)
    def _(i):
        attn_copy(MSPLIT - 1 - i, me).start()

    @pl.loop(1, hsplit)
    def _(d):
        attn_relay(0, mate(d), me).start()

    @pl.loop(1, members)
    def _(d):
        stream_copy(peer(d), me).start()

    attn_recv[me] = attn_send[...]
    stream_recv[me] = stream_rows[me]

    @pl.loop(1, MSPLIT)
    def _(i):
        slot = model(i) * hsplit + h
        attn_copy(i, slot).wait_recv()

        @pl.loop(1, hsplit)
        def _(d):
            attn_relay(i, mate(d), slot).start()

    @pl.loop(0, MSPLIT)
    def _(i):
        @pl.loop(1, hsplit)
        def _(d):
            attn_copy(i, model(i) * hsplit + mate(d)).wait_recv()

    stride = NH + PAD

    @pl.loop(0, members)
    def _(j):
        attn_wide[pl.ds(j * stride, stride), :] = attn_recv[j].astype(f32)

    for n in range(NH):
        attn_rows[:, n * HS : (n + 1) * HS] = attn_wide[pl.ds(n, batch, stride=stride), :].astype(
            bf16
        )
    scales = [attn_wide[pl.ds(NH + r, batch, stride=stride), :][:, :1] for r in range(RESIDENT)]

    sub = lax.broadcasted_iota(jnp.int32, (batch, batch), 0)
    lane = lax.broadcasted_iota(jnp.int32, (batch, batch), 1)
    named, rank, back = [], [], []
    for r in range(RESIDENT):
        col = jnp.where(scales[r] > 0.0, 1.0, 0.0)
        row = jnp.sum(jnp.where(sub == lane, col, 0.0), axis=0, keepdims=True)
        named.append(row)
        rank.append(jnp.sum(jnp.where(sub < lane, col, 0.0), axis=0, keepdims=True))
        place = jnp.sum(jnp.where(lane < sub, row, 0.0), axis=1, keepdims=True)
        at = lax.broadcasted_iota(jnp.int32, (batch, hid_rows), 1)
        hit = at == place.astype(jnp.int32) + r * cap
        back.append(jnp.where(hit, scales[r], 0.0))

    wo_copy.wait()
    proj = jnp.dot(attn_rows[...], wo[...], preferred_element_type=f32).astype(bf16)

    @pl.loop(1, members)
    def _(d):
        stream_copy(me, peer(d)).wait_recv()

    @pl.loop(0, members)
    def _(j):
        resid_send[pl.ds(j, 1), :] = stream_recv[j]

    resid = resid_send[...] + proj.astype(f32)
    resid_send[...] = resid
    sub_w = lax.broadcasted_iota(jnp.int32, (batch, lanes), 0)
    lane_w = lax.broadcasted_iota(jnp.int32, (batch, lanes), 1)
    squares = jnp.sum(resid * resid, axis=-1, keepdims=True)
    sq_send[...] = jnp.sum(jnp.where(sub_w == lane_w, squares, 0.0), axis=0, keepdims=True)

    def sq_copy(to, slot):
        return remote(sq_send, sq_recv.at[slot], q_send.at[to], q_recv.at[slot], to)

    def resid_copy(to, slot):
        return remote(
            resid_send, resid_recv.at[slot], r_send.at[to], r_recv.at[slot], m * hsplit + to
        )

    @pl.loop(1, members)
    def _(d):
        sq_copy(peer(d), me).start()

    @pl.loop(1, hsplit)
    def _(d):
        resid_copy(mate(d), h).start()

    sq_recv[me] = sq_send[...]
    resid_recv[h] = resid_send[...]

    @pl.loop(1, hsplit)
    def _(d):
        resid_copy(h, mate(d)).wait_recv()

    @pl.loop(1, members)
    def _(d):
        sq_copy(me, peer(d)).wait_recv()

    squares = jnp.sum(sq_recv[...], axis=0)
    squares = jnp.sum(jnp.where(sub_w == lane_w, squares, 0.0), axis=1, keepdims=True)
    power = squares * (1.0 / width)
    inverse = lax.rsqrt(power + 1e-05)
    block_resid = jnp.concatenate([resid_recv[j] for j in range(hsplit)], axis=1)
    normed[...] = (block_resid * inverse * gain[m]).astype(bf16)

    bases = [q * cap // 8 * 8 for q in range(4)]
    for q in range(4):
        r = q % 2
        shift = q * cap - bases[q]
        at = lax.broadcasted_iota(jnp.int32, (lead, batch), 0)
        hit = (at == rank[r].astype(jnp.int32) + shift) & (named[r] > 0.0)
        slots_in[q] = jnp.dot(
            jnp.where(hit, 1.0, 0.0).astype(bf16), normed[...], preferred_element_type=f32
        ).astype(bf16)
    acc[...] = jnp.zeros_like(acc)

    def part_copy(to, slot):
        return remote(
            part_send.at[to],
            part_recv.at[slot],
            p_send.at[to],
            p_recv.at[slot],
            to * hsplit + h,
        )

    def gather(slot, q):
        return jnp.dot(
            slots_in[ORDER[q]], gu[slot, q], preferred_element_type=f32
        ), pl.ds(bases[ORDER[q]], lead)

    if chunks == 1:
        for q in range(4):
            gu_copy(0, q).wait()
            value, rows = gather(0, q)
            acc[rows, :] += value
        for to in range(MSPLIT):
            part_send[to] = acc[:packed, to * narrow : (to + 1) * narrow].astype(bf16)

        @pl.loop(1, MSPLIT)
        def _(d):
            part_copy(model(d), m).start()

    else:

        @pl.loop(0, MSPLIT)
        def _(i):
            slot = lax.rem(i, ring)
            to = model(MSPLIT - 1 - i)
            for q in range(4):
                gu_copy(i, q).wait()
                value, rows = gather(slot, q)
                acc[rows, :] += value

                @pl.when(i < MSPLIT - ring)
                def _():
                    gu_copy(i + ring, q).start()

            part_send[to] = acc[:packed, :].astype(bf16)
            acc[...] = jnp.zeros_like(acc)

            @pl.when(i < MSPLIT - 1)
            def _():
                part_copy(to, m).start()

    @pl.loop(1, MSPLIT)
    def _(d):
        part_copy(m, model(d)).wait_recv()

    part_recv[m] = part_send[m]
    acc[:packed, :narrow] = jnp.sum(part_recv[...].astype(f32), axis=0)
    a = acc[:hid_rows, :narrow]
    b = acc[2 * cap : 2 * cap + hid_rows, :narrow]
    hid_send[...] = (a / (1.0 + jnp.exp(-a)) * b).astype(bf16)

    def hid_copy(d, slot):
        return remote(
            hid_send, hid_recv.at[slot], h_send.at[d], h_recv.at[slot], model(d) * hsplit + h
        )

    def hid_relay(j, slot):
        return remote(
            hid_recv.at[slot],
            hid_recv.at[slot],
            h_relay.at[j],
            h_recv.at[slot],
            model(1) * hsplit + h,
        )

    hid_copy(1, m).start()

    @pl.loop(1, MSPLIT // 2)
    def _(j):
        hid_copy(MSPLIT - 2 * j, m).start()

    hid_recv[m] = hid_send[...]
    total[...] = jnp.zeros_like(total)

    def expert_sums(i, slot):
        for r in range(RESIDENT):
            down_copy(i, r).wait()
            total[r] += jnp.dot(hid_recv[slot], down[i, r], preferred_element_type=f32)

    @pl.loop(0, MSPLIT // 2)
    def _(j):
        even, odd = model(2 * j), model(2 * j + 1)

        @pl.when(j > 0)
        def _():
            hid_copy(2 * j, even).wait_recv()
            hid_relay(j, even).start()

        expert_sums(2 * j, even)
        hid_copy(1, odd).wait_recv()
        expert_sums(2 * j + 1, odd)

    whole = jnp.where(h == 0, 1.0, 0.0) * block_resid
    for r in range(RESIDENT):
        if batch > 32:
            whole = whole + jnp.dot(
                back[r], total[r], precision=lax.Precision.HIGHEST, preferred_element_type=f32
            )
        else:
            for n in range(r * cap, (r + 1) * cap):
                whole = whole + back[r][:, n : n + 1] * total[r, n : n + 1, :]
    resid_full[...] = whole

    @pl.loop(0, members)
    def _(j):
        final_send[j] = resid_full[pl.ds(j, 1), :]

    def final_copy(to, slot):
        return remote(
            final_send.at[to], final_recv.at[slot], f_send.at[to], f_recv.at[slot], to
        )

    @pl.loop(1, members)
    def _(d):
        final_copy(peer(d), me).start()

    final_recv[me] = final_send[me]

    @pl.loop(1, members)
    def _(d):
        final_copy(me, peer(d)).wait_recv()

    for j in range(MSPLIT):
        line = final_recv[j * hsplit]
        for k in range(1, hsplit):
            line = line + final_recv[j * hsplit + k]
        out[:, j * block : (j + 1) * block] = line.astype(bf16)

    @pl.loop(1, members)
    def _(d):
        to = peer(d)
        stream_copy(to, me).wait_send()
        sq_copy(to, me).wait_send()
        final_copy(to, me).wait_send()

    @pl.loop(1, hsplit)
    def _(d):
        resid_copy(mate(d), h).wait_send()

    @pl.loop(0, MSPLIT)
    def _(i):
        @pl.loop(1, hsplit)
        def _(d):
            attn_relay(i, mate(d), me).wait_send()

    @pl.loop(1, MSPLIT)
    def _(d):
        attn_copy(d, me).wait_send()
        part_copy(model(d), m).wait_send()

    hid_copy(1, m).wait_send()

    @pl.loop(1, MSPLIT // 2)
    def _(j):
        hid_copy(2 * j, m).wait_send()
        hid_relay(j, m).wait_send()


def on_device(
    stream_in,
    query,
    key_new,
    value_new,
    key_cache,
    value_cache,
    lengths,
    route_ids,
    route_scores,
    out_weight,
    norm_gain,
    gate_weight,
    up_weight,
    down_weight,
):
    f32, bf16 = jnp.float32, jnp.bfloat16
    members = lax.axis_size("gx")
    width = stream_in.shape[1]
    hsplit = members // MSPLIT
    cols = width // members
    block = width // MSPLIT
    batch = members
    hidden_cols = gate_weight.shape[2]
    narrow = hidden_cols // MSPLIT
    chunk = narrow if narrow % 128 == 0 else hidden_cols
    ring = min(RING, hidden_cols // chunk)
    vmem = pl.BlockSpec(memory_space=pltpu.VMEM)
    smem = pl.BlockSpec(memory_space=pltpu.SMEM)
    hbm = pl.BlockSpec(memory_space=pl.ANY)
    dma = pltpu.SemaphoreType.DMA
    rows = key_cache.shape[1]
    cap = batch * 5 // 8
    packed = 2 * RESIDENT * cap
    shifts = [q * cap % 8 for q in range(4)]
    lead = (cap + max(shifts) + 7) // 8 * 8
    hid_rows = (RESIDENT * cap + 7) // 8 * 8
    lanes = (batch + 127) // 128 * 128
    if narrow % 128 == 0 and narrow <= block and NH * HS * cols == 4 * block * block:
        return large_call(
            stream_in,
            query,
            key_new,
            value_new,
            key_cache,
            value_cache,
            lengths,
            route_ids,
            route_scores,
            out_weight,
            norm_gain,
            gate_weight,
            up_weight,
            down_weight,
        )
    return pl.pallas_call(
        functools.partial(small_kernel, members),
        out_shape=jax.ShapeDtypeStruct((1, width), bf16),
        in_specs=[vmem] * 3 + [hbm] * 2 + [smem] * 3 + [vmem] * 2 + [hbm] * 4,
        out_specs=vmem,
        scratch_shapes=[
            pltpu.VMEM((rows, KVH * HS), bf16),
            pltpu.VMEM((rows, KVH * HS), bf16),
            dma((2,)),
            pltpu.VMEM((NH, HS), f32),
            pltpu.VMEM((2, KVH, HS), f32),
            pltpu.VMEM((members, 1, cols), f32),
            pltpu.VMEM(out_weight.shape, bf16),
            pltpu.VMEM((ring, 4, block, chunk), bf16),
            pltpu.VMEM((MSPLIT, RESIDENT, narrow, block), bf16),
            pltpu.VMEM((NH + PAD, HS), bf16),
            pltpu.VMEM((members, NH + PAD, HS), bf16),
            pltpu.VMEM((members * (NH + PAD), HS), f32),
            pltpu.VMEM((batch, NH * HS), bf16),
            pltpu.VMEM((members, 1, cols), f32),
            pltpu.VMEM((hsplit, batch, cols), f32),
            pltpu.VMEM((batch, cols), f32),
            pltpu.VMEM((1, lanes), f32),
            pltpu.VMEM((members, 1, lanes), f32),
            pltpu.VMEM((batch, block), bf16),
            pltpu.VMEM((4, lead, block), bf16),
            pltpu.VMEM((packed + 8, chunk), f32),
            pltpu.VMEM((MSPLIT, packed, narrow), bf16),
            pltpu.VMEM((MSPLIT, packed, narrow), bf16),
            pltpu.VMEM((hid_rows, narrow), bf16),
            pltpu.VMEM((MSPLIT, hid_rows, narrow), bf16),
            pltpu.VMEM((RESIDENT, hid_rows, block), f32),
            pltpu.VMEM((batch, block), f32),
            pltpu.VMEM((members, 1, block), f32),
            pltpu.VMEM((members, 1, block), f32),
            dma,
            dma((ring, 4)),
            dma((MSPLIT, RESIDENT)),
        ]
        + [dma((MSPLIT,)), dma((MSPLIT, hsplit))]
        + [dma((members,))] * 5
        + [dma((hsplit,))] * 2
        + [dma((MSPLIT,))] * 5
        + [dma((members,))] * 2,
        compiler_params=pltpu.CompilerParams(
            collective_id=0, has_side_effects=True, vmem_limit_bytes=67043328
        ),
    )(
        query,
        key_new,
        value_new,
        key_cache.reshape(rows, KVH * HS),
        value_cache.reshape(rows, KVH * HS),
        lengths,
        route_ids,
        route_scores,
        stream_in,
        norm_gain.reshape(MSPLIT, 1, block),
        out_weight,
        gate_weight,
        up_weight,
        down_weight,
    )


def solution(mesh):
    return jax.shard_map(
        on_device,
        mesh=mesh,
        in_specs=(
            P(("groups", "gx"), None),
            P(("groups", "gx"), None),
            P(("groups", "gx"), None),
            P(("groups", "gx"), None),
            P(("groups", "gx"), None, None),
            P(("groups", "gx"), None, None),
            P(("groups", "gx")),
            P(("groups", "gx"), None),
            P(("groups", "gx"), None),
            P(None, "gx"),
            P(),
            P(None, "gx", None),
            P(None, "gx", None),
            P(None, "gx", None),
        ),
        out_specs=P(("groups", "gx"), None),
        check_vma=False,
    )
```

```python
import functools

import jax
import jax.numpy as jnp
from jax import lax
from jax.experimental import pallas as pl
from jax.experimental.pallas import tpu as pltpu
from jax.sharding import PartitionSpec as P

NH = 64
KVH = 8
HS = 128
RESIDENT = 2
MSPLIT = 8
PAD = 16
RING = 3
ORDER = (0, 2, 1, 3)
MESH = pl.DeviceIdType.MESH

SLOTS = 28
STAGES = ((0, 0), (0, 1), (1, 0), (1, 1))
RELAYED = (True, False)
SPREAD = (0, 2, 6, 4, 1, 3, 7, 5)

def large_kernel(
    members,
    query_hbm,
    key_new_hbm,
    value_new_hbm,
    key_hbm,
    value_hbm,
    lengths_hbm,
    ids_hbm,
    scores_hbm,
    stream_hbm,
    gain_hbm,
    out_weight,
    gate_weight,
    up_weight,
    down_weight,
    out,
    lengths,
    route_ids,
    route_scores,
    query,
    key_new,
    value_new,
    stream,
    gain,
    key_cache,
    value_cache,
    in_sem,
    heads,
    own_rows,
    stream_rows,
    stream_recv,
    stream_flat,
    pool,
    attn_send,
    attn_recv,
    attn_wide,
    attn_rows,
    resid_keep,
    y_send,
    y_recv,
    sq_send,
    sq_recv,
    slots_in,
    acc_a,
    acc_b,
    px_send_a,
    px_send_b,
    px_recv_a,
    px_recv_b,
    pz_send_a,
    pz_send_b,
    pz_recv_a,
    pz_recv_b,
    hid_send_a,
    hid_send_b,
    hid_recv_a,
    hid_recv_b,
    total,
    final_flat,
    final_send,
    final_recv,
    wo_sem,
    gu_sem,
    down_sem,
    a_send,
    a_relay,
    a_recv,
    s_send,
    s_recv,
    q_send,
    q_recv,
    r_send,
    r_recv,
    x_send,
    x_recv,
    z_send,
    z_recv,
    h_send,
    h_relay,
    h_recv,
    f_send,
    f_recv,
):
    f32, bf16 = jnp.float32, jnp.bfloat16
    hsplit = members // MSPLIT
    me = lax.axis_index("gx")
    m = me // hsplit
    h = lax.rem(me, hsplit)
    batch = members
    cols = y_send.shape[1]
    width = cols * members
    block = width // MSPLIT
    group = NH // KVH
    acc, px_send, px_recv = (acc_a, acc_b), (px_send_a, px_send_b), (px_recv_a, px_recv_b)
    pz_send, pz_recv = (pz_send_a, pz_send_b), (pz_recv_a, pz_recv_b)
    hid_send, hid_recv = (hid_send_a, hid_send_b), (hid_recv_a, hid_recv_b)
    wide = (acc_a.shape[2], acc_b.shape[2])
    first = (0, wide[0])
    chunk = wide[0] + wide[1]
    cap = batch * 5 // 8
    packed = px_send_a.shape[1]
    hid_rows = hid_send_a.shape[0]
    lead = slots_in.shape[1] // 2
    lanes = sq_send.shape[1]
    half = MSPLIT // 2
    side = block // cols
    pieces = NH * HS // block

    def peer(d):
        return lax.rem(me + d, members)

    def model(d):
        d = jnp.asarray(d, jnp.int32)
        to = 0
        for b in (1, 2, 4):
            to = to + lax.rem(lax.div(m, b) + lax.div(d, b), 2) * b
        return to

    def mate(d):
        return lax.rem(h + d, hsplit)

    def remote(src, dst, send, recv, device):
        return pltpu.make_async_remote_copy(
            src_ref=src,
            dst_ref=dst,
            send_sem=send,
            recv_sem=recv,
            device_id={"gx": device},
            device_id_type=MESH,
        )

    barrier = pltpu.get_barrier_semaphore()
    inputs = [
        pltpu.make_async_copy(src, dst, in_sem.at[k])
        for k, (src, dst) in enumerate(
            (
                (query_hbm, query),
                (key_hbm, key_cache),
                (value_hbm, value_cache),
                (key_new_hbm, key_new),
                (value_new_hbm, value_new),
                (lengths_hbm, lengths),
                (ids_hbm, route_ids),
                (scores_hbm, route_scores),
                (stream_hbm, stream),
                (gain_hbm.at[me], gain),
            )
        )
    ]
    for copy in inputs:
        copy.start()

    @pl.loop(1, members)
    def _(d):
        pl.semaphore_signal(barrier, inc=1, device_id={"gx": peer(d)}, device_id_type=MESH)

    def wo_copy(k):
        return pltpu.make_async_copy(
            out_weight.at[pl.ds(k * block, block), :],
            pool.at[k // side, :, pl.ds(k % side * cols, cols)],
            wo_sem.at[k],
        )

    def gu_slot(p, z, i, r):
        return lax.rem(half + MSPLIT * STAGES.index((p, z)) + 2 * i + r, SLOTS)

    def gu_copy(p, z, i, q):
        r, w = q // 2, (gate_weight, up_weight)[q % 2]
        at = pl.multiple_of(model(2 * (half - 1 - i) + 1 - z) * chunk + first[p], 128)
        return pltpu.make_async_copy(
            w.at[r, :, pl.ds(at, wide[p])],
            pool.at[gu_slot(p, z, i, r), :, pl.ds(q % 2 * wide[p], wide[p])],
            gu_sem.at[p, z * half + i, q],
        )

    def gu_start(s, i):
        for q in range(4):
            gu_copy(*STAGES[s], i, q).start()

    def down_order(k):
        if isinstance(k, int):
            return SPREAD[k]
        d = 0
        for j, to in enumerate(SPREAD):
            d = d + jnp.where(k == j, to, 0)
        return d

    def down_slot(p, k):
        return lax.rem(half + (4 + p) * MSPLIT + k, SLOTS)

    def down_copy(p, k, r):
        at = pl.multiple_of(model(down_order(k)) * chunk + first[p], 16)
        return pltpu.make_async_copy(
            down_weight.at[r, pl.ds(at, wide[p]), :],
            pool.at[down_slot(p, k), pl.ds(r * wide[p], wide[p]), :],
            down_sem.at[p, k, r],
        )

    def down_start(p, k):
        for j in range(2):
            for r in range(RESIDENT):
                down_copy(p, k + j, r).start()

    def refill(p, z, i):
        s = STAGES.index((p, z))
        cases = (
            (lambda: gu_start(3, i + 2), lambda: down_start(0, 2 * i - 4)),
            (lambda: down_start(0, 2 * i + 4), lambda: down_start(1, 2 * i - 4)),
            (lambda: down_start(1, 2 * i + 4),),
            (),
        )
        for test, load in zip((i < 2, i >= 2), cases[s]):
            pl.when(test)(load)

    for k in range(pieces):
        wo_copy(k).start()

    scale = HS ** (-0.5)
    inputs[0].wait()
    for n in range(NH):
        heads[n : n + 1, :] = query[:, n * HS : (n + 1) * HS].astype(f32)

    for copy in inputs[1:]:
        copy.wait()

    for g in range(KVH):
        own_rows[0, g : g + 1, :] = key_new[:, g * HS : (g + 1) * HS].astype(f32)
        own_rows[1, g : g + 1, :] = value_new[:, g * HS : (g + 1) * HS].astype(f32)
    wide_q = heads[...]
    s = jnp.concatenate(
        [
            lax.dot_general(
                wide_q[g * group : (g + 1) * group].astype(bf16),
                key_cache[:, g * HS : (g + 1) * HS],
                (((1,), (1,)), ((), ())),
                preferred_element_type=f32,
            )
            for g in range(KVH)
        ],
        axis=0,
    )
    s = s * scale
    live = lax.broadcasted_iota(jnp.int32, s.shape, 1) < lengths[0]
    s = jnp.where(live, s, -1e30)
    k_own, v_own = own_rows[0], own_rows[1]
    spread = lambda v: jnp.concatenate(
        [jnp.broadcast_to(v[g : g + 1], (group, HS)) for g in range(KVH)], axis=0
    )
    own = jnp.sum(wide_q * spread(k_own), axis=-1, keepdims=True) * scale
    top = jnp.maximum(jnp.max(s, axis=-1, keepdims=True), own)
    e_cache = jnp.exp(s - top)
    e_own = jnp.exp(own - top)
    norm = jnp.sum(e_cache, axis=-1, keepdims=True) + e_own
    p = e_cache / norm
    p_own = (e_own / norm).astype(bf16).astype(f32)
    mixed = jnp.concatenate(
        [
            jnp.dot(
                p[g * group : (g + 1) * group].astype(bf16),
                value_cache[:, g * HS : (g + 1) * HS],
                preferred_element_type=f32,
            )
            for g in range(KVH)
        ],
        axis=0,
    )
    mixed = mixed + p_own * spread(v_own)
    attn_send[...] = mixed.astype(bf16)
    spot = lax.broadcasted_iota(jnp.int32, (1, HS), 1)
    full = lambda v: jnp.full((1, HS), v)
    s0, s1 = full(route_scores[0, 0]), full(route_scores[0, 1])
    i0, i1 = full(route_ids[0, 0]), full(route_ids[0, 1])
    peak = jnp.maximum(s0, s1)
    x0, x1 = jnp.exp(s0 - peak), jnp.exp(s1 - peak)
    pick = jnp.where(i0 == spot, x0 / (x0 + x1), 0.0) + jnp.where(i1 == spot, x1 / (x0 + x1), 0.0)
    pick = pick.astype(bf16).astype(f32)
    for j in range(members):
        stream_rows[j, :, :cols] = stream[:, j * cols : (j + 1) * cols].astype(f32)
        stream_rows[j, :, cols:] = pick

    pl.semaphore_wait(barrier, members - 1)

    def attn_copy(d, slot):
        return remote(
            attn_send, attn_recv.at[slot], a_send.at[d], a_recv.at[slot], model(d) * hsplit + h
        )

    def attn_relay(d, t, slot):
        src = attn_send if isinstance(d, int) else attn_recv.at[slot]
        return remote(
            src, attn_recv.at[slot], a_relay.at[d, t], a_recv.at[slot], m * hsplit + t
        )

    def stream_copy(to, slot):
        return remote(
            stream_rows.at[to], stream_recv.at[slot], s_send.at[to], s_recv.at[slot], to
        )

    @pl.loop(0, MSPLIT - 1)
    def _(i):
        attn_copy(MSPLIT - 1 - i, me).start()

    @pl.loop(1, hsplit)
    def _(d):
        attn_relay(0, mate(d), me).start()

    @pl.loop(1, members)
    def _(d):
        stream_copy(peer(d), me).start()

    def widen(slot, rows):
        at = pl.multiple_of(slot * NH, NH)
        attn_wide[pl.ds(at, NH), :] = rows.astype(f32)

    for s in range(3):

        @pl.loop(0, half)
        def _(i):
            gu_start(s, i)

    widen(me, attn_send[...])
    stream_recv[me] = stream_rows[me]

    @pl.loop(1, MSPLIT)
    def _(i):
        slot = model(i) * hsplit + h
        attn_copy(i, slot).wait_recv()

        @pl.loop(1, hsplit)
        def _(d):
            attn_relay(i, mate(d), slot).start()

        widen(slot, attn_recv[slot])

    @pl.loop(0, MSPLIT)
    def _(i):
        @pl.loop(1, hsplit)
        def _(d):
            slot = model(i) * hsplit + mate(d)
            attn_copy(i, slot).wait_recv()
            widen(slot, attn_recv[slot])

    for k in range(pieces):
        wo_copy(k).wait()

    @pl.loop(1, members)
    def _(d):
        stream_copy(me, peer(d)).wait_recv()

    for j in range(members):
        stream_flat[j : j + 1, :] = stream_recv[j]

    for n in range(NH):
        attn_rows[:, n * HS : (n + 1) * HS] = attn_wide[pl.ds(n, batch, stride=NH), :].astype(bf16)

    proj = jnp.zeros((batch, cols), f32)
    for k in range(pieces):
        proj = proj + jnp.dot(
            attn_rows[:, k * block : (k + 1) * block],
            pool[k // side, :, k % side * cols : (k % side + 1) * cols],
            preferred_element_type=f32,
        )
    gu_start(3, 0)
    gu_start(3, 1)

    resid = stream_flat[:, :cols] + proj.astype(bf16).astype(f32)
    resid_keep[...] = resid
    y_send[...] = (resid * gain[...]).astype(bf16)

    def y_copy(to, slot):
        return remote(y_send, y_recv.at[slot], r_send.at[to], r_recv.at[slot], m * hsplit + to)

    @pl.loop(1, hsplit)
    def _(d):
        y_copy(mate(d), h).start()

    sub_w = lax.broadcasted_iota(jnp.int32, (batch, lanes), 0)
    lane_w = lax.broadcasted_iota(jnp.int32, (batch, lanes), 1)
    squares = jnp.sum(resid * resid, axis=-1, keepdims=True)
    sq_send[...] = jnp.sum(jnp.where(sub_w == lane_w, squares, 0.0), axis=0, keepdims=True)

    def sq_copy(to, slot):
        return remote(sq_send, sq_recv.at[slot], q_send.at[to], q_recv.at[slot], to)

    @pl.loop(1, members)
    def _(d):
        sq_copy(peer(d), me).start()

    sq_recv[me] = sq_send[...]
    y_recv[h] = y_send[...]
    scales = [stream_flat[:, cols + r : cols + r + 1] for r in range(RESIDENT)]
    sub = lax.broadcasted_iota(jnp.int32, (batch, batch), 0)
    lane = lax.broadcasted_iota(jnp.int32, (batch, batch), 1)
    named, rank, back = [], [], []
    for r in range(RESIDENT):
        col = jnp.where(scales[r] > 0.0, 1.0, 0.0)
        row = jnp.sum(jnp.where(sub == lane, col, 0.0), axis=0, keepdims=True)
        named.append(row)
        rank.append(jnp.sum(jnp.where(sub < lane, col, 0.0), axis=0, keepdims=True))
        place = jnp.sum(jnp.where(lane < sub, row, 0.0), axis=1, keepdims=True)
        at = lax.broadcasted_iota(jnp.int32, (batch, hid_rows), 1)
        hit = at == place.astype(jnp.int32) + r * cap
        back.append(jnp.where(hit, scales[r], 0.0))

    @pl.loop(1, hsplit)
    def _(d):
        y_copy(h, mate(d)).wait_recv()

    y = jnp.concatenate([y_recv[j] for j in range(hsplit)], axis=1)
    bases = [q * cap // 8 * 8 for q in range(4)]
    for q in range(4):
        r = q % 2
        shift = q * cap - bases[q]
        at = lax.broadcasted_iota(jnp.int32, (lead, batch), 0)
        hit = (at == rank[r].astype(jnp.int32) + shift) & (named[r] > 0.0)
        slots_in[r, q // 2 * lead : (q // 2 + 1) * lead, :] = jnp.dot(
            jnp.where(hit, 1.0, 0.0).astype(bf16), y, preferred_element_type=f32
        ).astype(bf16)

    def px_copy(p, i):
        return remote(
            px_send[p].at[i],
            px_recv[p].at[i],
            x_send.at[p, i],
            x_recv.at[p, i],
            model(1) * hsplit + h,
        )

    def pz_copy(p, j):
        return remote(
            pz_send[p].at[j],
            pz_recv[p].at[j],
            z_send.at[p, j],
            z_recv.at[p, j],
            model(2 * (half - 1 - j)) * hsplit + h,
        )

    def sums(p, z, i):
        w = wide[p]
        slabs = [[] for _ in range(acc[p].shape[1] // 8)]
        for r in range(RESIDENT):
            where = gu_slot(p, z, i, r)
            values = [
                jnp.dot(
                    slots_in[r, q * lead : (q + 1) * lead, :],
                    pool[where, :, q * w : (q + 1) * w],
                    preferred_element_type=f32,
                )
                for q in range(2)
            ]
            for q in range(2):
                for k in range(lead // 8):
                    slabs[bases[2 * q + r] // 8 + k].append(values[q][k * 8 : (k + 1) * 8])
        empty = jnp.zeros((8, w), f32)
        return jnp.concatenate([sum(slab[1:], slab[0]) if slab else empty for slab in slabs], axis=0)

    def arrived(p, z, i):
        for q in range(4):
            gu_copy(p, z, i, q).wait()

    def gu_x(p, pair):
        @pl.loop(0, half, step=pair)
        def _(i):
            for j in range(pair):
                arrived(p, 0, i + j)
            for j in range(pair):
                px_send[p][i + j] = sums(p, 0, i + j)[:packed].astype(bf16)
            for j in range(pair):
                px_copy(p, i + j).start()
            for j in range(pair):
                refill(p, 0, i + j)

    def gu_z(p, pair):
        @pl.loop(0, half, step=pair)
        def _(i):
            for j in range(pair):
                arrived(p, 1, i + j)
            for j in range(pair):
                acc[p][j] = sums(p, 1, i + j)
            for j in range(pair):
                refill(p, 1, i + j)
                px_copy(p, i + j).wait_recv()
                acc[p][j, :packed, :] += px_recv[p][i + j].astype(f32)

                @pl.when(i + j < half - 1)
                def _():
                    pz_send[p][i + j] = acc[p][j, :packed, :].astype(bf16)
                    pz_copy(p, i + j).start()

    def hid_copy(p, d, slot):
        return remote(
            hid_send[p],
            hid_recv[p].at[slot],
            h_send.at[p, d],
            h_recv.at[p, slot],
            model(d) * hsplit + h,
        )

    def hid_relay(p, j, slot):
        return remote(
            hid_recv[p].at[slot],
            hid_recv[p].at[slot],
            h_relay.at[p, j],
            h_recv.at[p, slot],
            model(1) * hsplit + h,
        )

    def finish(p, last):
        for j in range(half - 1):
            pz_copy(p, j).wait_recv()
            acc[p][last, :packed, :] += pz_recv[p][j].astype(f32)
        a = acc[p][last, :hid_rows, :] * scaled
        b = acc[p][last, 2 * cap : 2 * cap + hid_rows, :] * scaled
        hid_send[p][...] = (a / (1.0 + jnp.exp(-a)) * b).astype(bf16)
        for d in (1, *SPREAD[1:half]) if RELAYED[p] else range(MSPLIT - 1, 0, -1):
            hid_copy(p, d, m).start()
        hid_recv[p][m] = hid_send[p][...]

    def relays(p):
        for k in range(1, half):
            slot = model(SPREAD[k])
            hid_copy(p, SPREAD[k], slot).wait_recv()
            hid_relay(p, k, slot).start()

    def down(p, ks, fresh=False):
        for k in ks:
            if k >= half or k and not RELAYED[p]:
                hid_copy(p, SPREAD[k], model(SPREAD[k])).wait_recv()
            for r in range(RESIDENT):
                down_copy(p, k, r).wait()
        line = lax.broadcasted_iota(jnp.int32, (hid_rows, wide[p]), 0)
        value = None if fresh else total[...]
        for k in ks:
            rows = hid_recv[p][model(SPREAD[k])].astype(f32)
            split = [
                jnp.where((line >= r * cap) & (line < (r + 1) * cap), rows, 0.0).astype(bf16)
                for r in range(RESIDENT)
            ]
            term = jnp.dot(
                jnp.concatenate(split, axis=1),
                pool[down_slot(p, k), : RESIDENT * wide[p], :],
                preferred_element_type=f32,
            )
            value = term if value is None else value + term
        total[...] = value

    gu_x(0, 1)

    gu_z(0, 2)

    gu_x(1, 2)

    @pl.loop(1, members)
    def _(d):
        sq_copy(me, peer(d)).wait_recv()

    power = jnp.sum(sq_recv[...], axis=0)[:, :batch] * (1.0 / width)
    inverse = lax.rsqrt(power + 1e-05)
    at = lax.broadcasted_iota(jnp.int32, (hid_rows, batch), 0)
    scaled = jnp.zeros((hid_rows, 1), f32)
    for r in range(RESIDENT):
        hit = (at == rank[r].astype(jnp.int32) + r * cap) & (named[r] > 0.0)
        scaled = scaled + jnp.sum(jnp.where(hit, inverse, 0.0), axis=1, keepdims=True)

    finish(0, 1)

    gu_z(1, 1)

    relays(0)

    down(0, range(half), True)

    finish(1, 0)

    down(0, range(half, MSPLIT))

    down(1, range(half))

    down(1, (4, 5))

    down(1, (6, 7))

    resid = resid_keep[...]
    whole = jnp.concatenate([jnp.where(h == j, resid, 0.0) for j in range(hsplit)], axis=1)
    mix = sum(back[1:], back[0])
    for n in range(RESIDENT * cap):
        whole = whole + mix[:, n : n + 1] * total[n : n + 1, :]
    tiles = block // HS
    for t in range(tiles):
        final_flat[t * batch : (t + 1) * batch, :] = whole[:, t * HS : (t + 1) * HS]
    for j in range(members):
        final_send[j] = final_flat[pl.ds(j, tiles, stride=batch), :].astype(bf16)

    def final_copy(to, slot):
        return remote(
            final_send.at[to], final_recv.at[slot], f_send.at[to], f_recv.at[slot], to
        )

    @pl.loop(1, members)
    def _(d):
        final_copy(peer(d), me).start()

    final_recv[me] = final_send[me]

    @pl.loop(1, members)
    def _(d):
        to = peer(d)
        stream_copy(to, me).wait_send()
        sq_copy(to, me).wait_send()

    @pl.loop(1, hsplit)
    def _(d):
        y_copy(mate(d), h).wait_send()

    @pl.loop(0, MSPLIT)
    def _(i):
        @pl.loop(1, hsplit)
        def _(d):
            attn_relay(i, mate(d), me).wait_send()

    @pl.loop(1, MSPLIT)
    def _(d):
        attn_copy(d, me).wait_send()

    for p in range(2):
        for i in range(half):
            px_copy(p, i).wait_send()
        for j in range(half - 1):
            pz_copy(p, j).wait_send()
        for d in (1, *SPREAD[1:half]) if RELAYED[p] else range(1, MSPLIT):
            hid_copy(p, d, m).wait_send()
        for j in range(1, half if RELAYED[p] else 1):
            hid_relay(p, j, m).wait_send()

    @pl.loop(1, members)
    def _(d):
        final_copy(me, peer(d)).wait_recv()

    for j in range(MSPLIT):
        line = final_recv[j * hsplit].astype(f32)
        for k in range(1, hsplit):
            line = line + final_recv[j * hsplit + k].astype(f32)
        out[j * tiles : (j + 1) * tiles, :] = line.astype(bf16)

    @pl.loop(1, members)
    def _(d):
        final_copy(peer(d), me).wait_send()

def large_call(
    stream_in,
    query,
    key_new,
    value_new,
    key_cache,
    value_cache,
    lengths,
    route_ids,
    route_scores,
    out_weight,
    norm_gain,
    gate_weight,
    up_weight,
    down_weight,
):
    f32, bf16 = jnp.float32, jnp.bfloat16
    members = lax.axis_size("gx")
    width = stream_in.shape[1]
    hsplit = members // MSPLIT
    cols = width // members
    block = width // MSPLIT
    batch = members
    narrow = gate_weight.shape[2] // MSPLIT
    vmem = pl.BlockSpec(memory_space=pltpu.VMEM)
    hbm = pl.BlockSpec(memory_space=pl.ANY)
    dma = pltpu.SemaphoreType.DMA
    rows = key_cache.shape[1]
    cap = batch * 5 // 8
    packed = 2 * RESIDENT * cap
    shifts = [q * cap % 8 for q in range(4)]
    lead = (cap + max(shifts) + 7) // 8 * 8
    hid_rows = (RESIDENT * cap + 7) // 8 * 8
    lanes = (batch + 127) // 128 * 128
    half = MSPLIT // 2
    tiles = block // HS
    wide = [(narrow // 128 + 1) // 2 * 128]
    wide.append(narrow - wide[0])
    result = pl.pallas_call(
        functools.partial(large_kernel, members),
        out_shape=pltpu.VMEM((width // HS, HS), bf16),
        in_specs=[hbm] * 14,
        out_specs=vmem,
        scratch_shapes=[
            pltpu.SMEM(lengths.shape, jnp.int32),
            pltpu.SMEM(route_ids.shape, jnp.int32),
            pltpu.SMEM(route_scores.shape, f32),
            pltpu.VMEM((1, NH * HS), bf16),
            pltpu.VMEM((1, KVH * HS), bf16),
            pltpu.VMEM((1, KVH * HS), bf16),
            pltpu.VMEM((1, width), bf16),
            pltpu.VMEM((1, cols), f32),
            pltpu.VMEM((rows, KVH * HS), bf16),
            pltpu.VMEM((rows, KVH * HS), bf16),
            dma((10,)),
            pltpu.VMEM((NH, HS), f32),
            pltpu.VMEM((2, KVH, HS), f32),
            pltpu.VMEM((members, 1, cols + HS), f32),
            pltpu.VMEM((members, 1, cols + HS), f32),
            pltpu.VMEM((batch, cols + HS), f32),
            pltpu.VMEM((SLOTS, block, block), bf16),
            pltpu.VMEM((NH, HS), bf16),
            pltpu.VMEM((members, NH, HS), bf16),
            pltpu.VMEM((members * NH, HS), f32),
            pltpu.VMEM((batch, NH * HS), bf16),
            pltpu.VMEM((batch, cols), f32),
            pltpu.VMEM((batch, cols), bf16),
            pltpu.VMEM((hsplit, batch, cols), bf16),
            pltpu.VMEM((1, lanes), f32),
            pltpu.VMEM((members, 1, lanes), f32),
            pltpu.VMEM((RESIDENT, 2 * lead, block), bf16),
            *[pltpu.VMEM((2, packed + 8, w), f32) for w in wide],
            *[pltpu.VMEM((half, packed, w), bf16) for w in wide],
            *[pltpu.VMEM((half, packed, w), bf16) for w in wide],
            *[pltpu.VMEM((half - 1, packed, w), bf16) for w in wide],
            *[pltpu.VMEM((half - 1, packed, w), bf16) for w in wide],
            *[pltpu.VMEM((hid_rows, w), bf16) for w in wide],
            *[pltpu.VMEM((MSPLIT, hid_rows, w), bf16) for w in wide],
            pltpu.VMEM((hid_rows, block), f32),
            pltpu.VMEM((tiles * batch, HS), f32),
            pltpu.VMEM((members, tiles, HS), bf16),
            pltpu.VMEM((members, tiles, HS), bf16),
            dma((NH * HS // block,)),
            dma((2, MSPLIT, 4)),
            dma((2, MSPLIT, RESIDENT)),
        ]
        + [dma((MSPLIT,)), dma((MSPLIT, hsplit))]
        + [dma((members,))] * 5
        + [dma((hsplit,))] * 2
        + [dma((2, half))] * 4
        + [dma((2, MSPLIT)), dma((2, half)), dma((2, MSPLIT))]
        + [dma((members,))] * 2,
        compiler_params=pltpu.CompilerParams(
            collective_id=0, has_side_effects=True, vmem_limit_bytes=66000000
        ),
    )(
        query,
        key_new,
        value_new,
        key_cache.reshape(rows, KVH * HS),
        value_cache.reshape(rows, KVH * HS),
        lengths,
        route_ids,
        route_scores,
        stream_in,
        norm_gain.reshape(members, 1, cols),
        out_weight,
        gate_weight,
        up_weight,
        down_weight,
    )
    return result.reshape(1, width)

def small_kernel(
    members,
    query,
    key_new,
    value_new,
    key_hbm,
    value_hbm,
    lengths,
    route_ids,
    route_scores,
    stream,
    gain,
    out_weight,
    gate_weight,
    up_weight,
    down_weight,
    out,
    key_cache,
    value_cache,
    cache_sem,
    heads,
    own_rows,
    stream_rows,
    wo,
    gu,
    down,
    attn_send,
    attn_recv,
    attn_wide,
    attn_rows,
    stream_recv,
    resid_recv,
    resid_send,
    sq_send,
    sq_recv,
    normed,
    slots_in,
    acc,
    part_send,
    part_recv,
    hid_send,
    hid_recv,
    total,
    resid_full,
    final_send,
    final_recv,
    wo_sem,
    gu_sem,
    down_sem,
    a_send,
    a_relay,
    a_recv,
    s_send,
    s_recv,
    q_send,
    q_recv,
    r_send,
    r_recv,
    p_send,
    p_recv,
    h_send,
    h_relay,
    h_recv,
    f_send,
    f_recv,
):
    f32, bf16 = jnp.float32, jnp.bfloat16
    hsplit = members // MSPLIT
    me = lax.axis_index("gx")
    m = me // hsplit
    h = lax.rem(me, hsplit)
    batch = members
    cols = wo.shape[1]
    width = cols * members
    block = width // MSPLIT
    group = NH // KVH
    chunk = gu.shape[3]
    chunks = gate_weight.shape[2] // chunk
    narrow = part_send.shape[2]
    cap = batch * 5 // 8
    packed = part_send.shape[1]
    hid_rows = hid_send.shape[0]
    lead = slots_in.shape[1]
    lanes = sq_send.shape[1]
    ring = gu.shape[0]

    def peer(d):
        return lax.rem(me + d, members)

    def model(d):
        d = jnp.asarray(d, jnp.int32)
        to = 0
        for b in (1, 2, 4):
            to = to + lax.rem(lax.div(m, b) + lax.div(d, b), 2) * b
        return to

    def mate(d):
        return lax.rem(h + d, hsplit)

    def remote(src, dst, send, recv, device):
        return pltpu.make_async_remote_copy(
            src_ref=src,
            dst_ref=dst,
            send_sem=send,
            recv_sem=recv,
            device_id={"gx": device},
            device_id_type=MESH,
        )

    barrier = pltpu.get_barrier_semaphore()

    @pl.loop(1, members)
    def _(d):
        pl.semaphore_signal(barrier, inc=1, device_id={"gx": peer(d)}, device_id_type=MESH)

    key_copy = pltpu.make_async_copy(key_hbm, key_cache, cache_sem.at[0])
    value_copy = pltpu.make_async_copy(value_hbm, value_cache, cache_sem.at[1])
    key_copy.start()
    value_copy.start()
    wo_copy = pltpu.make_async_copy(out_weight, wo, wo_sem)
    wo_copy.start()

    def gu_copy(i, q):
        r, w = q // 2, (gate_weight, up_weight)[q % 2]
        if chunks == 1:
            src = w.at[r]
        else:
            at = pl.multiple_of(model(MSPLIT - 1 - i) * chunk, 128)
            src = w.at[r, :, pl.ds(at, chunk)]
        slot = lax.rem(i, ring)
        return pltpu.make_async_copy(src, gu.at[slot, q], gu_sem.at[slot, q])

    def down_copy(i, r):
        at = pl.multiple_of(model(i) * narrow, 16)
        return pltpu.make_async_copy(
            down_weight.at[r, pl.ds(at, narrow), :], down.at[i, r], down_sem.at[i, r]
        )

    @pl.loop(0, ring)
    def _(i):
        for q in range(4):
            gu_copy(i, q).start()

    @pl.loop(0, MSPLIT)
    def _(i):
        for r in range(RESIDENT):
            down_copy(i, r).start()

    scale = HS ** (-0.5)
    for n in range(NH):
        heads[n : n + 1, :] = query[:, n * HS : (n + 1) * HS].astype(f32)
    for g in range(KVH):
        own_rows[0, g : g + 1, :] = key_new[:, g * HS : (g + 1) * HS].astype(f32)
        own_rows[1, g : g + 1, :] = value_new[:, g * HS : (g + 1) * HS].astype(f32)
    for j in range(members):
        stream_rows[j] = stream[:, j * cols : (j + 1) * cols].astype(f32)
    wide_q = heads[...]
    key_copy.wait()
    value_copy.wait()
    s = jnp.concatenate(
        [
            lax.dot_general(
                wide_q[g * group : (g + 1) * group].astype(bf16),
                key_cache[:, g * HS : (g + 1) * HS],
                (((1,), (1,)), ((), ())),
                preferred_element_type=f32,
            )
            for g in range(KVH)
        ],
        axis=0,
    )
    s = s * scale
    live = lax.broadcasted_iota(jnp.int32, s.shape, 1) < lengths[0]
    s = jnp.where(live, s, -1e30)
    k_own, v_own = own_rows[0], own_rows[1]
    spread = lambda v: jnp.concatenate(
        [jnp.broadcast_to(v[g : g + 1], (group, HS)) for g in range(KVH)], axis=0
    )
    own = jnp.sum(wide_q * spread(k_own), axis=-1, keepdims=True) * scale
    top = jnp.maximum(jnp.max(s, axis=-1, keepdims=True), own)
    e_cache = jnp.exp(s - top)
    e_own = jnp.exp(own - top)
    norm = jnp.sum(e_cache, axis=-1, keepdims=True) + e_own
    p = e_cache / norm
    p_own = (e_own / norm).astype(bf16).astype(f32)
    mixed = jnp.concatenate(
        [
            jnp.dot(
                p[g * group : (g + 1) * group].astype(bf16),
                value_cache[:, g * HS : (g + 1) * HS],
                preferred_element_type=f32,
            )
            for g in range(KVH)
        ],
        axis=0,
    )
    mixed = mixed + p_own * spread(v_own)
    attn_send[:NH, :] = mixed.astype(bf16)
    full = lambda v: jnp.full((PAD, HS), v)
    s0, s1 = full(route_scores[0, 0]), full(route_scores[0, 1])
    i0, i1 = full(route_ids[0, 0]), full(route_ids[0, 1])
    peak = jnp.maximum(s0, s1)
    x0, x1 = jnp.exp(s0 - peak), jnp.exp(s1 - peak)
    row = lax.broadcasted_iota(jnp.int32, (PAD, HS), 0)
    pick = jnp.where(i0 == row, x0 / (x0 + x1), 0.0) + jnp.where(i1 == row, x1 / (x0 + x1), 0.0)
    attn_send[NH:, :] = pick.astype(bf16)

    pl.semaphore_wait(barrier, members - 1)

    def attn_copy(d, slot):
        return remote(
            attn_send, attn_recv.at[slot], a_send.at[d], a_recv.at[slot], model(d) * hsplit + h
        )

    def attn_relay(d, t, slot):
        src = attn_send if isinstance(d, int) else attn_recv.at[slot]
        return remote(
            src, attn_recv.at[slot], a_relay.at[d, t], a_recv.at[slot], m * hsplit + t
        )

    def stream_copy(to, slot):
        return remote(
            stream_rows.at[to], stream_recv.at[slot], s_send.at[to], s_recv.at[slot], to
        )

    @pl.loop(0, MSPLIT - 1)
    def _(i):
        attn_copy(MSPLIT - 1 - i, me).start()

    @pl.loop(1, hsplit)
    def _(d):
        attn_relay(0, mate(d), me).start()

    @pl.loop(1, members)
    def _(d):
        stream_copy(peer(d), me).start()

    attn_recv[me] = attn_send[...]
    stream_recv[me] = stream_rows[me]

    @pl.loop(1, MSPLIT)
    def _(i):
        slot = model(i) * hsplit + h
        attn_copy(i, slot).wait_recv()

        @pl.loop(1, hsplit)
        def _(d):
            attn_relay(i, mate(d), slot).start()

    @pl.loop(0, MSPLIT)
    def _(i):
        @pl.loop(1, hsplit)
        def _(d):
            attn_copy(i, model(i) * hsplit + mate(d)).wait_recv()

    stride = NH + PAD

    @pl.loop(0, members)
    def _(j):
        attn_wide[pl.ds(j * stride, stride), :] = attn_recv[j].astype(f32)

    for n in range(NH):
        attn_rows[:, n * HS : (n + 1) * HS] = attn_wide[pl.ds(n, batch, stride=stride), :].astype(
            bf16
        )
    scales = [attn_wide[pl.ds(NH + r, batch, stride=stride), :][:, :1] for r in range(RESIDENT)]

    sub = lax.broadcasted_iota(jnp.int32, (batch, batch), 0)
    lane = lax.broadcasted_iota(jnp.int32, (batch, batch), 1)
    named, rank, back = [], [], []
    for r in range(RESIDENT):
        col = jnp.where(scales[r] > 0.0, 1.0, 0.0)
        row = jnp.sum(jnp.where(sub == lane, col, 0.0), axis=0, keepdims=True)
        named.append(row)
        rank.append(jnp.sum(jnp.where(sub < lane, col, 0.0), axis=0, keepdims=True))
        place = jnp.sum(jnp.where(lane < sub, row, 0.0), axis=1, keepdims=True)
        at = lax.broadcasted_iota(jnp.int32, (batch, hid_rows), 1)
        hit = at == place.astype(jnp.int32) + r * cap
        back.append(jnp.where(hit, scales[r], 0.0))

    wo_copy.wait()
    proj = jnp.dot(attn_rows[...], wo[...], preferred_element_type=f32).astype(bf16)

    @pl.loop(1, members)
    def _(d):
        stream_copy(me, peer(d)).wait_recv()

    @pl.loop(0, members)
    def _(j):
        resid_send[pl.ds(j, 1), :] = stream_recv[j]

    resid = resid_send[...] + proj.astype(f32)
    resid_send[...] = resid
    sub_w = lax.broadcasted_iota(jnp.int32, (batch, lanes), 0)
    lane_w = lax.broadcasted_iota(jnp.int32, (batch, lanes), 1)
    squares = jnp.sum(resid * resid, axis=-1, keepdims=True)
    sq_send[...] = jnp.sum(jnp.where(sub_w == lane_w, squares, 0.0), axis=0, keepdims=True)

    def sq_copy(to, slot):
        return remote(sq_send, sq_recv.at[slot], q_send.at[to], q_recv.at[slot], to)

    def resid_copy(to, slot):
        return remote(
            resid_send, resid_recv.at[slot], r_send.at[to], r_recv.at[slot], m * hsplit + to
        )

    @pl.loop(1, members)
    def _(d):
        sq_copy(peer(d), me).start()

    @pl.loop(1, hsplit)
    def _(d):
        resid_copy(mate(d), h).start()

    sq_recv[me] = sq_send[...]
    resid_recv[h] = resid_send[...]

    @pl.loop(1, hsplit)
    def _(d):
        resid_copy(h, mate(d)).wait_recv()

    @pl.loop(1, members)
    def _(d):
        sq_copy(me, peer(d)).wait_recv()

    squares = jnp.sum(sq_recv[...], axis=0)
    squares = jnp.sum(jnp.where(sub_w == lane_w, squares, 0.0), axis=1, keepdims=True)
    power = squares * (1.0 / width)
    inverse = lax.rsqrt(power + 1e-05)
    block_resid = jnp.concatenate([resid_recv[j] for j in range(hsplit)], axis=1)
    normed[...] = (block_resid * inverse * gain[m]).astype(bf16)

    bases = [q * cap // 8 * 8 for q in range(4)]
    for q in range(4):
        r = q % 2
        shift = q * cap - bases[q]
        at = lax.broadcasted_iota(jnp.int32, (lead, batch), 0)
        hit = (at == rank[r].astype(jnp.int32) + shift) & (named[r] > 0.0)
        slots_in[q] = jnp.dot(
            jnp.where(hit, 1.0, 0.0).astype(bf16), normed[...], preferred_element_type=f32
        ).astype(bf16)
    acc[...] = jnp.zeros_like(acc)

    def part_copy(to, slot):
        return remote(
            part_send.at[to],
            part_recv.at[slot],
            p_send.at[to],
            p_recv.at[slot],
            to * hsplit + h,
        )

    def gather(slot, q):
        return jnp.dot(
            slots_in[ORDER[q]], gu[slot, q], preferred_element_type=f32
        ), pl.ds(bases[ORDER[q]], lead)

    if chunks == 1:
        for q in range(4):
            gu_copy(0, q).wait()
            value, rows = gather(0, q)
            acc[rows, :] += value
        for to in range(MSPLIT):
            part_send[to] = acc[:packed, to * narrow : (to + 1) * narrow].astype(bf16)

        @pl.loop(1, MSPLIT)
        def _(d):
            part_copy(model(d), m).start()

    else:

        @pl.loop(0, MSPLIT)
        def _(i):
            slot = lax.rem(i, ring)
            to = model(MSPLIT - 1 - i)
            for q in range(4):
                gu_copy(i, q).wait()
                value, rows = gather(slot, q)
                acc[rows, :] += value

                @pl.when(i < MSPLIT - ring)
                def _():
                    gu_copy(i + ring, q).start()

            part_send[to] = acc[:packed, :].astype(bf16)
            acc[...] = jnp.zeros_like(acc)

            @pl.when(i < MSPLIT - 1)
            def _():
                part_copy(to, m).start()

    @pl.loop(1, MSPLIT)
    def _(d):
        part_copy(m, model(d)).wait_recv()

    part_recv[m] = part_send[m]
    acc[:packed, :narrow] = jnp.sum(part_recv[...].astype(f32), axis=0)
    a = acc[:hid_rows, :narrow]
    b = acc[2 * cap : 2 * cap + hid_rows, :narrow]
    hid_send[...] = (a / (1.0 + jnp.exp(-a)) * b).astype(bf16)

    def hid_copy(d, slot):
        return remote(
            hid_send, hid_recv.at[slot], h_send.at[d], h_recv.at[slot], model(d) * hsplit + h
        )

    def hid_relay(j, slot):
        return remote(
            hid_recv.at[slot],
            hid_recv.at[slot],
            h_relay.at[j],
            h_recv.at[slot],
            model(1) * hsplit + h,
        )

    hid_copy(1, m).start()

    @pl.loop(1, MSPLIT // 2)
    def _(j):
        hid_copy(MSPLIT - 2 * j, m).start()

    hid_recv[m] = hid_send[...]
    total[...] = jnp.zeros_like(total)

    def expert_sums(i, slot):
        for r in range(RESIDENT):
            down_copy(i, r).wait()
            total[r] += jnp.dot(hid_recv[slot], down[i, r], preferred_element_type=f32)

    @pl.loop(0, MSPLIT // 2)
    def _(j):
        even, odd = model(2 * j), model(2 * j + 1)

        @pl.when(j > 0)
        def _():
            hid_copy(2 * j, even).wait_recv()
            hid_relay(j, even).start()

        expert_sums(2 * j, even)
        hid_copy(1, odd).wait_recv()
        expert_sums(2 * j + 1, odd)

    whole = jnp.where(h == 0, 1.0, 0.0) * block_resid
    for r in range(RESIDENT):
        if batch > 32:
            whole = whole + jnp.dot(
                back[r], total[r], precision=lax.Precision.HIGHEST, preferred_element_type=f32
            )
        else:
            for n in range(r * cap, (r + 1) * cap):
                whole = whole + back[r][:, n : n + 1] * total[r, n : n + 1, :]
    resid_full[...] = whole

    @pl.loop(0, members)
    def _(j):
        final_send[j] = resid_full[pl.ds(j, 1), :]

    def final_copy(to, slot):
        return remote(
            final_send.at[to], final_recv.at[slot], f_send.at[to], f_recv.at[slot], to
        )

    @pl.loop(1, members)
    def _(d):
        final_copy(peer(d), me).start()

    final_recv[me] = final_send[me]

    @pl.loop(1, members)
    def _(d):
        final_copy(me, peer(d)).wait_recv()

    for j in range(MSPLIT):
        line = final_recv[j * hsplit]
        for k in range(1, hsplit):
            line = line + final_recv[j * hsplit + k]
        out[:, j * block : (j + 1) * block] = line.astype(bf16)

    @pl.loop(1, members)
    def _(d):
        to = peer(d)
        stream_copy(to, me).wait_send()
        sq_copy(to, me).wait_send()
        final_copy(to, me).wait_send()

    @pl.loop(1, hsplit)
    def _(d):
        resid_copy(mate(d), h).wait_send()

    @pl.loop(0, MSPLIT)
    def _(i):
        @pl.loop(1, hsplit)
        def _(d):
            attn_relay(i, mate(d), me).wait_send()

    @pl.loop(1, MSPLIT)
    def _(d):
        attn_copy(d, me).wait_send()
        part_copy(model(d), m).wait_send()

    hid_copy(1, m).wait_send()

    @pl.loop(1, MSPLIT // 2)
    def _(j):
        hid_copy(2 * j, m).wait_send()
        hid_relay(j, m).wait_send()

def on_device(
    stream_in,
    query,
    key_new,
    value_new,
    key_cache,
    value_cache,
    lengths,
    route_ids,
    route_scores,
    out_weight,
    norm_gain,
    gate_weight,
    up_weight,
    down_weight,
):
    f32, bf16 = jnp.float32, jnp.bfloat16
    members = lax.axis_size("gx")
    width = stream_in.shape[1]
    hsplit = members // MSPLIT
    cols = width // members
    block = width // MSPLIT
    batch = members
    hidden_cols = gate_weight.shape[2]
    narrow = hidden_cols // MSPLIT
    chunk = narrow if narrow % 128 == 0 else hidden_cols
    ring = min(RING, hidden_cols // chunk)
    vmem = pl.BlockSpec(memory_space=pltpu.VMEM)
    smem = pl.BlockSpec(memory_space=pltpu.SMEM)
    hbm = pl.BlockSpec(memory_space=pl.ANY)
    dma = pltpu.SemaphoreType.DMA
    rows = key_cache.shape[1]
    cap = batch * 5 // 8
    packed = 2 * RESIDENT * cap
    shifts = [q * cap % 8 for q in range(4)]
    lead = (cap + max(shifts) + 7) // 8 * 8
    hid_rows = (RESIDENT * cap + 7) // 8 * 8
    lanes = (batch + 127) // 128 * 128
    if narrow % 128 == 0 and 256 <= narrow <= block and NH * HS * cols == 4 * block * block:
        return large_call(
            stream_in,
            query,
            key_new,
            value_new,
            key_cache,
            value_cache,
            lengths,
            route_ids,
            route_scores,
            out_weight,
            norm_gain,
            gate_weight,
            up_weight,
            down_weight,
        )
    return pl.pallas_call(
        functools.partial(small_kernel, members),
        out_shape=jax.ShapeDtypeStruct((1, width), bf16),
        in_specs=[vmem] * 3 + [hbm] * 2 + [smem] * 3 + [vmem] * 2 + [hbm] * 4,
        out_specs=vmem,
        scratch_shapes=[
            pltpu.VMEM((rows, KVH * HS), bf16),
            pltpu.VMEM((rows, KVH * HS), bf16),
            dma((2,)),
            pltpu.VMEM((NH, HS), f32),
            pltpu.VMEM((2, KVH, HS), f32),
            pltpu.VMEM((members, 1, cols), f32),
            pltpu.VMEM(out_weight.shape, bf16),
            pltpu.VMEM((ring, 4, block, chunk), bf16),
            pltpu.VMEM((MSPLIT, RESIDENT, narrow, block), bf16),
            pltpu.VMEM((NH + PAD, HS), bf16),
            pltpu.VMEM((members, NH + PAD, HS), bf16),
            pltpu.VMEM((members * (NH + PAD), HS), f32),
            pltpu.VMEM((batch, NH * HS), bf16),
            pltpu.VMEM((members, 1, cols), f32),
            pltpu.VMEM((hsplit, batch, cols), f32),
            pltpu.VMEM((batch, cols), f32),
            pltpu.VMEM((1, lanes), f32),
            pltpu.VMEM((members, 1, lanes), f32),
            pltpu.VMEM((batch, block), bf16),
            pltpu.VMEM((4, lead, block), bf16),
            pltpu.VMEM((packed + 8, chunk), f32),
            pltpu.VMEM((MSPLIT, packed, narrow), bf16),
            pltpu.VMEM((MSPLIT, packed, narrow), bf16),
            pltpu.VMEM((hid_rows, narrow), bf16),
            pltpu.VMEM((MSPLIT, hid_rows, narrow), bf16),
            pltpu.VMEM((RESIDENT, hid_rows, block), f32),
            pltpu.VMEM((batch, block), f32),
            pltpu.VMEM((members, 1, block), f32),
            pltpu.VMEM((members, 1, block), f32),
            dma,
            dma((ring, 4)),
            dma((MSPLIT, RESIDENT)),
        ]
        + [dma((MSPLIT,)), dma((MSPLIT, hsplit))]
        + [dma((members,))] * 5
        + [dma((hsplit,))] * 2
        + [dma((MSPLIT,))] * 5
        + [dma((members,))] * 2,
        compiler_params=pltpu.CompilerParams(
            collective_id=0, has_side_effects=True, vmem_limit_bytes=67043328
        ),
    )(
        query,
        key_new,
        value_new,
        key_cache.reshape(rows, KVH * HS),
        value_cache.reshape(rows, KVH * HS),
        lengths,
        route_ids,
        route_scores,
        stream_in,
        norm_gain.reshape(MSPLIT, 1, block),
        out_weight,
        gate_weight,
        up_weight,
        down_weight,
    )

def solution(mesh):
    return jax.shard_map(
        on_device,
        mesh=mesh,
        in_specs=(
            P(("groups", "gx"), None),
            P(("groups", "gx"), None),
            P(("groups", "gx"), None),
            P(("groups", "gx"), None),
            P(("groups", "gx"), None, None),
            P(("groups", "gx"), None, None),
            P(("groups", "gx")),
            P(("groups", "gx"), None),
            P(("groups", "gx"), None),
            P(None, "gx"),
            P(),
            P(None, "gx", None),
            P(None, "gx", None),
            P(None, "gx", None),
        ),
        out_specs=P(("groups", "gx"), None),
        check_vma=False,
    )
```

```python
import functools

import jax
import jax.numpy as jnp
from jax import lax
from jax.experimental import pallas as pl
from jax.experimental.pallas import tpu as pltpu
from jax.sharding import PartitionSpec as P

NH = 64
KVH = 8
HS = 128
RESIDENT = 2
MSPLIT = 8
PAD = 16
RING = 3
ORDER = (0, 2, 1, 3)
MESH = pl.DeviceIdType.MESH

SLOTS = 28
CHUNKS = (
    (0, 0, 0),
    (0, 0, 1),
    (0, 0, 2),
    (0, 0, 3),
    (0, 1, 0),
    (0, 1, 1),
    (0, 1, 2),
    (0, 1, 3),
    (1, 0, 0),
    (1, 0, 1),
    (1, 0, 2),
    (1, 0, 3),
    (1, 1, 0),
    (1, 1, 1),
    (1, 1, 2),
    (1, 1, 3),
)
SPREAD = (0, 2, 6, 4, 1, 3, 7, 5)

def large_kernel(
    members,
    query_hbm,
    key_new_hbm,
    value_new_hbm,
    key_hbm,
    value_hbm,
    lengths_hbm,
    ids_hbm,
    scores_hbm,
    stream_hbm,
    gain_hbm,
    out_weight,
    gate_weight,
    up_weight,
    down_weight,
    out,
    lengths,
    route_ids,
    route_scores,
    query,
    fresh_kv,
    stream,
    gain,
    cache,
    in_sem,
    heads,
    own_rows,
    stream_rows,
    stream_recv,
    stream_flat,
    pool,
    attn_send,
    attn_recv,
    attn_wide,
    attn_rows,
    resid_keep,
    y_send,
    y_recv,
    sq_send,
    sq_recv,
    slots_in,
    acc_a,
    acc_b,
    px_send_a,
    px_send_b,
    px_recv_a,
    px_recv_b,
    pz_send_a,
    pz_send_b,
    pz_recv_a,
    pz_recv_b,
    hid_send_a,
    hid_send_b,
    hid_recv_a,
    hid_recv_b,
    total,
    final_flat,
    final_send,
    final_recv,
    wo_sem,
    gu_sem,
    down_sem,
    a_send,
    a_relay,
    a_recv,
    a_mate,
    s_send,
    s_recv,
    q_send,
    q_recv,
    r_send,
    r_recv,
    x_send,
    x_recv,
    z_send,
    z_recv,
    h_send,
    h_relay,
    h_recv,
    f_send,
    f_recv,
):
    f32, bf16 = jnp.float32, jnp.bfloat16
    hsplit = members // MSPLIT
    me = lax.axis_index("gx")
    m = me // hsplit
    h = lax.rem(me, hsplit)
    batch = members
    cols = y_send.shape[1]
    width = cols * members
    block = width // MSPLIT
    group = NH // KVH
    acc, px_send, px_recv = (acc_a, acc_b), (px_send_a, px_send_b), (px_recv_a, px_recv_b)
    pz_send, pz_recv = (pz_send_a, pz_send_b), (pz_recv_a, pz_recv_b)
    hid_send, hid_recv = (hid_send_a, hid_send_b), (hid_recv_a, hid_recv_b)
    wide = (acc_a.shape[2], acc_b.shape[2])
    first = (0, wide[0])
    chunk = wide[0] + wide[1]
    cap = batch * 5 // 8
    packed = px_send_a.shape[1]
    hid_rows = hid_send_a.shape[0]
    lead = slots_in.shape[1] // 2
    lanes = sq_send.shape[1]
    half = MSPLIT // 2
    side = block // cols
    pieces = NH * HS // block

    def peer(d):
        return lax.rem(me + d, members)

    def model(d):
        d = jnp.asarray(d, jnp.int32)
        to = 0
        for b in (1, 2, 4):
            to = to + lax.rem(lax.div(m, b) + lax.div(d, b), 2) * b
        return to

    def mate(d):
        return lax.rem(h + d, hsplit)

    def far(i):
        d = members - i
        return model(d // hsplit) * hsplit + lax.rem(h + lax.rem(d, hsplit), hsplit)

    def settle(ref, sem):
        pltpu.make_async_copy(ref, ref, sem).wait()

    def remote(src, dst, send, recv, device):
        return pltpu.make_async_remote_copy(
            src_ref=src,
            dst_ref=dst,
            send_sem=send,
            recv_sem=recv,
            device_id={"gx": device},
            device_id_type=MESH,
        )

    barrier = pltpu.get_barrier_semaphore()
    key_cache, value_cache = cache.at[0], cache.at[1]
    sources = (
        ((query_hbm, query),),
        ((key_hbm, key_cache), (value_hbm, value_cache)),
        ((key_new_hbm, fresh_kv.at[0]), (value_new_hbm, fresh_kv.at[1])),
        ((lengths_hbm, lengths),),
        ((ids_hbm, route_ids),),
        ((scores_hbm, route_scores),),
        ((stream_hbm, stream),),
        ((gain_hbm.at[me], gain),),
    )
    for k, pairs in enumerate(sources):
        for src, dst in pairs:
            pltpu.make_async_copy(src, dst, in_sem.at[k]).start()

    @pl.loop(1, members)
    def _(d):
        pl.semaphore_signal(barrier, inc=1, device_id={"gx": peer(d)}, device_id_type=MESH)

    def wo_copy(k):
        return pltpu.make_async_copy(
            out_weight.at[pl.ds(k * block, block), :],
            pool.at[k // side, :, pl.ds(k % side * cols, cols)],
            wo_sem.at[0],
        )

    def gu_slot(c):
        return (half + 2 * c) % SLOTS

    def gu_start(c):
        p, z, i = CHUNKS[c]
        at = pl.multiple_of(model(2 * (half - 1 - i) + 1 - z) * chunk + first[p], 128)
        for q in range(4):
            r, w = q // 2, (gate_weight, up_weight)[q % 2]
            pltpu.make_async_copy(
                w.at[r, :, pl.ds(at, wide[p])],
                pool.at[gu_slot(c) + r, :, pl.ds(q % 2 * wide[p], wide[p])],
                gu_sem.at[c],
            ).start()

    def arrived(c):
        p = CHUNKS[c][0]
        settle(pool.at[pl.ds(gu_slot(c), 2), :, pl.ds(0, 2 * wide[p])], gu_sem.at[c])

    def down_slot(p, k):
        return (half + (4 + p) * MSPLIT + k) % SLOTS

    def down_start(t):
        p, k = t // MSPLIT, t % MSPLIT
        at = pl.multiple_of(model(SPREAD[k]) * chunk + first[p], 16)
        for r in range(RESIDENT):
            pltpu.make_async_copy(
                down_weight.at[r, pl.ds(at, wide[p]), :],
                pool.at[down_slot(p, k), pl.ds(r * wide[p], wide[p]), :],
                down_sem.at[t],
            ).start()

    def refill(c):
        if c < 2:
            gu_start(2 * MSPLIT - 2 + c)
        elif c < MSPLIT + 2:
            down_start(2 * c - 4)
            down_start(2 * c - 3)

    for k in range(pieces):
        wo_copy(k).start()

    scale = HS ** (-0.5)
    settle(query, in_sem.at[0])
    for n in range(NH):
        heads[n : n + 1, :] = query[:, n * HS : (n + 1) * HS].astype(f32)

    for k, ref in enumerate(
        (cache, fresh_kv, lengths, route_ids, route_scores, stream, gain), start=1
    ):
        settle(ref, in_sem.at[k])

    for g in range(KVH):
        own_rows[0, g : g + 1, :] = fresh_kv[0, :, g * HS : (g + 1) * HS].astype(f32)
        own_rows[1, g : g + 1, :] = fresh_kv[1, :, g * HS : (g + 1) * HS].astype(f32)
    wide_q = heads[...]
    s = jnp.concatenate(
        [
            lax.dot_general(
                wide_q[g * group : (g + 1) * group].astype(bf16),
                key_cache[:, g * HS : (g + 1) * HS],
                (((1,), (1,)), ((), ())),
                preferred_element_type=f32,
            )
            for g in range(KVH)
        ],
        axis=0,
    )
    s = s * scale
    live = lax.broadcasted_iota(jnp.int32, s.shape, 1) < lengths[0]
    s = jnp.where(live, s, -1e30)
    k_own, v_own = own_rows[0], own_rows[1]
    spread = lambda v: jnp.concatenate(
        [jnp.broadcast_to(v[g : g + 1], (group, HS)) for g in range(KVH)], axis=0
    )
    own = jnp.sum(wide_q * spread(k_own), axis=-1, keepdims=True) * scale
    top = jnp.maximum(jnp.max(s, axis=-1, keepdims=True), own)
    e_cache = jnp.exp(s - top)
    e_own = jnp.exp(own - top)
    norm = jnp.sum(e_cache, axis=-1, keepdims=True) + e_own
    p = e_cache / norm
    p_own = (e_own / norm).astype(bf16).astype(f32)
    mixed = jnp.concatenate(
        [
            jnp.dot(
                p[g * group : (g + 1) * group].astype(bf16),
                value_cache[:, g * HS : (g + 1) * HS],
                preferred_element_type=f32,
            )
            for g in range(KVH)
        ],
        axis=0,
    )
    mixed = mixed + p_own * spread(v_own)
    attn_send[...] = mixed.astype(bf16)
    spot = lax.broadcasted_iota(jnp.int32, (1, HS), 1)
    full = lambda v: jnp.full((1, HS), v)
    s0, s1 = full(route_scores[0, 0]), full(route_scores[0, 1])
    i0, i1 = full(route_ids[0, 0]), full(route_ids[0, 1])
    peak = jnp.maximum(s0, s1)
    x0, x1 = jnp.exp(s0 - peak), jnp.exp(s1 - peak)
    pick = jnp.where(i0 == spot, x0 / (x0 + x1), 0.0) + jnp.where(i1 == spot, x1 / (x0 + x1), 0.0)
    pick = pick.astype(bf16).astype(f32)
    for j in range(members):
        stream_rows[j, :, :cols] = stream[:, j * cols : (j + 1) * cols].astype(f32)
        stream_rows[j, :, cols:] = pick

    pl.semaphore_wait(barrier, members - 1)

    def attn_copy(d, slot):
        return remote(
            attn_send, attn_recv.at[slot], a_send.at[0], a_recv.at[d], model(d) * hsplit + h
        )

    def attn_relay(d, t, slot):
        src = attn_send if isinstance(d, int) else attn_recv.at[slot]
        return remote(
            src, attn_recv.at[slot], a_relay.at[0], a_mate.at[0], m * hsplit + t
        )

    def stream_copy(to, slot):
        return remote(
            stream_rows.at[to], stream_recv.at[slot], s_send.at[0], s_recv.at[0], to
        )

    @pl.loop(0, MSPLIT - 1)
    def _(i):
        attn_copy(MSPLIT - 1 - i, me).start()

    @pl.loop(1, hsplit)
    def _(d):
        attn_relay(0, mate(d), me).start()

    @pl.loop(1, members)
    def _(d):
        stream_copy(peer(d), me).start()

    def widen(slot, rows):
        at = pl.multiple_of(slot * NH, NH)
        attn_wide[pl.ds(at, NH), :] = rows.astype(f32)

    for c in range(2 * MSPLIT - half):
        gu_start(c)

    widen(me, attn_send[...])
    stream_recv[me] = stream_rows[me]

    @pl.loop(1, MSPLIT)
    def _(i):
        slot = model(i) * hsplit + h
        attn_copy(i, slot).wait_recv()

        @pl.loop(1, hsplit)
        def _(d):
            attn_relay(i, mate(d), slot).start()

        widen(slot, attn_recv[slot])

    settle(attn_recv.at[pl.ds(0, MSPLIT * (hsplit - 1))], a_mate.at[0])

    @pl.loop(0, MSPLIT)
    def _(i):
        @pl.loop(1, hsplit)
        def _(d):
            slot = model(i) * hsplit + mate(d)
            widen(slot, attn_recv[slot])

    settle(pool.at[pl.ds(0, half)], wo_sem.at[0])

    settle(stream_recv.at[pl.ds(0, members - 1)], s_recv.at[0])

    for j in range(members):
        stream_flat[j : j + 1, :] = stream_recv[j]

    for n in range(NH):
        attn_rows[:, n * HS : (n + 1) * HS] = attn_wide[pl.ds(n, batch, stride=NH), :].astype(bf16)

    proj = jnp.zeros((batch, cols), f32)
    for k in range(pieces):
        proj = proj + jnp.dot(
            attn_rows[:, k * block : (k + 1) * block],
            pool[k // side, :, k % side * cols : (k % side + 1) * cols],
            preferred_element_type=f32,
        )
    gu_start(2 * MSPLIT - 4)
    gu_start(2 * MSPLIT - 3)

    resid = stream_flat[:, :cols] + proj.astype(bf16).astype(f32)
    resid_keep[...] = resid
    y_send[...] = (resid * gain[...]).astype(bf16)

    def y_copy(to, slot):
        return remote(y_send, y_recv.at[slot], r_send.at[0], r_recv.at[0], m * hsplit + to)

    @pl.loop(1, hsplit)
    def _(d):
        y_copy(mate(d), h).start()

    sub_w = lax.broadcasted_iota(jnp.int32, (batch, lanes), 0)
    lane_w = lax.broadcasted_iota(jnp.int32, (batch, lanes), 1)
    squares = jnp.sum(resid * resid, axis=-1, keepdims=True)
    sq_send[...] = jnp.sum(jnp.where(sub_w == lane_w, squares, 0.0), axis=0, keepdims=True)

    def sq_copy(to, slot):
        return remote(sq_send, sq_recv.at[slot], q_send.at[0], q_recv.at[0], to)

    @pl.loop(1, members)
    def _(d):
        sq_copy(peer(d), me).start()

    sq_recv[me] = sq_send[...]
    y_recv[h] = y_send[...]
    scales = [stream_flat[:, cols + r : cols + r + 1] for r in range(RESIDENT)]
    sub = lax.broadcasted_iota(jnp.int32, (batch, batch), 0)
    lane = lax.broadcasted_iota(jnp.int32, (batch, batch), 1)
    named, rank, back = [], [], []
    for r in range(RESIDENT):
        col = jnp.where(scales[r] > 0.0, 1.0, 0.0)
        row = jnp.sum(jnp.where(sub == lane, col, 0.0), axis=0, keepdims=True)
        named.append(row)
        rank.append(jnp.sum(jnp.where(sub < lane, col, 0.0), axis=0, keepdims=True))
        place = jnp.sum(jnp.where(lane < sub, row, 0.0), axis=1, keepdims=True)
        at = lax.broadcasted_iota(jnp.int32, (batch, hid_rows), 1)
        hit = at == place.astype(jnp.int32) + r * cap
        back.append(jnp.where(hit, scales[r], 0.0))

    settle(y_recv.at[pl.ds(0, hsplit - 1)], r_recv.at[0])

    y = jnp.concatenate([y_recv[j] for j in range(hsplit)], axis=1)
    bases = [q * cap // 8 * 8 for q in range(4)]
    for q in range(4):
        r = q % 2
        shift = q * cap - bases[q]
        at = lax.broadcasted_iota(jnp.int32, (lead, batch), 0)
        hit = (at == rank[r].astype(jnp.int32) + shift) & (named[r] > 0.0)
        slots_in[r, q // 2 * lead : (q // 2 + 1) * lead, :] = jnp.dot(
            jnp.where(hit, 1.0, 0.0).astype(bf16), y, preferred_element_type=f32
        ).astype(bf16)

    def px_copy(p, i):
        return remote(
            px_send[p].at[i],
            px_recv[p].at[i],
            x_send.at[p],
            x_recv.at[p, i],
            model(1) * hsplit + h,
        )

    def pz_copy(p, j):
        return remote(
            pz_send[p].at[j],
            pz_recv[p].at[j],
            z_send.at[p],
            z_recv.at[p],
            model(2 * (half - 1 - j)) * hsplit + h,
        )

    def sums(c):
        p = CHUNKS[c][0]
        w = wide[p]
        slabs = [[] for _ in range(acc[p].shape[1] // 8)]
        for r in range(RESIDENT):
            where = gu_slot(c) + r
            values = [
                jnp.dot(
                    slots_in[r, q * lead : (q + 1) * lead, :],
                    pool[where, :, q * w : (q + 1) * w],
                    preferred_element_type=f32,
                )
                for q in range(2)
            ]
            for q in range(2):
                for k in range(lead // 8):
                    slabs[bases[2 * q + r] // 8 + k].append(values[q][k * 8 : (k + 1) * 8])
        empty = jnp.zeros((8, w), f32)
        return jnp.concatenate([sum(slab[1:], slab[0]) if slab else empty for slab in slabs], axis=0)

    def gate_up(*cs):
        for c in cs:
            arrived(c)
        for c in cs:
            p, z, i = CHUNKS[c]
            if z:
                acc[p][i % 2] = sums(c)
            else:
                px_send[p][i] = sums(c)[:packed].astype(bf16)
                px_copy(p, i).start()
        for c in cs:
            refill(c)
        for c in cs:
            p, z, i = CHUNKS[c]
            if z:
                px_copy(p, i).wait_recv()
                acc[p][i % 2, :packed, :] += px_recv[p][i].astype(f32)
                if i < half - 1:
                    pz_send[p][i] = acc[p][i % 2, :packed, :].astype(bf16)
                    pz_copy(p, i).start()

    def hid_group(p, d):
        if p == 0:
            return d // 2 if d % 2 == 0 else 0
        return (0, 0, 0, 0, 1, 1, 2, 2)[SPREAD.index(d)]

    def hid_copy(p, d, slot):
        return remote(
            hid_send[p],
            hid_recv[p].at[slot],
            h_send.at[p],
            h_recv.at[p, hid_group(p, d)],
            model(d) * hsplit + h,
        )

    def hid_relay(p, j, slot):
        return remote(
            hid_recv[p].at[slot],
            hid_recv[p].at[slot],
            h_relay.at[0],
            h_recv.at[p, 0],
            model(1) * hsplit + h,
        )

    def finish(p, last):
        settle(pz_recv[p], z_recv.at[p])
        for j in range(half - 1):
            acc[p][last, :packed, :] += pz_recv[p][j].astype(f32)
        a = acc[p][last, :hid_rows, :] * scaled
        b = acc[p][last, 2 * cap : 2 * cap + hid_rows, :] * scaled
        hid_send[p][...] = (a / (1.0 + jnp.exp(-a)) * b).astype(bf16)
        for d in (1, *SPREAD[1:half]) if p == 0 else range(MSPLIT - 1, 0, -1):
            hid_copy(p, d, m).start()
        hid_recv[p][m] = hid_send[p][...]

    def relays(p):
        for k in range(1, half):
            slot = model(SPREAD[k])
            hid_copy(p, SPREAD[k], slot).wait_recv()
            hid_relay(p, k, slot).start()

    def down(p, ks, fresh=False):
        groups = {}
        for k in ks:
            if k >= half or k and p:
                groups.setdefault(hid_group(p, SPREAD[k]), []).append(k)
            settle(pool.at[down_slot(p, k), pl.ds(0, 2 * wide[p]), :], down_sem.at[p * MSPLIT + k])
        for g, members_of in groups.items():
            settle(hid_recv[p].at[pl.ds(0, len(members_of))], h_recv.at[p, g])
        line = lax.broadcasted_iota(jnp.int32, (hid_rows, wide[p]), 0)
        value = None if fresh else total[...]
        for k in ks:
            rows = hid_recv[p][model(SPREAD[k])].astype(f32)
            split = [
                jnp.where((line >= r * cap) & (line < (r + 1) * cap), rows, 0.0).astype(bf16)
                for r in range(RESIDENT)
            ]
            term = jnp.dot(
                jnp.concatenate(split, axis=1),
                pool[down_slot(p, k), : RESIDENT * wide[p], :],
                preferred_element_type=f32,
            )
            value = term if value is None else value + term
        total[...] = value

    gate_up(0)
    gate_up(1)
    gate_up(2)
    gate_up(3)

    gate_up(4, 5)
    gate_up(6, 7)

    gate_up(8, 9)
    gate_up(10, 11)

    settle(sq_recv.at[pl.ds(0, members - 1)], q_recv.at[0])

    power = jnp.sum(sq_recv[...], axis=0)[:, :batch] * (1.0 / width)
    inverse = lax.rsqrt(power + 1e-05)
    at = lax.broadcasted_iota(jnp.int32, (hid_rows, batch), 0)
    scaled = jnp.zeros((hid_rows, 1), f32)
    for r in range(RESIDENT):
        hit = (at == rank[r].astype(jnp.int32) + r * cap) & (named[r] > 0.0)
        scaled = scaled + jnp.sum(jnp.where(hit, inverse, 0.0), axis=1, keepdims=True)

    finish(0, 1)

    gate_up(12)
    gate_up(13)
    gate_up(14)
    gate_up(15)

    relays(0)

    down(0, range(half), True)

    finish(1, 1)

    down(0, range(half, MSPLIT))

    down(1, range(half))

    down(1, (4, 5))

    down(1, (6, 7))

    resid = resid_keep[...]
    whole = jnp.concatenate([jnp.where(h == j, resid, 0.0) for j in range(hsplit)], axis=1)
    mix = sum(back[1:], back[0])
    for n in range(RESIDENT * cap):
        whole = whole + mix[:, n : n + 1] * total[n : n + 1, :]
    tiles = block // HS
    for t in range(tiles):
        final_flat[t * batch : (t + 1) * batch, :] = whole[:, t * HS : (t + 1) * HS]
    for j in range(members):
        final_send[j] = final_flat[pl.ds(j, tiles, stride=batch), :].astype(bf16)

    def final_copy(to, slot):
        return remote(
            final_send.at[to], final_recv.at[slot], f_send.at[0], f_recv.at[0], to
        )

    @pl.loop(1, members)
    def _(d):
        final_copy(far(d), me).start()

    final_recv[me] = final_send[me]

    settle(stream_recv.at[pl.ds(0, members - 1)], s_send.at[0])
    settle(sq_recv.at[pl.ds(0, members - 1)], q_send.at[0])
    settle(y_recv.at[pl.ds(0, hsplit - 1)], r_send.at[0])
    settle(attn_recv.at[pl.ds(0, MSPLIT * (hsplit - 1))], a_relay.at[0])
    settle(attn_recv.at[pl.ds(0, MSPLIT - 1)], a_send.at[0])
    for p in range(2):
        settle(px_recv[p], x_send.at[p])
        settle(pz_recv[p], z_send.at[p])
        settle(hid_recv[p].at[pl.ds(0, MSPLIT - 1 if p else half)], h_send.at[p])
    settle(hid_recv[0].at[pl.ds(0, half - 1)], h_relay.at[0])

    settle(final_recv.at[pl.ds(0, members - 1)], f_recv.at[0])

    for j in range(MSPLIT):
        line = final_recv[j * hsplit].astype(f32)
        for k in range(1, hsplit):
            line = line + final_recv[j * hsplit + k].astype(f32)
        out[j * tiles : (j + 1) * tiles, :] = line.astype(bf16)

    settle(final_recv.at[pl.ds(0, members - 1)], f_send.at[0])

def large_call(
    stream_in,
    query,
    key_new,
    value_new,
    key_cache,
    value_cache,
    lengths,
    route_ids,
    route_scores,
    out_weight,
    norm_gain,
    gate_weight,
    up_weight,
    down_weight,
):
    f32, bf16 = jnp.float32, jnp.bfloat16
    members = lax.axis_size("gx")
    width = stream_in.shape[1]
    hsplit = members // MSPLIT
    cols = width // members
    block = width // MSPLIT
    batch = members
    narrow = gate_weight.shape[2] // MSPLIT
    vmem = pl.BlockSpec(memory_space=pltpu.VMEM)
    hbm = pl.BlockSpec(memory_space=pl.ANY)
    dma = pltpu.SemaphoreType.DMA
    rows = key_cache.shape[1]
    cap = batch * 5 // 8
    packed = 2 * RESIDENT * cap
    shifts = [q * cap % 8 for q in range(4)]
    lead = (cap + max(shifts) + 7) // 8 * 8
    hid_rows = (RESIDENT * cap + 7) // 8 * 8
    lanes = (batch + 127) // 128 * 128
    half = MSPLIT // 2
    tiles = block // HS
    wide = [(narrow // 128 + 1) // 2 * 128]
    wide.append(narrow - wide[0])
    result = pl.pallas_call(
        functools.partial(large_kernel, members),
        out_shape=pltpu.VMEM((width // HS, HS), bf16),
        in_specs=[hbm] * 14,
        out_specs=vmem,
        scratch_shapes=[
            pltpu.SMEM(lengths.shape, jnp.int32),
            pltpu.SMEM(route_ids.shape, jnp.int32),
            pltpu.SMEM(route_scores.shape, f32),
            pltpu.VMEM((1, NH * HS), bf16),
            pltpu.VMEM((2, 1, KVH * HS), bf16),
            pltpu.VMEM((1, width), bf16),
            pltpu.VMEM((1, cols), f32),
            pltpu.VMEM((2, rows, KVH * HS), bf16),
            dma((8,)),
            pltpu.VMEM((NH, HS), f32),
            pltpu.VMEM((2, KVH, HS), f32),
            pltpu.VMEM((members, 1, cols + HS), f32),
            pltpu.VMEM((members, 1, cols + HS), f32),
            pltpu.VMEM((batch, cols + HS), f32),
            pltpu.VMEM((SLOTS, block, block), bf16),
            pltpu.VMEM((NH, HS), bf16),
            pltpu.VMEM((members, NH, HS), bf16),
            pltpu.VMEM((members * NH, HS), f32),
            pltpu.VMEM((batch, NH * HS), bf16),
            pltpu.VMEM((batch, cols), f32),
            pltpu.VMEM((batch, cols), bf16),
            pltpu.VMEM((hsplit, batch, cols), bf16),
            pltpu.VMEM((1, lanes), f32),
            pltpu.VMEM((members, 1, lanes), f32),
            pltpu.VMEM((RESIDENT, 2 * lead, block), bf16),
            *[pltpu.VMEM((2, packed + 8, w), f32) for w in wide],
            *[pltpu.VMEM((half, packed, w), bf16) for w in wide],
            *[pltpu.VMEM((half, packed, w), bf16) for w in wide],
            *[pltpu.VMEM((half - 1, packed, w), bf16) for w in wide],
            *[pltpu.VMEM((half - 1, packed, w), bf16) for w in wide],
            *[pltpu.VMEM((hid_rows, w), bf16) for w in wide],
            *[pltpu.VMEM((MSPLIT, hid_rows, w), bf16) for w in wide],
            pltpu.VMEM((hid_rows, block), f32),
            pltpu.VMEM((tiles * batch, HS), f32),
            pltpu.VMEM((members, tiles, HS), bf16),
            pltpu.VMEM((members, tiles, HS), bf16),
            dma((1,)),
            dma((2 * MSPLIT,)),
            dma((2 * MSPLIT,)),
        ]
        + [dma((1,))] * 2
        + [dma((MSPLIT,))]
        + [dma((1,))] * 7
        + [dma((2,)), dma((2, half))]
        + [dma((2,))] * 3
        + [dma((1,)), dma((2, half))]
        + [dma((1,))] * 2,
        compiler_params=pltpu.CompilerParams(
            collective_id=0, has_side_effects=True, vmem_limit_bytes=66000000
        ),
    )(
        query,
        key_new,
        value_new,
        key_cache.reshape(rows, KVH * HS),
        value_cache.reshape(rows, KVH * HS),
        lengths,
        route_ids,
        route_scores,
        stream_in,
        norm_gain.reshape(members, 1, cols),
        out_weight,
        gate_weight,
        up_weight,
        down_weight,
    )
    return result.reshape(1, width)

def small_kernel(
    members,
    query,
    key_new,
    value_new,
    key_hbm,
    value_hbm,
    lengths,
    route_ids,
    route_scores,
    stream,
    gain,
    out_weight,
    gate_weight,
    up_weight,
    down_weight,
    out,
    key_cache,
    value_cache,
    cache_sem,
    heads,
    own_rows,
    stream_rows,
    wo,
    gu,
    down,
    attn_send,
    attn_recv,
    attn_wide,
    attn_rows,
    stream_recv,
    resid_recv,
    resid_send,
    sq_send,
    sq_recv,
    normed,
    slots_in,
    acc,
    part_send,
    part_recv,
    hid_send,
    hid_recv,
    total,
    resid_full,
    final_send,
    final_recv,
    wo_sem,
    gu_sem,
    down_sem,
    a_send,
    a_relay,
    a_recv,
    s_send,
    s_recv,
    q_send,
    q_recv,
    r_send,
    r_recv,
    p_send,
    p_recv,
    h_send,
    h_relay,
    h_recv,
    f_send,
    f_recv,
):
    f32, bf16 = jnp.float32, jnp.bfloat16
    hsplit = members // MSPLIT
    me = lax.axis_index("gx")
    m = me // hsplit
    h = lax.rem(me, hsplit)
    batch = members
    cols = wo.shape[1]
    width = cols * members
    block = width // MSPLIT
    group = NH // KVH
    chunk = gu.shape[3]
    chunks = gate_weight.shape[2] // chunk
    narrow = part_send.shape[2]
    cap = batch * 5 // 8
    packed = part_send.shape[1]
    hid_rows = hid_send.shape[0]
    lead = slots_in.shape[1]
    lanes = sq_send.shape[1]
    ring = gu.shape[0]

    def peer(d):
        return lax.rem(me + d, members)

    def model(d):
        d = jnp.asarray(d, jnp.int32)
        to = 0
        for b in (1, 2, 4):
            to = to + lax.rem(lax.div(m, b) + lax.div(d, b), 2) * b
        return to

    def mate(d):
        return lax.rem(h + d, hsplit)

    def remote(src, dst, send, recv, device):
        return pltpu.make_async_remote_copy(
            src_ref=src,
            dst_ref=dst,
            send_sem=send,
            recv_sem=recv,
            device_id={"gx": device},
            device_id_type=MESH,
        )

    barrier = pltpu.get_barrier_semaphore()

    @pl.loop(1, members)
    def _(d):
        pl.semaphore_signal(barrier, inc=1, device_id={"gx": peer(d)}, device_id_type=MESH)

    key_copy = pltpu.make_async_copy(key_hbm, key_cache, cache_sem.at[0])
    value_copy = pltpu.make_async_copy(value_hbm, value_cache, cache_sem.at[1])
    key_copy.start()
    value_copy.start()
    wo_copy = pltpu.make_async_copy(out_weight, wo, wo_sem)
    wo_copy.start()

    def gu_copy(i, q):
        r, w = q // 2, (gate_weight, up_weight)[q % 2]
        if chunks == 1:
            src = w.at[r]
        else:
            at = pl.multiple_of(model(MSPLIT - 1 - i) * chunk, 128)
            src = w.at[r, :, pl.ds(at, chunk)]
        slot = lax.rem(i, ring)
        return pltpu.make_async_copy(src, gu.at[slot, q], gu_sem.at[slot, q])

    def down_copy(i, r):
        at = pl.multiple_of(model(i) * narrow, 16)
        return pltpu.make_async_copy(
            down_weight.at[r, pl.ds(at, narrow), :], down.at[i, r], down_sem.at[i, r]
        )

    @pl.loop(0, ring)
    def _(i):
        for q in range(4):
            gu_copy(i, q).start()

    @pl.loop(0, MSPLIT)
    def _(i):
        for r in range(RESIDENT):
            down_copy(i, r).start()

    scale = HS ** (-0.5)
    for n in range(NH):
        heads[n : n + 1, :] = query[:, n * HS : (n + 1) * HS].astype(f32)
    for g in range(KVH):
        own_rows[0, g : g + 1, :] = key_new[:, g * HS : (g + 1) * HS].astype(f32)
        own_rows[1, g : g + 1, :] = value_new[:, g * HS : (g + 1) * HS].astype(f32)
    for j in range(members):
        stream_rows[j] = stream[:, j * cols : (j + 1) * cols].astype(f32)
    wide_q = heads[...]
    key_copy.wait()
    value_copy.wait()
    s = jnp.concatenate(
        [
            lax.dot_general(
                wide_q[g * group : (g + 1) * group].astype(bf16),
                key_cache[:, g * HS : (g + 1) * HS],
                (((1,), (1,)), ((), ())),
                preferred_element_type=f32,
            )
            for g in range(KVH)
        ],
        axis=0,
    )
    s = s * scale
    live = lax.broadcasted_iota(jnp.int32, s.shape, 1) < lengths[0]
    s = jnp.where(live, s, -1e30)
    k_own, v_own = own_rows[0], own_rows[1]
    spread = lambda v: jnp.concatenate(
        [jnp.broadcast_to(v[g : g + 1], (group, HS)) for g in range(KVH)], axis=0
    )
    own = jnp.sum(wide_q * spread(k_own), axis=-1, keepdims=True) * scale
    top = jnp.maximum(jnp.max(s, axis=-1, keepdims=True), own)
    e_cache = jnp.exp(s - top)
    e_own = jnp.exp(own - top)
    norm = jnp.sum(e_cache, axis=-1, keepdims=True) + e_own
    p = e_cache / norm
    p_own = (e_own / norm).astype(bf16).astype(f32)
    mixed = jnp.concatenate(
        [
            jnp.dot(
                p[g * group : (g + 1) * group].astype(bf16),
                value_cache[:, g * HS : (g + 1) * HS],
                preferred_element_type=f32,
            )
            for g in range(KVH)
        ],
        axis=0,
    )
    mixed = mixed + p_own * spread(v_own)
    attn_send[:NH, :] = mixed.astype(bf16)
    full = lambda v: jnp.full((PAD, HS), v)
    s0, s1 = full(route_scores[0, 0]), full(route_scores[0, 1])
    i0, i1 = full(route_ids[0, 0]), full(route_ids[0, 1])
    peak = jnp.maximum(s0, s1)
    x0, x1 = jnp.exp(s0 - peak), jnp.exp(s1 - peak)
    row = lax.broadcasted_iota(jnp.int32, (PAD, HS), 0)
    pick = jnp.where(i0 == row, x0 / (x0 + x1), 0.0) + jnp.where(i1 == row, x1 / (x0 + x1), 0.0)
    attn_send[NH:, :] = pick.astype(bf16)

    pl.semaphore_wait(barrier, members - 1)

    def attn_copy(d, slot):
        return remote(
            attn_send, attn_recv.at[slot], a_send.at[d], a_recv.at[slot], model(d) * hsplit + h
        )

    def attn_relay(d, t, slot):
        src = attn_send if isinstance(d, int) else attn_recv.at[slot]
        return remote(
            src, attn_recv.at[slot], a_relay.at[d, t], a_recv.at[slot], m * hsplit + t
        )

    def stream_copy(to, slot):
        return remote(
            stream_rows.at[to], stream_recv.at[slot], s_send.at[to], s_recv.at[slot], to
        )

    @pl.loop(0, MSPLIT - 1)
    def _(i):
        attn_copy(MSPLIT - 1 - i, me).start()

    @pl.loop(1, hsplit)
    def _(d):
        attn_relay(0, mate(d), me).start()

    @pl.loop(1, members)
    def _(d):
        stream_copy(peer(d), me).start()

    attn_recv[me] = attn_send[...]
    stream_recv[me] = stream_rows[me]

    @pl.loop(1, MSPLIT)
    def _(i):
        slot = model(i) * hsplit + h
        attn_copy(i, slot).wait_recv()

        @pl.loop(1, hsplit)
        def _(d):
            attn_relay(i, mate(d), slot).start()

    @pl.loop(0, MSPLIT)
    def _(i):
        @pl.loop(1, hsplit)
        def _(d):
            attn_copy(i, model(i) * hsplit + mate(d)).wait_recv()

    stride = NH + PAD

    @pl.loop(0, members)
    def _(j):
        attn_wide[pl.ds(j * stride, stride), :] = attn_recv[j].astype(f32)

    for n in range(NH):
        attn_rows[:, n * HS : (n + 1) * HS] = attn_wide[pl.ds(n, batch, stride=stride), :].astype(
            bf16
        )
    scales = [attn_wide[pl.ds(NH + r, batch, stride=stride), :][:, :1] for r in range(RESIDENT)]

    sub = lax.broadcasted_iota(jnp.int32, (batch, batch), 0)
    lane = lax.broadcasted_iota(jnp.int32, (batch, batch), 1)
    named, rank, back = [], [], []
    for r in range(RESIDENT):
        col = jnp.where(scales[r] > 0.0, 1.0, 0.0)
        row = jnp.sum(jnp.where(sub == lane, col, 0.0), axis=0, keepdims=True)
        named.append(row)
        rank.append(jnp.sum(jnp.where(sub < lane, col, 0.0), axis=0, keepdims=True))
        place = jnp.sum(jnp.where(lane < sub, row, 0.0), axis=1, keepdims=True)
        at = lax.broadcasted_iota(jnp.int32, (batch, hid_rows), 1)
        hit = at == place.astype(jnp.int32) + r * cap
        back.append(jnp.where(hit, scales[r], 0.0))

    wo_copy.wait()
    proj = jnp.dot(attn_rows[...], wo[...], preferred_element_type=f32).astype(bf16)

    @pl.loop(1, members)
    def _(d):
        stream_copy(me, peer(d)).wait_recv()

    @pl.loop(0, members)
    def _(j):
        resid_send[pl.ds(j, 1), :] = stream_recv[j]

    resid = resid_send[...] + proj.astype(f32)
    resid_send[...] = resid
    sub_w = lax.broadcasted_iota(jnp.int32, (batch, lanes), 0)
    lane_w = lax.broadcasted_iota(jnp.int32, (batch, lanes), 1)
    squares = jnp.sum(resid * resid, axis=-1, keepdims=True)
    sq_send[...] = jnp.sum(jnp.where(sub_w == lane_w, squares, 0.0), axis=0, keepdims=True)

    def sq_copy(to, slot):
        return remote(sq_send, sq_recv.at[slot], q_send.at[to], q_recv.at[slot], to)

    def resid_copy(to, slot):
        return remote(
            resid_send, resid_recv.at[slot], r_send.at[to], r_recv.at[slot], m * hsplit + to
        )

    @pl.loop(1, members)
    def _(d):
        sq_copy(peer(d), me).start()

    @pl.loop(1, hsplit)
    def _(d):
        resid_copy(mate(d), h).start()

    sq_recv[me] = sq_send[...]
    resid_recv[h] = resid_send[...]

    @pl.loop(1, hsplit)
    def _(d):
        resid_copy(h, mate(d)).wait_recv()

    @pl.loop(1, members)
    def _(d):
        sq_copy(me, peer(d)).wait_recv()

    squares = jnp.sum(sq_recv[...], axis=0)
    squares = jnp.sum(jnp.where(sub_w == lane_w, squares, 0.0), axis=1, keepdims=True)
    power = squares * (1.0 / width)
    inverse = lax.rsqrt(power + 1e-05)
    block_resid = jnp.concatenate([resid_recv[j] for j in range(hsplit)], axis=1)
    normed[...] = (block_resid * inverse * gain[m]).astype(bf16)

    bases = [q * cap // 8 * 8 for q in range(4)]
    for q in range(4):
        r = q % 2
        shift = q * cap - bases[q]
        at = lax.broadcasted_iota(jnp.int32, (lead, batch), 0)
        hit = (at == rank[r].astype(jnp.int32) + shift) & (named[r] > 0.0)
        slots_in[q] = jnp.dot(
            jnp.where(hit, 1.0, 0.0).astype(bf16), normed[...], preferred_element_type=f32
        ).astype(bf16)
    acc[...] = jnp.zeros_like(acc)

    def part_copy(to, slot):
        return remote(
            part_send.at[to],
            part_recv.at[slot],
            p_send.at[to],
            p_recv.at[slot],
            to * hsplit + h,
        )

    def gather(slot, q):
        return jnp.dot(
            slots_in[ORDER[q]], gu[slot, q], preferred_element_type=f32
        ), pl.ds(bases[ORDER[q]], lead)

    if chunks == 1:
        for q in range(4):
            gu_copy(0, q).wait()
            value, rows = gather(0, q)
            acc[rows, :] += value
        for to in range(MSPLIT):
            part_send[to] = acc[:packed, to * narrow : (to + 1) * narrow].astype(bf16)

        @pl.loop(1, MSPLIT)
        def _(d):
            part_copy(model(d), m).start()

    else:

        @pl.loop(0, MSPLIT)
        def _(i):
            slot = lax.rem(i, ring)
            to = model(MSPLIT - 1 - i)
            for q in range(4):
                gu_copy(i, q).wait()
                value, rows = gather(slot, q)
                acc[rows, :] += value

                @pl.when(i < MSPLIT - ring)
                def _():
                    gu_copy(i + ring, q).start()

            part_send[to] = acc[:packed, :].astype(bf16)
            acc[...] = jnp.zeros_like(acc)

            @pl.when(i < MSPLIT - 1)
            def _():
                part_copy(to, m).start()

    @pl.loop(1, MSPLIT)
    def _(d):
        part_copy(m, model(d)).wait_recv()

    part_recv[m] = part_send[m]
    acc[:packed, :narrow] = jnp.sum(part_recv[...].astype(f32), axis=0)
    a = acc[:hid_rows, :narrow]
    b = acc[2 * cap : 2 * cap + hid_rows, :narrow]
    hid_send[...] = (a / (1.0 + jnp.exp(-a)) * b).astype(bf16)

    def hid_copy(d, slot):
        return remote(
            hid_send, hid_recv.at[slot], h_send.at[d], h_recv.at[slot], model(d) * hsplit + h
        )

    def hid_relay(j, slot):
        return remote(
            hid_recv.at[slot],
            hid_recv.at[slot],
            h_relay.at[j],
            h_recv.at[slot],
            model(1) * hsplit + h,
        )

    hid_copy(1, m).start()

    @pl.loop(1, MSPLIT // 2)
    def _(j):
        hid_copy(MSPLIT - 2 * j, m).start()

    hid_recv[m] = hid_send[...]
    total[...] = jnp.zeros_like(total)

    def expert_sums(i, slot):
        for r in range(RESIDENT):
            down_copy(i, r).wait()
            total[r] += jnp.dot(hid_recv[slot], down[i, r], preferred_element_type=f32)

    @pl.loop(0, MSPLIT // 2)
    def _(j):
        even, odd = model(2 * j), model(2 * j + 1)

        @pl.when(j > 0)
        def _():
            hid_copy(2 * j, even).wait_recv()
            hid_relay(j, even).start()

        expert_sums(2 * j, even)
        hid_copy(1, odd).wait_recv()
        expert_sums(2 * j + 1, odd)

    whole = jnp.where(h == 0, 1.0, 0.0) * block_resid
    for r in range(RESIDENT):
        if batch > 32:
            whole = whole + jnp.dot(
                back[r], total[r], precision=lax.Precision.HIGHEST, preferred_element_type=f32
            )
        else:
            for n in range(r * cap, (r + 1) * cap):
                whole = whole + back[r][:, n : n + 1] * total[r, n : n + 1, :]
    resid_full[...] = whole

    @pl.loop(0, members)
    def _(j):
        final_send[j] = resid_full[pl.ds(j, 1), :]

    def final_copy(to, slot):
        return remote(
            final_send.at[to], final_recv.at[slot], f_send.at[to], f_recv.at[slot], to
        )

    @pl.loop(1, members)
    def _(d):
        final_copy(peer(d), me).start()

    final_recv[me] = final_send[me]

    @pl.loop(1, members)
    def _(d):
        final_copy(me, peer(d)).wait_recv()

    for j in range(MSPLIT):
        line = final_recv[j * hsplit]
        for k in range(1, hsplit):
            line = line + final_recv[j * hsplit + k]
        out[:, j * block : (j + 1) * block] = line.astype(bf16)

    @pl.loop(1, members)
    def _(d):
        to = peer(d)
        stream_copy(to, me).wait_send()
        sq_copy(to, me).wait_send()
        final_copy(to, me).wait_send()

    @pl.loop(1, hsplit)
    def _(d):
        resid_copy(mate(d), h).wait_send()

    @pl.loop(0, MSPLIT)
    def _(i):
        @pl.loop(1, hsplit)
        def _(d):
            attn_relay(i, mate(d), me).wait_send()

    @pl.loop(1, MSPLIT)
    def _(d):
        attn_copy(d, me).wait_send()
        part_copy(model(d), m).wait_send()

    hid_copy(1, m).wait_send()

    @pl.loop(1, MSPLIT // 2)
    def _(j):
        hid_copy(2 * j, m).wait_send()
        hid_relay(j, m).wait_send()

def on_device(
    stream_in,
    query,
    key_new,
    value_new,
    key_cache,
    value_cache,
    lengths,
    route_ids,
    route_scores,
    out_weight,
    norm_gain,
    gate_weight,
    up_weight,
    down_weight,
):
    f32, bf16 = jnp.float32, jnp.bfloat16
    members = lax.axis_size("gx")
    width = stream_in.shape[1]
    hsplit = members // MSPLIT
    cols = width // members
    block = width // MSPLIT
    batch = members
    hidden_cols = gate_weight.shape[2]
    narrow = hidden_cols // MSPLIT
    chunk = narrow if narrow % 128 == 0 else hidden_cols
    ring = min(RING, hidden_cols // chunk)
    vmem = pl.BlockSpec(memory_space=pltpu.VMEM)
    smem = pl.BlockSpec(memory_space=pltpu.SMEM)
    hbm = pl.BlockSpec(memory_space=pl.ANY)
    dma = pltpu.SemaphoreType.DMA
    rows = key_cache.shape[1]
    cap = batch * 5 // 8
    packed = 2 * RESIDENT * cap
    shifts = [q * cap % 8 for q in range(4)]
    lead = (cap + max(shifts) + 7) // 8 * 8
    hid_rows = (RESIDENT * cap + 7) // 8 * 8
    lanes = (batch + 127) // 128 * 128
    if narrow % 128 == 0 and 256 <= narrow <= block and NH * HS * cols == 4 * block * block:
        return large_call(
            stream_in,
            query,
            key_new,
            value_new,
            key_cache,
            value_cache,
            lengths,
            route_ids,
            route_scores,
            out_weight,
            norm_gain,
            gate_weight,
            up_weight,
            down_weight,
        )
    return pl.pallas_call(
        functools.partial(small_kernel, members),
        out_shape=jax.ShapeDtypeStruct((1, width), bf16),
        in_specs=[vmem] * 3 + [hbm] * 2 + [smem] * 3 + [vmem] * 2 + [hbm] * 4,
        out_specs=vmem,
        scratch_shapes=[
            pltpu.VMEM((rows, KVH * HS), bf16),
            pltpu.VMEM((rows, KVH * HS), bf16),
            dma((2,)),
            pltpu.VMEM((NH, HS), f32),
            pltpu.VMEM((2, KVH, HS), f32),
            pltpu.VMEM((members, 1, cols), f32),
            pltpu.VMEM(out_weight.shape, bf16),
            pltpu.VMEM((ring, 4, block, chunk), bf16),
            pltpu.VMEM((MSPLIT, RESIDENT, narrow, block), bf16),
            pltpu.VMEM((NH + PAD, HS), bf16),
            pltpu.VMEM((members, NH + PAD, HS), bf16),
            pltpu.VMEM((members * (NH + PAD), HS), f32),
            pltpu.VMEM((batch, NH * HS), bf16),
            pltpu.VMEM((members, 1, cols), f32),
            pltpu.VMEM((hsplit, batch, cols), f32),
            pltpu.VMEM((batch, cols), f32),
            pltpu.VMEM((1, lanes), f32),
            pltpu.VMEM((members, 1, lanes), f32),
            pltpu.VMEM((batch, block), bf16),
            pltpu.VMEM((4, lead, block), bf16),
            pltpu.VMEM((packed + 8, chunk), f32),
            pltpu.VMEM((MSPLIT, packed, narrow), bf16),
            pltpu.VMEM((MSPLIT, packed, narrow), bf16),
            pltpu.VMEM((hid_rows, narrow), bf16),
            pltpu.VMEM((MSPLIT, hid_rows, narrow), bf16),
            pltpu.VMEM((RESIDENT, hid_rows, block), f32),
            pltpu.VMEM((batch, block), f32),
            pltpu.VMEM((members, 1, block), f32),
            pltpu.VMEM((members, 1, block), f32),
            dma,
            dma((ring, 4)),
            dma((MSPLIT, RESIDENT)),
        ]
        + [dma((MSPLIT,)), dma((MSPLIT, hsplit))]
        + [dma((members,))] * 5
        + [dma((hsplit,))] * 2
        + [dma((MSPLIT,))] * 5
        + [dma((members,))] * 2,
        compiler_params=pltpu.CompilerParams(
            collective_id=0, has_side_effects=True, vmem_limit_bytes=67043328
        ),
    )(
        query,
        key_new,
        value_new,
        key_cache.reshape(rows, KVH * HS),
        value_cache.reshape(rows, KVH * HS),
        lengths,
        route_ids,
        route_scores,
        stream_in,
        norm_gain.reshape(MSPLIT, 1, block),
        out_weight,
        gate_weight,
        up_weight,
        down_weight,
    )

def solution(mesh):
    return jax.shard_map(
        on_device,
        mesh=mesh,
        in_specs=(
            P(("groups", "gx"), None),
            P(("groups", "gx"), None),
            P(("groups", "gx"), None),
            P(("groups", "gx"), None),
            P(("groups", "gx"), None, None),
            P(("groups", "gx"), None, None),
            P(("groups", "gx")),
            P(("groups", "gx"), None),
            P(("groups", "gx"), None),
            P(None, "gx"),
            P(),
            P(None, "gx", None),
            P(None, "gx", None),
            P(None, "gx", None),
        ),
        out_specs=P(("groups", "gx"), None),
        check_vma=False,
    )
```

```python
import functools

import jax
import jax.numpy as jnp
from jax import lax
from jax.experimental import pallas as pl
from jax.experimental.pallas import tpu as pltpu
from jax.sharding import PartitionSpec as P

NH = 64
KVH = 8
HS = 128
RESIDENT = 2
MSPLIT = 8
PAD = 16
RING = 3
ORDER = (0, 2, 1, 3)
MESH = pl.DeviceIdType.MESH

SLOTS = 28
CHUNKS = (
    (0, 0, 0),
    (0, 0, 1),
    (0, 0, 2),
    (0, 0, 3),
    (0, 1, 0),
    (0, 1, 1),
    (0, 1, 2),
    (0, 1, 3),
    (1, 0, 0),
    (1, 0, 1),
    (1, 0, 2),
    (1, 0, 3),
    (1, 1, 0),
    (1, 1, 1),
    (1, 1, 2),
    (1, 1, 3),
)
SPREAD = (0, 2, 6, 4, 1, 3, 7, 5)

def large_kernel(
    members,
    query_hbm,
    key_new_hbm,
    value_new_hbm,
    key_hbm,
    value_hbm,
    lengths_hbm,
    ids_hbm,
    scores_hbm,
    stream_hbm,
    gain_hbm,
    out_weight,
    gate_weight,
    up_weight,
    down_weight,
    out,
    lengths,
    route_ids,
    route_scores,
    query,
    fresh_kv,
    stream,
    gain,
    cache,
    in_sem,
    heads,
    own_rows,
    stream_rows,
    stream_recv,
    stream_flat,
    pool,
    attn_send,
    attn_recv,
    attn_wide,
    attn_rows,
    resid_keep,
    y_send,
    y_recv,
    sq_send,
    sq_recv,
    slots_in,
    acc_a,
    acc_b,
    px_send_a,
    px_send_b,
    px_recv_a,
    px_recv_b,
    pz_send_a,
    pz_send_b,
    pz_recv_a,
    pz_recv_b,
    hid_send_a,
    hid_send_b,
    hid_recv_a,
    hid_recv_b,
    total,
    final_flat,
    final_send,
    final_recv,
    wo_sem,
    gu_sem,
    down_sem,
    a_send,
    a_relay,
    a_recv,
    a_mate,
    s_send,
    s_recv,
    q_send,
    q_recv,
    r_send,
    r_recv,
    x_send,
    x_recv,
    z_send,
    z_recv,
    h_send,
    h_relay,
    h_recv,
    f_send,
    f_recv,
):
    f32, bf16 = jnp.float32, jnp.bfloat16
    hsplit = members // MSPLIT
    me = lax.axis_index("gx")
    m = me // hsplit
    h = lax.rem(me, hsplit)
    batch = members
    cols = y_send.shape[1]
    width = cols * members
    block = width // MSPLIT
    group = NH // KVH
    acc, px_send, px_recv = (acc_a, acc_b), (px_send_a, px_send_b), (px_recv_a, px_recv_b)
    pz_send, pz_recv = (pz_send_a, pz_send_b), (pz_recv_a, pz_recv_b)
    hid_send, hid_recv = (hid_send_a, hid_send_b), (hid_recv_a, hid_recv_b)
    wide = (acc_a.shape[2], acc_b.shape[2])
    first = (0, wide[0])
    chunk = wide[0] + wide[1]
    cap = batch * 5 // 8
    packed = px_send_a.shape[1]
    hid_rows = hid_send_a.shape[0]
    lead = slots_in.shape[1] // 2
    lanes = sq_send.shape[1]
    half = MSPLIT // 2
    side = block // cols
    pieces = NH * HS // block

    def peer(d):
        return lax.rem(me + d, members)

    def model(d):
        to = 0
        for b in (1, 2, 4):
            if isinstance(d, int):
                bit = lax.rem(lax.div(m, b), 2)
                to = to + (1 - bit if d // b % 2 else bit) * b
            else:
                to = to + lax.rem(lax.div(m, b) + lax.div(d, b), 2) * b
        return to

    def mate(d):
        return lax.rem(h + d, hsplit)

    def far(i):
        d = members - i
        return model(d // hsplit) * hsplit + mate(d % hsplit)

    def settle(ref, sem):
        pltpu.make_async_copy(ref, ref, sem).wait()

    def remote(src, dst, send, recv, device):
        return pltpu.make_async_remote_copy(
            src_ref=src,
            dst_ref=dst,
            send_sem=send,
            recv_sem=recv,
            device_id={"gx": device},
            device_id_type=MESH,
        )

    barrier = pltpu.get_barrier_semaphore()
    key_cache, value_cache = cache.at[0], cache.at[1]
    sources = (
        ((query_hbm, query),),
        ((key_hbm, key_cache), (value_hbm, value_cache)),
        ((key_new_hbm, fresh_kv.at[0]), (value_new_hbm, fresh_kv.at[1])),
        ((lengths_hbm, lengths),),
        ((ids_hbm, route_ids),),
        ((scores_hbm, route_scores),),
        ((stream_hbm, stream),),
        ((gain_hbm.at[me], gain),),
    )
    for k, pairs in enumerate(sources):
        for src, dst in pairs:
            pltpu.make_async_copy(src, dst, in_sem.at[k]).start()

    @pl.loop(1, members)
    def _(d):
        pl.semaphore_signal(barrier, inc=1, device_id={"gx": peer(d)}, device_id_type=MESH)

    def wo_copy(k):
        return pltpu.make_async_copy(
            out_weight.at[pl.ds(k * block, block), :],
            pool.at[k // side, :, pl.ds(k % side * cols, cols)],
            wo_sem.at[0],
        )

    def gu_slot(c):
        return (half + 2 * c) % SLOTS

    def gu_start(c):
        p, z, i = CHUNKS[c]
        at = pl.multiple_of(model(2 * (half - 1 - i) + 1 - z) * chunk + first[p], 128)
        for q in range(4):
            r, w = q // 2, (gate_weight, up_weight)[q % 2]
            pltpu.make_async_copy(
                w.at[r, :, pl.ds(at, wide[p])],
                pool.at[gu_slot(c) + r, :, pl.ds(q % 2 * wide[p], wide[p])],
                gu_sem.at[c],
            ).start()

    def arrived(c):
        p = CHUNKS[c][0]
        settle(pool.at[pl.ds(gu_slot(c), 2), :, pl.ds(0, 2 * wide[p])], gu_sem.at[c])

    def down_slot(p, k):
        return (half + (4 + p) * MSPLIT + k) % SLOTS

    def down_start(t):
        p, k = t // MSPLIT, t % MSPLIT
        at = pl.multiple_of(model(SPREAD[k]) * chunk + first[p], 16)
        for r in range(RESIDENT):
            pltpu.make_async_copy(
                down_weight.at[r, pl.ds(at, wide[p]), :],
                pool.at[down_slot(p, k), pl.ds(r * wide[p], wide[p]), :],
                down_sem.at[t],
            ).start()

    def refill(c):
        if c < 2:
            gu_start(2 * MSPLIT - 2 + c)
        elif c < MSPLIT + 2:
            down_start(2 * c - 4)
            down_start(2 * c - 3)

    for k in range(pieces):
        wo_copy(k).start()

    scale = HS ** (-0.5)
    settle(query, in_sem.at[0])
    for n in range(NH):
        heads[n : n + 1, :] = query[:, n * HS : (n + 1) * HS].astype(f32)

    for k, ref in enumerate(
        (cache, fresh_kv, lengths, route_ids, route_scores, stream, gain), start=1
    ):
        settle(ref, in_sem.at[k])

    for g in range(KVH):
        own_rows[0, g : g + 1, :] = fresh_kv[0, :, g * HS : (g + 1) * HS].astype(f32)
        own_rows[1, g : g + 1, :] = fresh_kv[1, :, g * HS : (g + 1) * HS].astype(f32)
    wide_q = heads[...]
    s = jnp.concatenate(
        [
            lax.dot_general(
                wide_q[g * group : (g + 1) * group].astype(bf16),
                key_cache[:, g * HS : (g + 1) * HS],
                (((1,), (1,)), ((), ())),
                preferred_element_type=f32,
            )
            for g in range(KVH)
        ],
        axis=0,
    )
    s = s * scale
    live = lax.broadcasted_iota(jnp.int32, s.shape, 1) < lengths[0]
    s = jnp.where(live, s, -1e30)
    k_own, v_own = own_rows[0], own_rows[1]
    spread = lambda v: jnp.concatenate(
        [jnp.broadcast_to(v[g : g + 1], (group, HS)) for g in range(KVH)], axis=0
    )
    own = jnp.sum(wide_q * spread(k_own), axis=-1, keepdims=True) * scale
    top = jnp.maximum(jnp.max(s, axis=-1, keepdims=True), own)
    e_cache = jnp.exp(s - top)
    e_own = jnp.exp(own - top)
    norm = jnp.sum(e_cache, axis=-1, keepdims=True) + e_own
    p = e_cache / norm
    p_own = (e_own / norm).astype(bf16).astype(f32)
    mixed = jnp.concatenate(
        [
            jnp.dot(
                p[g * group : (g + 1) * group].astype(bf16),
                value_cache[:, g * HS : (g + 1) * HS],
                preferred_element_type=f32,
            )
            for g in range(KVH)
        ],
        axis=0,
    )
    mixed = mixed + p_own * spread(v_own)
    attn_send[...] = mixed.astype(bf16)
    spot = lax.broadcasted_iota(jnp.int32, (1, HS), 1)
    full = lambda v: jnp.full((1, HS), v)
    s0, s1 = full(route_scores[0, 0]), full(route_scores[0, 1])
    i0, i1 = full(route_ids[0, 0]), full(route_ids[0, 1])
    peak = jnp.maximum(s0, s1)
    x0, x1 = jnp.exp(s0 - peak), jnp.exp(s1 - peak)
    pick = jnp.where(i0 == spot, x0 / (x0 + x1), 0.0) + jnp.where(i1 == spot, x1 / (x0 + x1), 0.0)
    pick = pick.astype(bf16).astype(f32)
    for j in range(members):
        stream_rows[j, :, :cols] = stream[:, j * cols : (j + 1) * cols].astype(f32)
        stream_rows[j, :, cols:] = pick

    pl.semaphore_wait(barrier, members - 1)

    def attn_copy(d, slot):
        return remote(
            attn_send, attn_recv.at[slot], a_send.at[0], a_recv.at[d], model(d) * hsplit + h
        )

    def attn_relay(d, t, slot):
        src = attn_send if isinstance(d, int) else attn_recv.at[slot]
        return remote(
            src, attn_recv.at[slot], a_relay.at[0], a_mate.at[0], m * hsplit + t
        )

    def stream_copy(to, slot):
        return remote(
            stream_rows.at[to], stream_recv.at[slot], s_send.at[0], s_recv.at[0], to
        )

    @pl.loop(0, MSPLIT - 1)
    def _(i):
        attn_copy(MSPLIT - 1 - i, me).start()

    @pl.loop(1, hsplit)
    def _(d):
        attn_relay(0, mate(d), me).start()

    @pl.loop(1, members)
    def _(d):
        stream_copy(peer(d), me).start()

    def widen(slot, rows):
        at = pl.multiple_of(slot * NH, NH)
        attn_wide[pl.ds(at, NH), :] = rows.astype(f32)

    for c in range(2 * MSPLIT - half):
        gu_start(c)

    widen(me, attn_send[...])
    stream_recv[me] = stream_rows[me]

    @pl.loop(1, MSPLIT)
    def _(i):
        slot = model(i) * hsplit + h
        attn_copy(i, slot).wait_recv()

        @pl.loop(1, hsplit)
        def _(d):
            attn_relay(i, mate(d), slot).start()

        widen(slot, attn_recv[slot])

    settle(attn_recv.at[pl.ds(0, MSPLIT * (hsplit - 1))], a_mate.at[0])

    @pl.loop(0, MSPLIT)
    def _(i):
        @pl.loop(1, hsplit)
        def _(d):
            slot = model(i) * hsplit + mate(d)
            widen(slot, attn_recv[slot])

    settle(pool.at[pl.ds(0, half)], wo_sem.at[0])

    settle(stream_recv.at[pl.ds(0, members - 1)], s_recv.at[0])

    for j in range(members):
        stream_flat[j : j + 1, :] = stream_recv[j]

    for n in range(NH):
        attn_rows[:, n * HS : (n + 1) * HS] = attn_wide[pl.ds(n, batch, stride=NH), :].astype(bf16)

    proj = jnp.zeros((batch, cols), f32)
    for k in range(pieces):
        proj = proj + jnp.dot(
            attn_rows[:, k * block : (k + 1) * block],
            pool[k // side, :, k % side * cols : (k % side + 1) * cols],
            preferred_element_type=f32,
        )
    gu_start(2 * MSPLIT - 4)
    gu_start(2 * MSPLIT - 3)

    resid = stream_flat[:, :cols] + proj.astype(bf16).astype(f32)
    resid_keep[...] = resid
    y_send[...] = (resid * gain[...]).astype(bf16)

    def y_copy(to, slot):
        return remote(y_send, y_recv.at[slot], r_send.at[0], r_recv.at[0], m * hsplit + to)

    @pl.loop(1, hsplit)
    def _(d):
        y_copy(mate(d), h).start()

    sub_w = lax.broadcasted_iota(jnp.int32, (batch, lanes), 0)
    lane_w = lax.broadcasted_iota(jnp.int32, (batch, lanes), 1)
    squares = jnp.sum(resid * resid, axis=-1, keepdims=True)
    sq_send[...] = jnp.sum(jnp.where(sub_w == lane_w, squares, 0.0), axis=0, keepdims=True)

    def sq_copy(to, slot):
        return remote(sq_send, sq_recv.at[slot], q_send.at[0], q_recv.at[0], to)

    @pl.loop(1, members)
    def _(d):
        sq_copy(peer(d), me).start()

    sq_recv[me] = sq_send[...]
    y_recv[h] = y_send[...]
    scales = [stream_flat[:, cols + r : cols + r + 1] for r in range(RESIDENT)]
    sub = lax.broadcasted_iota(jnp.int32, (batch, batch), 0)
    lane = lax.broadcasted_iota(jnp.int32, (batch, batch), 1)
    named, rank, back = [], [], []
    for r in range(RESIDENT):
        col = jnp.where(scales[r] > 0.0, 1.0, 0.0)
        row = jnp.sum(jnp.where(sub == lane, col, 0.0), axis=0, keepdims=True)
        named.append(row)
        rank.append(jnp.sum(jnp.where(sub < lane, col, 0.0), axis=0, keepdims=True))
        place = jnp.sum(jnp.where(lane < sub, row, 0.0), axis=1, keepdims=True)
        at = lax.broadcasted_iota(jnp.int32, (batch, hid_rows), 1)
        hit = at == place.astype(jnp.int32) + r * cap
        back.append(jnp.where(hit, scales[r], 0.0))

    settle(y_recv.at[pl.ds(0, hsplit - 1)], r_recv.at[0])

    y = jnp.concatenate([y_recv[j] for j in range(hsplit)], axis=1)
    bases = [q * cap // 8 * 8 for q in range(4)]
    for q in range(4):
        r = q % 2
        shift = q * cap - bases[q]
        at = lax.broadcasted_iota(jnp.int32, (lead, batch), 0)
        hit = (at == rank[r].astype(jnp.int32) + shift) & (named[r] > 0.0)
        slots_in[r, q // 2 * lead : (q // 2 + 1) * lead, :] = jnp.dot(
            jnp.where(hit, 1.0, 0.0).astype(bf16), y, preferred_element_type=f32
        ).astype(bf16)

    def px_copy(p, i):
        return remote(
            px_send[p].at[i],
            px_recv[p].at[i],
            x_send.at[p],
            x_recv.at[p, i],
            model(1) * hsplit + h,
        )

    def pz_copy(p, j):
        return remote(
            pz_send[p].at[j],
            pz_recv[p].at[j],
            z_send.at[p],
            z_recv.at[p],
            model(2 * (half - 1 - j)) * hsplit + h,
        )

    def sums(c):
        p = CHUNKS[c][0]
        w = wide[p]
        slabs = [[] for _ in range(acc[p].shape[1] // 8)]
        for r in range(RESIDENT):
            where = gu_slot(c) + r
            values = [
                jnp.dot(
                    slots_in[r, q * lead : (q + 1) * lead, :],
                    pool[where, :, q * w : (q + 1) * w],
                    preferred_element_type=f32,
                )
                for q in range(2)
            ]
            for q in range(2):
                for k in range(lead // 8):
                    slabs[bases[2 * q + r] // 8 + k].append(values[q][k * 8 : (k + 1) * 8])
        empty = jnp.zeros((8, w), f32)
        return jnp.concatenate([sum(slab[1:], slab[0]) if slab else empty for slab in slabs], axis=0)

    def gate_up(*cs):
        for c in cs:
            arrived(c)
        for c in cs:
            p, z, i = CHUNKS[c]
            if z:
                acc[p][i % 2] = sums(c)
            else:
                px_send[p][i] = sums(c)[:packed].astype(bf16)
                px_copy(p, i).start()
        for c in cs:
            refill(c)
        for c in cs:
            p, z, i = CHUNKS[c]
            if z:
                px_copy(p, i).wait_recv()
                acc[p][i % 2, :packed, :] += px_recv[p][i].astype(f32)
                if i < half - 1:
                    pz_send[p][i] = acc[p][i % 2, :packed, :].astype(bf16)
                    pz_copy(p, i).start()

    def hid_group(p, d):
        if p == 0:
            return d // 2 if d % 2 == 0 else 0
        return (0, 0, 0, 0, 1, 1, 2, 2)[SPREAD.index(d)]

    def hid_copy(p, d, slot):
        return remote(
            hid_send[p],
            hid_recv[p].at[slot],
            h_send.at[p],
            h_recv.at[p, hid_group(p, d)],
            model(d) * hsplit + h,
        )

    def hid_relay(p, j, slot):
        return remote(
            hid_recv[p].at[slot],
            hid_recv[p].at[slot],
            h_relay.at[0],
            h_recv.at[p, 0],
            model(1) * hsplit + h,
        )

    def finish(p, last):
        settle(pz_recv[p], z_recv.at[p])
        for j in range(half - 1):
            acc[p][last, :packed, :] += pz_recv[p][j].astype(f32)
        a = acc[p][last, :hid_rows, :] * scaled
        b = acc[p][last, 2 * cap : 2 * cap + hid_rows, :] * scaled
        hid_send[p][...] = (a / (1.0 + jnp.exp(-a)) * b).astype(bf16)
        for d in (1, *SPREAD[1:half]) if p == 0 else (6, 4, 2, 1, 3, 7, 5):
            hid_copy(p, d, m).start()
        hid_recv[p][m] = hid_send[p][...]

    def relays(p):
        for k in range(1, half):
            slot = model(SPREAD[k])
            hid_copy(p, SPREAD[k], slot).wait_recv()
            hid_relay(p, k, slot).start()

    def down(p, ks, fresh=False):
        groups = {}
        for k in ks:
            if k >= half or k and p:
                groups.setdefault(hid_group(p, SPREAD[k]), []).append(k)
            settle(pool.at[down_slot(p, k), pl.ds(0, 2 * wide[p]), :], down_sem.at[p * MSPLIT + k])
        for g, members_of in groups.items():
            settle(hid_recv[p].at[pl.ds(0, len(members_of))], h_recv.at[p, g])
        line = lax.broadcasted_iota(jnp.int32, (hid_rows, wide[p]), 0)
        value = None if fresh else total[...]
        for k in ks:
            rows = hid_recv[p][model(SPREAD[k])].astype(f32)
            split = [
                jnp.where((line >= r * cap) & (line < (r + 1) * cap), rows, 0.0).astype(bf16)
                for r in range(RESIDENT)
            ]
            term = jnp.dot(
                jnp.concatenate(split, axis=1),
                pool[down_slot(p, k), : RESIDENT * wide[p], :],
                preferred_element_type=f32,
            )
            value = term if value is None else value + term
        total[...] = value

    gate_up(0)
    gate_up(1)
    gate_up(2)
    gate_up(3)

    gate_up(4)
    gate_up(5, 6)
    gate_up(7)

    gate_up(8, 9)
    gate_up(10, 11)

    settle(sq_recv.at[pl.ds(0, members - 1)], q_recv.at[0])

    power = jnp.sum(sq_recv[...], axis=0)[:, :batch] * (1.0 / width)
    inverse = lax.rsqrt(power + 1e-05)
    at = lax.broadcasted_iota(jnp.int32, (hid_rows, batch), 0)
    scaled = jnp.zeros((hid_rows, 1), f32)
    for r in range(RESIDENT):
        hit = (at == rank[r].astype(jnp.int32) + r * cap) & (named[r] > 0.0)
        scaled = scaled + jnp.sum(jnp.where(hit, inverse, 0.0), axis=1, keepdims=True)

    finish(0, 1)

    gate_up(12)
    gate_up(13)
    gate_up(14)
    gate_up(15)

    down(0, (0,), True)

    relays(0)

    down(0, range(1, half))

    finish(1, 1)

    down(1, (0,))

    down(0, range(half, MSPLIT))

    down(1, range(1, half))

    down(1, (4, 5))

    down(1, (6, 7))

    resid = resid_keep[...]
    whole = jnp.concatenate([jnp.where(h == j, resid, 0.0) for j in range(hsplit)], axis=1)
    mix = sum(back[1:], back[0])
    for n in range(RESIDENT * cap):
        whole = whole + mix[:, n : n + 1] * total[n : n + 1, :]
    tiles = block // HS
    for t in range(tiles):
        final_flat[t * batch : (t + 1) * batch, :] = whole[:, t * HS : (t + 1) * HS]
    for j in range(members):
        final_send[j] = final_flat[pl.ds(j, tiles, stride=batch), :].astype(bf16)

    def final_copy(to, slot):
        return remote(
            final_send.at[to], final_recv.at[slot], f_send.at[0], f_recv.at[0], to
        )

    for i in range(1, members):
        final_copy(far(i), me).start()

    final_recv[me] = final_send[me]

    settle(stream_recv.at[pl.ds(0, members - 1)], s_send.at[0])
    settle(sq_recv.at[pl.ds(0, members - 1)], q_send.at[0])
    settle(y_recv.at[pl.ds(0, hsplit - 1)], r_send.at[0])
    settle(attn_recv.at[pl.ds(0, MSPLIT * (hsplit - 1))], a_relay.at[0])
    settle(attn_recv.at[pl.ds(0, MSPLIT - 1)], a_send.at[0])
    for p in range(2):
        settle(px_recv[p], x_send.at[p])
        settle(pz_recv[p], z_send.at[p])
        settle(hid_recv[p].at[pl.ds(0, MSPLIT - 1 if p else half)], h_send.at[p])
    settle(hid_recv[0].at[pl.ds(0, half - 1)], h_relay.at[0])

    settle(final_recv.at[pl.ds(0, members - 1)], f_recv.at[0])

    for j in range(MSPLIT):
        line = final_recv[j * hsplit].astype(f32)
        for k in range(1, hsplit):
            line = line + final_recv[j * hsplit + k].astype(f32)
        out[j * tiles : (j + 1) * tiles, :] = line.astype(bf16)

    settle(final_recv.at[pl.ds(0, members - 1)], f_send.at[0])

def large_call(
    stream_in,
    query,
    key_new,
    value_new,
    key_cache,
    value_cache,
    lengths,
    route_ids,
    route_scores,
    out_weight,
    norm_gain,
    gate_weight,
    up_weight,
    down_weight,
):
    f32, bf16 = jnp.float32, jnp.bfloat16
    members = lax.axis_size("gx")
    width = stream_in.shape[1]
    hsplit = members // MSPLIT
    cols = width // members
    block = width // MSPLIT
    batch = members
    narrow = gate_weight.shape[2] // MSPLIT
    vmem = pl.BlockSpec(memory_space=pltpu.VMEM)
    hbm = pl.BlockSpec(memory_space=pl.ANY)
    dma = pltpu.SemaphoreType.DMA
    rows = key_cache.shape[1]
    cap = batch * 5 // 8
    packed = 2 * RESIDENT * cap
    shifts = [q * cap % 8 for q in range(4)]
    lead = (cap + max(shifts) + 7) // 8 * 8
    hid_rows = (RESIDENT * cap + 7) // 8 * 8
    lanes = (batch + 127) // 128 * 128
    half = MSPLIT // 2
    tiles = block // HS
    wide = [(narrow // 128 + 1) // 2 * 128]
    wide.append(narrow - wide[0])
    result = pl.pallas_call(
        functools.partial(large_kernel, members),
        out_shape=pltpu.VMEM((width // HS, HS), bf16),
        in_specs=[hbm] * 14,
        out_specs=vmem,
        scratch_shapes=[
            pltpu.SMEM(lengths.shape, jnp.int32),
            pltpu.SMEM(route_ids.shape, jnp.int32),
            pltpu.SMEM(route_scores.shape, f32),
            pltpu.VMEM((1, NH * HS), bf16),
            pltpu.VMEM((2, 1, KVH * HS), bf16),
            pltpu.VMEM((1, width), bf16),
            pltpu.VMEM((1, cols), f32),
            pltpu.VMEM((2, rows, KVH * HS), bf16),
            dma((8,)),
            pltpu.VMEM((NH, HS), f32),
            pltpu.VMEM((2, KVH, HS), f32),
            pltpu.VMEM((members, 1, cols + HS), f32),
            pltpu.VMEM((members, 1, cols + HS), f32),
            pltpu.VMEM((batch, cols + HS), f32),
            pltpu.VMEM((SLOTS, block, block), bf16),
            pltpu.VMEM((NH, HS), bf16),
            pltpu.VMEM((members, NH, HS), bf16),
            pltpu.VMEM((members * NH, HS), f32),
            pltpu.VMEM((batch, NH * HS), bf16),
            pltpu.VMEM((batch, cols), f32),
            pltpu.VMEM((batch, cols), bf16),
            pltpu.VMEM((hsplit, batch, cols), bf16),
            pltpu.VMEM((1, lanes), f32),
            pltpu.VMEM((members, 1, lanes), f32),
            pltpu.VMEM((RESIDENT, 2 * lead, block), bf16),
            *[pltpu.VMEM((2, packed + 8, w), f32) for w in wide],
            *[pltpu.VMEM((half, packed, w), bf16) for w in wide],
            *[pltpu.VMEM((half, packed, w), bf16) for w in wide],
            *[pltpu.VMEM((half - 1, packed, w), bf16) for w in wide],
            *[pltpu.VMEM((half - 1, packed, w), bf16) for w in wide],
            *[pltpu.VMEM((hid_rows, w), bf16) for w in wide],
            *[pltpu.VMEM((MSPLIT, hid_rows, w), bf16) for w in wide],
            pltpu.VMEM((hid_rows, block), f32),
            pltpu.VMEM((tiles * batch, HS), f32),
            pltpu.VMEM((members, tiles, HS), bf16),
            pltpu.VMEM((members, tiles, HS), bf16),
            dma((1,)),
            dma((2 * MSPLIT,)),
            dma((2 * MSPLIT,)),
        ]
        + [dma((1,))] * 2
        + [dma((MSPLIT,))]
        + [dma((1,))] * 7
        + [dma((2,)), dma((2, half))]
        + [dma((2,))] * 3
        + [dma((1,)), dma((2, half))]
        + [dma((1,))] * 2,
        compiler_params=pltpu.CompilerParams(
            collective_id=0, has_side_effects=True, vmem_limit_bytes=66000000
        ),
    )(
        query,
        key_new,
        value_new,
        key_cache.reshape(rows, KVH * HS),
        value_cache.reshape(rows, KVH * HS),
        lengths,
        route_ids,
        route_scores,
        stream_in,
        norm_gain.reshape(members, 1, cols),
        out_weight,
        gate_weight,
        up_weight,
        down_weight,
    )
    return result.reshape(1, width)

def small_kernel(
    members,
    query,
    key_new,
    value_new,
    key_hbm,
    value_hbm,
    lengths,
    route_ids,
    route_scores,
    stream,
    gain,
    out_weight,
    gate_weight,
    up_weight,
    down_weight,
    out,
    key_cache,
    value_cache,
    cache_sem,
    heads,
    own_rows,
    stream_rows,
    wo,
    gu,
    down,
    attn_send,
    attn_recv,
    attn_wide,
    attn_rows,
    stream_recv,
    resid_recv,
    resid_send,
    sq_send,
    sq_recv,
    normed,
    slots_in,
    acc,
    part_send,
    part_recv,
    hid_send,
    hid_recv,
    total,
    resid_full,
    final_send,
    final_recv,
    wo_sem,
    gu_sem,
    down_sem,
    a_send,
    a_relay,
    a_recv,
    s_send,
    s_recv,
    q_send,
    q_recv,
    r_send,
    r_recv,
    p_send,
    p_recv,
    h_send,
    h_relay,
    h_recv,
    f_send,
    f_recv,
):
    f32, bf16 = jnp.float32, jnp.bfloat16
    hsplit = members // MSPLIT
    me = lax.axis_index("gx")
    m = me // hsplit
    h = lax.rem(me, hsplit)
    batch = members
    cols = wo.shape[1]
    width = cols * members
    block = width // MSPLIT
    group = NH // KVH
    chunk = gu.shape[3]
    chunks = gate_weight.shape[2] // chunk
    narrow = part_send.shape[2]
    cap = batch * 5 // 8
    packed = part_send.shape[1]
    hid_rows = hid_send.shape[0]
    lead = slots_in.shape[1]
    lanes = sq_send.shape[1]
    ring = gu.shape[0]

    def peer(d):
        return lax.rem(me + d, members)

    def model(d):
        d = jnp.asarray(d, jnp.int32)
        to = 0
        for b in (1, 2, 4):
            to = to + lax.rem(lax.div(m, b) + lax.div(d, b), 2) * b
        return to

    def mate(d):
        return lax.rem(h + d, hsplit)

    def remote(src, dst, send, recv, device):
        return pltpu.make_async_remote_copy(
            src_ref=src,
            dst_ref=dst,
            send_sem=send,
            recv_sem=recv,
            device_id={"gx": device},
            device_id_type=MESH,
        )

    barrier = pltpu.get_barrier_semaphore()

    @pl.loop(1, members)
    def _(d):
        pl.semaphore_signal(barrier, inc=1, device_id={"gx": peer(d)}, device_id_type=MESH)

    key_copy = pltpu.make_async_copy(key_hbm, key_cache, cache_sem.at[0])
    value_copy = pltpu.make_async_copy(value_hbm, value_cache, cache_sem.at[1])
    key_copy.start()
    value_copy.start()
    wo_copy = pltpu.make_async_copy(out_weight, wo, wo_sem)
    wo_copy.start()

    def gu_copy(i, q):
        r, w = q // 2, (gate_weight, up_weight)[q % 2]
        if chunks == 1:
            src = w.at[r]
        else:
            at = pl.multiple_of(model(MSPLIT - 1 - i) * chunk, 128)
            src = w.at[r, :, pl.ds(at, chunk)]
        slot = lax.rem(i, ring)
        return pltpu.make_async_copy(src, gu.at[slot, q], gu_sem.at[slot, q])

    def down_copy(i, r):
        at = pl.multiple_of(model(i) * narrow, 16)
        return pltpu.make_async_copy(
            down_weight.at[r, pl.ds(at, narrow), :], down.at[i, r], down_sem.at[i, r]
        )

    @pl.loop(0, ring)
    def _(i):
        for q in range(4):
            gu_copy(i, q).start()

    @pl.loop(0, MSPLIT)
    def _(i):
        for r in range(RESIDENT):
            down_copy(i, r).start()

    scale = HS ** (-0.5)
    for n in range(NH):
        heads[n : n + 1, :] = query[:, n * HS : (n + 1) * HS].astype(f32)
    for g in range(KVH):
        own_rows[0, g : g + 1, :] = key_new[:, g * HS : (g + 1) * HS].astype(f32)
        own_rows[1, g : g + 1, :] = value_new[:, g * HS : (g + 1) * HS].astype(f32)
    for j in range(members):
        stream_rows[j] = stream[:, j * cols : (j + 1) * cols].astype(f32)
    wide_q = heads[...]
    key_copy.wait()
    value_copy.wait()
    s = jnp.concatenate(
        [
            lax.dot_general(
                wide_q[g * group : (g + 1) * group].astype(bf16),
                key_cache[:, g * HS : (g + 1) * HS],
                (((1,), (1,)), ((), ())),
                preferred_element_type=f32,
            )
            for g in range(KVH)
        ],
        axis=0,
    )
    s = s * scale
    live = lax.broadcasted_iota(jnp.int32, s.shape, 1) < lengths[0]
    s = jnp.where(live, s, -1e30)
    k_own, v_own = own_rows[0], own_rows[1]
    spread = lambda v: jnp.concatenate(
        [jnp.broadcast_to(v[g : g + 1], (group, HS)) for g in range(KVH)], axis=0
    )
    own = jnp.sum(wide_q * spread(k_own), axis=-1, keepdims=True) * scale
    top = jnp.maximum(jnp.max(s, axis=-1, keepdims=True), own)
    e_cache = jnp.exp(s - top)
    e_own = jnp.exp(own - top)
    norm = jnp.sum(e_cache, axis=-1, keepdims=True) + e_own
    p = e_cache / norm
    p_own = (e_own / norm).astype(bf16).astype(f32)
    mixed = jnp.concatenate(
        [
            jnp.dot(
                p[g * group : (g + 1) * group].astype(bf16),
                value_cache[:, g * HS : (g + 1) * HS],
                preferred_element_type=f32,
            )
            for g in range(KVH)
        ],
        axis=0,
    )
    mixed = mixed + p_own * spread(v_own)
    attn_send[:NH, :] = mixed.astype(bf16)
    full = lambda v: jnp.full((PAD, HS), v)
    s0, s1 = full(route_scores[0, 0]), full(route_scores[0, 1])
    i0, i1 = full(route_ids[0, 0]), full(route_ids[0, 1])
    peak = jnp.maximum(s0, s1)
    x0, x1 = jnp.exp(s0 - peak), jnp.exp(s1 - peak)
    row = lax.broadcasted_iota(jnp.int32, (PAD, HS), 0)
    pick = jnp.where(i0 == row, x0 / (x0 + x1), 0.0) + jnp.where(i1 == row, x1 / (x0 + x1), 0.0)
    attn_send[NH:, :] = pick.astype(bf16)

    pl.semaphore_wait(barrier, members - 1)

    def attn_copy(d, slot):
        return remote(
            attn_send, attn_recv.at[slot], a_send.at[d], a_recv.at[slot], model(d) * hsplit + h
        )

    def attn_relay(d, t, slot):
        src = attn_send if isinstance(d, int) else attn_recv.at[slot]
        return remote(
            src, attn_recv.at[slot], a_relay.at[d, t], a_recv.at[slot], m * hsplit + t
        )

    def stream_copy(to, slot):
        return remote(
            stream_rows.at[to], stream_recv.at[slot], s_send.at[to], s_recv.at[slot], to
        )

    @pl.loop(0, MSPLIT - 1)
    def _(i):
        attn_copy(MSPLIT - 1 - i, me).start()

    @pl.loop(1, hsplit)
    def _(d):
        attn_relay(0, mate(d), me).start()

    @pl.loop(1, members)
    def _(d):
        stream_copy(peer(d), me).start()

    attn_recv[me] = attn_send[...]
    stream_recv[me] = stream_rows[me]

    @pl.loop(1, MSPLIT)
    def _(i):
        slot = model(i) * hsplit + h
        attn_copy(i, slot).wait_recv()

        @pl.loop(1, hsplit)
        def _(d):
            attn_relay(i, mate(d), slot).start()

    @pl.loop(0, MSPLIT)
    def _(i):
        @pl.loop(1, hsplit)
        def _(d):
            attn_copy(i, model(i) * hsplit + mate(d)).wait_recv()

    stride = NH + PAD

    @pl.loop(0, members)
    def _(j):
        attn_wide[pl.ds(j * stride, stride), :] = attn_recv[j].astype(f32)

    for n in range(NH):
        attn_rows[:, n * HS : (n + 1) * HS] = attn_wide[pl.ds(n, batch, stride=stride), :].astype(
            bf16
        )
    scales = [attn_wide[pl.ds(NH + r, batch, stride=stride), :][:, :1] for r in range(RESIDENT)]

    sub = lax.broadcasted_iota(jnp.int32, (batch, batch), 0)
    lane = lax.broadcasted_iota(jnp.int32, (batch, batch), 1)
    named, rank, back = [], [], []
    for r in range(RESIDENT):
        col = jnp.where(scales[r] > 0.0, 1.0, 0.0)
        row = jnp.sum(jnp.where(sub == lane, col, 0.0), axis=0, keepdims=True)
        named.append(row)
        rank.append(jnp.sum(jnp.where(sub < lane, col, 0.0), axis=0, keepdims=True))
        place = jnp.sum(jnp.where(lane < sub, row, 0.0), axis=1, keepdims=True)
        at = lax.broadcasted_iota(jnp.int32, (batch, hid_rows), 1)
        hit = at == place.astype(jnp.int32) + r * cap
        back.append(jnp.where(hit, scales[r], 0.0))

    wo_copy.wait()
    proj = jnp.dot(attn_rows[...], wo[...], preferred_element_type=f32).astype(bf16)

    @pl.loop(1, members)
    def _(d):
        stream_copy(me, peer(d)).wait_recv()

    @pl.loop(0, members)
    def _(j):
        resid_send[pl.ds(j, 1), :] = stream_recv[j]

    resid = resid_send[...] + proj.astype(f32)
    resid_send[...] = resid
    sub_w = lax.broadcasted_iota(jnp.int32, (batch, lanes), 0)
    lane_w = lax.broadcasted_iota(jnp.int32, (batch, lanes), 1)
    squares = jnp.sum(resid * resid, axis=-1, keepdims=True)
    sq_send[...] = jnp.sum(jnp.where(sub_w == lane_w, squares, 0.0), axis=0, keepdims=True)

    def sq_copy(to, slot):
        return remote(sq_send, sq_recv.at[slot], q_send.at[to], q_recv.at[slot], to)

    def resid_copy(to, slot):
        return remote(
            resid_send, resid_recv.at[slot], r_send.at[to], r_recv.at[slot], m * hsplit + to
        )

    @pl.loop(1, members)
    def _(d):
        sq_copy(peer(d), me).start()

    @pl.loop(1, hsplit)
    def _(d):
        resid_copy(mate(d), h).start()

    sq_recv[me] = sq_send[...]
    resid_recv[h] = resid_send[...]

    @pl.loop(1, hsplit)
    def _(d):
        resid_copy(h, mate(d)).wait_recv()

    @pl.loop(1, members)
    def _(d):
        sq_copy(me, peer(d)).wait_recv()

    squares = jnp.sum(sq_recv[...], axis=0)
    squares = jnp.sum(jnp.where(sub_w == lane_w, squares, 0.0), axis=1, keepdims=True)
    power = squares * (1.0 / width)
    inverse = lax.rsqrt(power + 1e-05)
    block_resid = jnp.concatenate([resid_recv[j] for j in range(hsplit)], axis=1)
    normed[...] = (block_resid * inverse * gain[m]).astype(bf16)

    bases = [q * cap // 8 * 8 for q in range(4)]
    for q in range(4):
        r = q % 2
        shift = q * cap - bases[q]
        at = lax.broadcasted_iota(jnp.int32, (lead, batch), 0)
        hit = (at == rank[r].astype(jnp.int32) + shift) & (named[r] > 0.0)
        slots_in[q] = jnp.dot(
            jnp.where(hit, 1.0, 0.0).astype(bf16), normed[...], preferred_element_type=f32
        ).astype(bf16)
    acc[...] = jnp.zeros_like(acc)

    def part_copy(to, slot):
        return remote(
            part_send.at[to],
            part_recv.at[slot],
            p_send.at[to],
            p_recv.at[slot],
            to * hsplit + h,
        )

    def gather(slot, q):
        return jnp.dot(
            slots_in[ORDER[q]], gu[slot, q], preferred_element_type=f32
        ), pl.ds(bases[ORDER[q]], lead)

    if chunks == 1:
        for q in range(4):
            gu_copy(0, q).wait()
            value, rows = gather(0, q)
            acc[rows, :] += value
        for to in range(MSPLIT):
            part_send[to] = acc[:packed, to * narrow : (to + 1) * narrow].astype(bf16)

        @pl.loop(1, MSPLIT)
        def _(d):
            part_copy(model(d), m).start()

    else:

        @pl.loop(0, MSPLIT)
        def _(i):
            slot = lax.rem(i, ring)
            to = model(MSPLIT - 1 - i)
            for q in range(4):
                gu_copy(i, q).wait()
                value, rows = gather(slot, q)
                acc[rows, :] += value

                @pl.when(i < MSPLIT - ring)
                def _():
                    gu_copy(i + ring, q).start()

            part_send[to] = acc[:packed, :].astype(bf16)
            acc[...] = jnp.zeros_like(acc)

            @pl.when(i < MSPLIT - 1)
            def _():
                part_copy(to, m).start()

    @pl.loop(1, MSPLIT)
    def _(d):
        part_copy(m, model(d)).wait_recv()

    part_recv[m] = part_send[m]
    acc[:packed, :narrow] = jnp.sum(part_recv[...].astype(f32), axis=0)
    a = acc[:hid_rows, :narrow]
    b = acc[2 * cap : 2 * cap + hid_rows, :narrow]
    hid_send[...] = (a / (1.0 + jnp.exp(-a)) * b).astype(bf16)

    def hid_copy(d, slot):
        return remote(
            hid_send, hid_recv.at[slot], h_send.at[d], h_recv.at[slot], model(d) * hsplit + h
        )

    def hid_relay(j, slot):
        return remote(
            hid_recv.at[slot],
            hid_recv.at[slot],
            h_relay.at[j],
            h_recv.at[slot],
            model(1) * hsplit + h,
        )

    hid_copy(1, m).start()

    @pl.loop(1, MSPLIT // 2)
    def _(j):
        hid_copy(MSPLIT - 2 * j, m).start()

    hid_recv[m] = hid_send[...]
    total[...] = jnp.zeros_like(total)

    def expert_sums(i, slot):
        for r in range(RESIDENT):
            down_copy(i, r).wait()
            total[r] += jnp.dot(hid_recv[slot], down[i, r], preferred_element_type=f32)

    @pl.loop(0, MSPLIT // 2)
    def _(j):
        even, odd = model(2 * j), model(2 * j + 1)

        @pl.when(j > 0)
        def _():
            hid_copy(2 * j, even).wait_recv()
            hid_relay(j, even).start()

        expert_sums(2 * j, even)
        hid_copy(1, odd).wait_recv()
        expert_sums(2 * j + 1, odd)

    whole = jnp.where(h == 0, 1.0, 0.0) * block_resid
    for r in range(RESIDENT):
        if batch > 32:
            whole = whole + jnp.dot(
                back[r], total[r], precision=lax.Precision.HIGHEST, preferred_element_type=f32
            )
        else:
            for n in range(r * cap, (r + 1) * cap):
                whole = whole + back[r][:, n : n + 1] * total[r, n : n + 1, :]
    resid_full[...] = whole

    @pl.loop(0, members)
    def _(j):
        final_send[j] = resid_full[pl.ds(j, 1), :]

    def final_copy(to, slot):
        return remote(
            final_send.at[to], final_recv.at[slot], f_send.at[to], f_recv.at[slot], to
        )

    @pl.loop(1, members)
    def _(d):
        final_copy(peer(d), me).start()

    final_recv[me] = final_send[me]

    @pl.loop(1, members)
    def _(d):
        final_copy(me, peer(d)).wait_recv()

    for j in range(MSPLIT):
        line = final_recv[j * hsplit]
        for k in range(1, hsplit):
            line = line + final_recv[j * hsplit + k]
        out[:, j * block : (j + 1) * block] = line.astype(bf16)

    @pl.loop(1, members)
    def _(d):
        to = peer(d)
        stream_copy(to, me).wait_send()
        sq_copy(to, me).wait_send()
        final_copy(to, me).wait_send()

    @pl.loop(1, hsplit)
    def _(d):
        resid_copy(mate(d), h).wait_send()

    @pl.loop(0, MSPLIT)
    def _(i):
        @pl.loop(1, hsplit)
        def _(d):
            attn_relay(i, mate(d), me).wait_send()

    @pl.loop(1, MSPLIT)
    def _(d):
        attn_copy(d, me).wait_send()
        part_copy(model(d), m).wait_send()

    hid_copy(1, m).wait_send()

    @pl.loop(1, MSPLIT // 2)
    def _(j):
        hid_copy(2 * j, m).wait_send()
        hid_relay(j, m).wait_send()

def on_device(
    stream_in,
    query,
    key_new,
    value_new,
    key_cache,
    value_cache,
    lengths,
    route_ids,
    route_scores,
    out_weight,
    norm_gain,
    gate_weight,
    up_weight,
    down_weight,
):
    f32, bf16 = jnp.float32, jnp.bfloat16
    members = lax.axis_size("gx")
    width = stream_in.shape[1]
    hsplit = members // MSPLIT
    cols = width // members
    block = width // MSPLIT
    batch = members
    hidden_cols = gate_weight.shape[2]
    narrow = hidden_cols // MSPLIT
    chunk = narrow if narrow % 128 == 0 else hidden_cols
    ring = min(RING, hidden_cols // chunk)
    vmem = pl.BlockSpec(memory_space=pltpu.VMEM)
    smem = pl.BlockSpec(memory_space=pltpu.SMEM)
    hbm = pl.BlockSpec(memory_space=pl.ANY)
    dma = pltpu.SemaphoreType.DMA
    rows = key_cache.shape[1]
    cap = batch * 5 // 8
    packed = 2 * RESIDENT * cap
    shifts = [q * cap % 8 for q in range(4)]
    lead = (cap + max(shifts) + 7) // 8 * 8
    hid_rows = (RESIDENT * cap + 7) // 8 * 8
    lanes = (batch + 127) // 128 * 128
    if narrow % 128 == 0 and 256 <= narrow <= block and NH * HS * cols == 4 * block * block:
        return large_call(
            stream_in,
            query,
            key_new,
            value_new,
            key_cache,
            value_cache,
            lengths,
            route_ids,
            route_scores,
            out_weight,
            norm_gain,
            gate_weight,
            up_weight,
            down_weight,
        )
    return pl.pallas_call(
        functools.partial(small_kernel, members),
        out_shape=jax.ShapeDtypeStruct((1, width), bf16),
        in_specs=[vmem] * 3 + [hbm] * 2 + [smem] * 3 + [vmem] * 2 + [hbm] * 4,
        out_specs=vmem,
        scratch_shapes=[
            pltpu.VMEM((rows, KVH * HS), bf16),
            pltpu.VMEM((rows, KVH * HS), bf16),
            dma((2,)),
            pltpu.VMEM((NH, HS), f32),
            pltpu.VMEM((2, KVH, HS), f32),
            pltpu.VMEM((members, 1, cols), f32),
            pltpu.VMEM(out_weight.shape, bf16),
            pltpu.VMEM((ring, 4, block, chunk), bf16),
            pltpu.VMEM((MSPLIT, RESIDENT, narrow, block), bf16),
            pltpu.VMEM((NH + PAD, HS), bf16),
            pltpu.VMEM((members, NH + PAD, HS), bf16),
            pltpu.VMEM((members * (NH + PAD), HS), f32),
            pltpu.VMEM((batch, NH * HS), bf16),
            pltpu.VMEM((members, 1, cols), f32),
            pltpu.VMEM((hsplit, batch, cols), f32),
            pltpu.VMEM((batch, cols), f32),
            pltpu.VMEM((1, lanes), f32),
            pltpu.VMEM((members, 1, lanes), f32),
            pltpu.VMEM((batch, block), bf16),
            pltpu.VMEM((4, lead, block), bf16),
            pltpu.VMEM((packed + 8, chunk), f32),
            pltpu.VMEM((MSPLIT, packed, narrow), bf16),
            pltpu.VMEM((MSPLIT, packed, narrow), bf16),
            pltpu.VMEM((hid_rows, narrow), bf16),
            pltpu.VMEM((MSPLIT, hid_rows, narrow), bf16),
            pltpu.VMEM((RESIDENT, hid_rows, block), f32),
            pltpu.VMEM((batch, block), f32),
            pltpu.VMEM((members, 1, block), f32),
            pltpu.VMEM((members, 1, block), f32),
            dma,
            dma((ring, 4)),
            dma((MSPLIT, RESIDENT)),
        ]
        + [dma((MSPLIT,)), dma((MSPLIT, hsplit))]
        + [dma((members,))] * 5
        + [dma((hsplit,))] * 2
        + [dma((MSPLIT,))] * 5
        + [dma((members,))] * 2,
        compiler_params=pltpu.CompilerParams(
            collective_id=0, has_side_effects=True, vmem_limit_bytes=67043328
        ),
    )(
        query,
        key_new,
        value_new,
        key_cache.reshape(rows, KVH * HS),
        value_cache.reshape(rows, KVH * HS),
        lengths,
        route_ids,
        route_scores,
        stream_in,
        norm_gain.reshape(MSPLIT, 1, block),
        out_weight,
        gate_weight,
        up_weight,
        down_weight,
    )

def solution(mesh):
    return jax.shard_map(
        on_device,
        mesh=mesh,
        in_specs=(
            P(("groups", "gx"), None),
            P(("groups", "gx"), None),
            P(("groups", "gx"), None),
            P(("groups", "gx"), None),
            P(("groups", "gx"), None, None),
            P(("groups", "gx"), None, None),
            P(("groups", "gx")),
            P(("groups", "gx"), None),
            P(("groups", "gx"), None),
            P(None, "gx"),
            P(),
            P(None, "gx", None),
            P(None, "gx", None),
            P(None, "gx", None),
        ),
        out_specs=P(("groups", "gx"), None),
        check_vma=False,
    )
```
